32 devices in a mesh: dom: 32 (over z, y, x, core).
Axes of the slice: x: 2, y: 2, z: 4, core: 2. Of those that a mesh axis runs over, the one named last changes fastest.
Arguments:
- features: bfloat16 [32768, 256], P('dom'), may hold values from -6 to 6
- edge_source: int32 [32, 128, 128], P('dom'), may hold values from 0 to 2047, as said below
- edge_relation: int32 [32, 128, 128], P('dom'), may hold values from 0 to 7
- edge_target: int32 [32, 128, 128], P('dom'), may hold values from 0 to 1023, as said below
- block_count: int32 [32], P('dom'), may hold values from 1 to 128, as said below
- send_list: int32 [32, 32, 32], P('dom'), may hold values from 0 to 1023
- bases_first: bfloat16 [30, 256, 256], P(None, 'dom'), may hold values from -0.375 to 0.375
- self_first: bfloat16 [256, 256], P('dom'), may hold values from -0.375 to 0.375
- coef_first: float32 [8, 30], replicated, may hold values from -1 to 1
- bias_first: float32 [256], replicated, may hold values from -3 to 3
- bases_second: bfloat16 [30, 256, 256], P(None, 'dom'), may hold values from -0.375 to 0.375
- self_second: bfloat16 [256, 256], P('dom'), may hold values from -0.375 to 0.375
- coef_second: float32 [8, 30], replicated, may hold values from -1 to 1
- bias_second: float32 [256], replicated, may hold values from -3 to 3
Outputs:
- embedded: bfloat16 [32768, 256], P('dom')
The draws below stay inside these ranges and needn't reach their ends.
Inputs may be any that keep to these rules, and one draw needn't show every extreme that they name: `edge_source`: an entry below 1024 names a row of the edge's own partition; an entry 1024 + p * 32 + s names the row that partition p sends to the edge's partition in slot s, and p is never the edge's own partition. `edge_target`: non-decreasing within each block; all targets of one block lie in one aligned window of 16 rows, from 16 * k to 16 * k + 15 for some k. `block_count`: blocks at and beyond it are ignored; some partition uses all 128.
All inputs are finite; a program needn't handle non-finite values.
Results may differ from the reference program's by a relative error of at most 0.0064.
Values may be sent and summed in bfloat16 or wider, within the bound.
No kernel may reach another device: no remote copies, remote signals or barrier semaphores. Data moves between devices by JAX's collectives and lax.ppermute only.
A program may use at most 128 MiB of HBM per device.

```python
import jax
import jax.numpy as jnp
from jax import lax

D = 256
REL = 8
BASES = 30
NODE_DEV = 1024
SLOT = 32
BLOCKS = 128
EBLK = 128
WIN = 16
NODES = 32768
N_DOM = 32


def draw_edge_source(key, part):
    key_used, key_local, key_offset, key_slot, key_remote = jax.random.split(key, 5)
    shape = (N_DOM, BLOCKS, EBLK)
    sent_counts = jax.random.randint(key_used, (N_DOM, N_DOM), SLOT // 4, SLOT + 1)
    local_rows = jax.random.randint(key_local, shape, 0, NODE_DEV)
    offset = jax.random.randint(key_offset, shape, 1, N_DOM)
    target_part = jnp.arange(N_DOM, dtype=jnp.int32)[:, None, None]
    owner = (target_part + offset) % N_DOM
    limit = sent_counts[owner, target_part]
    slot_index = jax.random.randint(key_slot, shape, 0, 1 << 20) % limit
    remote = jax.random.randint(key_remote, shape, 0, 2) == 1
    return jnp.where(remote, NODE_DEV + owner * SLOT + slot_index, local_rows).astype(jnp.int32)


def draw_edge_target(key, part):
    key_window, key_offset = jax.random.split(key)
    windows = jnp.sort(jax.random.randint(key_window, (N_DOM, BLOCKS), 0, NODE_DEV // WIN), axis=1)
    offsets = jnp.sort(jax.random.randint(key_offset, (N_DOM, BLOCKS, EBLK), 0, WIN), axis=2)
    return (windows[:, :, None] * WIN + offsets).astype(jnp.int32)


def draw_block_count(key, part):
    key_counts, key_top = jax.random.split(key)
    counts = jax.random.randint(key_counts, (N_DOM,), max(BLOCKS // 2, 1), BLOCKS + 1)
    busiest = jax.random.randint(key_top, (), 0, N_DOM)
    return counts.at[busiest].set(BLOCKS).astype(jnp.int32)


def place_ends(entries, own_key, least, largest):
    spot = [jax.random.randint(jax.random.fold_in(own_key, axis), (), 0, length) for axis, length in enumerate(entries.shape)]
    main_axis = entries.shape.index(max(entries.shape))
    next_to = spot[:main_axis] + [(spot[main_axis] + 1) % entries.shape[main_axis]] + spot[main_axis + 1:]
    return entries.at[tuple(spot)].set(least).at[tuple(next_to)].set(largest)


def steps_of(own_key, shape, cuts, least, top_value):
    loudness = 1.0
    for dim, blocks in cuts:
        heights = jax.random.uniform(jax.random.fold_in(jax.random.fold_in(own_key, 6), dim), (blocks,), jnp.float32, least / len(cuts), top_value / len(cuts))
        loudness = loudness * jnp.repeat(jnp.exp(heights), shape[dim] // blocks).reshape((-1,) + (1,) * (len(shape) - 1 - dim))
    return loudness


def scatter_about(rng, dims, deviation, most, pieces=(), kind=jnp.bfloat16):
    drawn = deviation * jax.random.normal(rng, dims, jnp.float32)
    if pieces:
        drawn = drawn * steps_of(rng, dims, pieces, -0.22, 0.18)
    return jnp.clip(drawn, -most, most).astype(kind)


def setup_inputs(seed: int = 0) -> dict:
    streams_of = jax.random.split(jax.random.key(seed), 15)
    return {
        "features": scatter_about(streams_of[0], (NODES, D), 1.0, 6.0, ((0, 32),)),
        "edge_source": draw_edge_source(jax.random.fold_in(streams_of[14], 71), 0),
        "edge_relation": place_ends(jax.random.randint(streams_of[2], (N_DOM, BLOCKS, EBLK), 0, REL), jax.random.fold_in(streams_of[2], 1), 0, REL - 1).astype(jnp.int32),
        "edge_target": draw_edge_target(jax.random.fold_in(streams_of[14], 71), 0),
        "block_count": draw_block_count(jax.random.fold_in(streams_of[14], 71), 0),
        "send_list": place_ends(jax.random.randint(streams_of[5], (N_DOM, N_DOM, SLOT), 0, NODE_DEV), jax.random.fold_in(streams_of[5], 1), 0, NODE_DEV - 1).astype(jnp.int32),
        "bases_first": scatter_about(streams_of[6], (BASES, D, D), D ** -0.5, 0.375, ((1, 32),)),
        "self_first": scatter_about(streams_of[7], (D, D), D ** -0.5, 0.375, ((0, 32),)),
        "coef_first": scatter_about(streams_of[8], (REL, BASES), BASES ** -0.5, 1.0, (), jnp.float32),
        "bias_first": scatter_about(streams_of[9], (D,), 0.5, 3.0, (), jnp.float32),
        "bases_second": scatter_about(streams_of[10], (BASES, D, D), D ** -0.5, 0.375, ((1, 32),)),
        "self_second": scatter_about(streams_of[11], (D, D), D ** -0.5, 0.375, ((0, 32),)),
        "coef_second": scatter_about(streams_of[12], (REL, BASES), BASES ** -0.5, 1.0, (), jnp.float32),
        "bias_second": scatter_about(streams_of[13], (D,), 0.5, 3.0, (), jnp.float32),
    }


def compose_weights(coef, bases):
    mixed = jnp.einsum("rb,bij->rij", coef, bases.astype(jnp.float32), precision=lax.Precision.HIGHEST)
    return mixed.astype(jnp.bfloat16)


def relational_layer(inputs_now, edge_source, edge_relation, edge_target, block_count, send_list, mixed, self_weight, bias):
    owners = jnp.arange(N_DOM, dtype=jnp.int32)

    def one_part(part_index):
        received = inputs_now[owners[:, None], send_list[:, part_index, :]].reshape(-1, D)
        row_table = jnp.concatenate([inputs_now[part_index], received], axis=0)
        sources = edge_source[part_index].reshape(-1)
        relation_ids = edge_relation[part_index].reshape(-1)
        targets = edge_target[part_index].reshape(-1)
        block_ids = lax.broadcasted_iota(jnp.int32, (BLOCKS, EBLK), 0).reshape(-1)
        in_use = block_ids < block_count[part_index]
        messages = row_table[sources].astype(jnp.float32)
        segment = jnp.where(in_use, targets * REL + relation_ids, NODE_DEV * REL)
        degree = jax.ops.segment_sum(jnp.ones(segment.shape, jnp.float32), segment, NODE_DEV * REL + 1)[:NODE_DEV * REL]
        pooled = jax.ops.segment_sum(messages, segment, NODE_DEV * REL + 1)[:NODE_DEV * REL]
        averaged = (pooled / jnp.maximum(degree, 1.0)[:, None]).astype(jnp.bfloat16).reshape(NODE_DEV, REL, D)
        summed_all = jnp.dot(inputs_now[part_index], self_weight, preferred_element_type=jnp.float32) + bias
        for relation in range(REL):
            summed_all = summed_all + jnp.dot(averaged[:, relation, :], mixed[relation], preferred_element_type=jnp.float32)
        return summed_all

    return lax.map(one_part, owners)


def reference(features, edge_source, edge_relation, edge_target, block_count, send_list, bases_first, self_first, coef_first, bias_first, bases_second, self_second, coef_second, bias_second):
    inputs_now = features.reshape(N_DOM, NODE_DEV, D)
    mixed_first = compose_weights(coef_first, bases_first)
    first = relational_layer(inputs_now, edge_source, edge_relation, edge_target, block_count, send_list, mixed_first, self_first, bias_first)
    hidden = jnp.maximum(first, 0.0).astype(jnp.bfloat16)
    mixed_second = compose_weights(coef_second, bases_second)
    second = relational_layer(hidden, edge_source, edge_relation, edge_target, block_count, send_list, mixed_second, self_second, bias_second)
    return second.astype(jnp.bfloat16).reshape(N_DOM * NODE_DEV, D)
```

```python
import functools

import jax
import jax.numpy as jnp
from jax import lax
from jax.experimental import pallas as pl
from jax.experimental.pallas import tpu as pltpu
from jax.sharding import PartitionSpec as P

WIN = 16
CHUNK = 512
MIB = 1 << 20
RESIDENT_MAX = 36 * MIB
CONTRACT_LANES = (((1,), (1,)), ((), ()))


def estimate(flops, nbytes):
    return pl.CostEstimate(flops=int(flops), bytes_accessed=int(nbytes), transcendentals=0)


def params(mib, **more):
    return pltpu.CompilerParams(vmem_limit_bytes=mib * MIB, **more)


def hot(rows, lanes):
    row_ids = lax.broadcasted_iota(jnp.int32, (rows, lanes.shape[1]), 0)
    return jnp.where(row_ids == lanes, 1.0, 0.0)


def code_edges(source_ref, relation_ref, target_ref, slot_ref, code_ref, low_ref, relations):
    slot = relation_ref[...] * WIN + (target_ref[...] & (WIN - 1))
    slot_ref[...] = slot
    code_ref[...] = (source_ref[...] // CHUNK) * (WIN * relations) + slot
    low_ref[...] = source_ref[...] & (CHUNK - 1)


def link_blocks(tile_ref, count_ref, head_ref, next_ref, tiles):
    def clear(t, carry):
        head_ref[t] = -1
        return carry

    lax.fori_loop(0, tiles, clear, 0)

    def link(b, carry):
        t = tile_ref[b] // WIN
        next_ref[b] = head_ref[t]
        head_ref[t] = b
        return carry

    lax.fori_loop(0, count_ref[0], link, 0)


def pair_of(first, next_ref):
    second = jnp.where(first >= 0, next_ref[jnp.maximum(first, 0)], -1)
    after = jnp.where(second >= 0, next_ref[jnp.maximum(second, 0)], -1)
    return second, after


def pair_rows(ref, first, second):
    one = jnp.where(first >= 0, ref[pl.ds(jnp.maximum(first, 0), 1), :], -1)
    two = jnp.where(second >= 0, ref[pl.ds(jnp.maximum(second, 0), 1), :], -1)
    return jnp.concatenate([one, two], axis=1)


def pair_counts(first, second, slot_ref, code_ref, low_ref, rows, slots):
    left = hot(rows, pair_rows(code_ref, first, second)).astype(jnp.bfloat16)
    right = hot(CHUNK, pair_rows(low_ref, first, second)).astype(jnp.bfloat16)
    counts = lax.dot_general(left, right, CONTRACT_LANES, preferred_element_type=jnp.float32)
    degree = jnp.sum(hot(slots, pair_rows(slot_ref, first, second)), axis=1, keepdims=True)
    return counts, degree


def put_counts(counts, local_ref, remote_ref, row, slots, locals_):
    for piece in range(counts.shape[0] // slots):
        part = counts[piece * slots : (piece + 1) * slots].astype(jnp.bfloat16)
        if piece < locals_:
            local_ref[pl.ds(row, slots), pl.ds(piece * CHUNK, CHUNK)] = part
        else:
            remote_ref[pl.ds(row, slots), pl.ds((piece - locals_) * CHUNK, CHUNK)] = part


def build_resident(
    tile_ref, count_ref, source_ref, relation_ref, target_ref,
    local_ref, remote_ref, degree_ref,
    head_ref, next_ref, slot_ref, code_ref, low_ref, sum_ref,
    *, tiles, relations, locals_, pieces, unroll,
):
    slots = WIN * relations
    rows = pieces * slots
    code_edges(source_ref, relation_ref, target_ref, slot_ref, code_ref, low_ref, relations)
    link_blocks(tile_ref, count_ref, head_ref, next_ref, tiles)

    def base(i, carry):
        for u in range(unroll):
            t = i * unroll + u
            first = head_ref[t]
            second, after = pair_of(first, next_ref)
            counts, degree = pair_counts(first, second, slot_ref, code_ref, low_ref, rows, slots)
            row = pl.multiple_of(t * slots, slots)
            put_counts(counts, local_ref, remote_ref, row, slots, locals_)
            degree_ref[pl.ds(row, slots), :] = degree
            head_ref[t] = after
        return carry

    lax.fori_loop(0, tiles // unroll, base, 0)

    def rest(t, carry):
        @pl.when(head_ref[t] >= 0)
        def _():
            row = pl.multiple_of(t * slots, slots)
            for piece in range(pieces):
                ref, at = (local_ref, piece) if piece < locals_ else (remote_ref, piece - locals_)
                sum_ref[pl.ds(piece * slots, slots), :] = ref[
                    pl.ds(row, slots), pl.ds(at * CHUNK, CHUNK)
                ].astype(jnp.float32)

            def step(first):
                second, after = pair_of(first, next_ref)
                counts, degree = pair_counts(first, second, slot_ref, code_ref, low_ref, rows, slots)
                sum_ref[...] += counts
                degree_ref[pl.ds(row, slots), :] += degree
                return after

            lax.while_loop(lambda first: first >= 0, step, head_ref[t])
            put_counts(sum_ref[...], local_ref, remote_ref, row, slots, locals_)

        return carry

    lax.fori_loop(0, tiles, rest, 0)


def build_streamed(
    tile_ref, count_ref, source_ref, relation_ref, target_ref,
    local_ref, remote_ref, degree_ref,
    head_ref, next_ref, slot_ref, code_ref, low_ref, sum_ref,
    *, tiles, relations, locals_, pieces, unroll,
):
    slots = WIN * relations
    rows = pieces * slots
    t = pl.program_id(0)

    @pl.when(t == 0)
    def _():
        code_edges(source_ref, relation_ref, target_ref, slot_ref, code_ref, low_ref, relations)
        link_blocks(tile_ref, count_ref, head_ref, next_ref, tiles)

    sum_ref[...] = jnp.zeros_like(sum_ref)
    degree_ref[...] = jnp.zeros_like(degree_ref)

    def step(first):
        second, after = pair_of(first, next_ref)
        counts, degree = pair_counts(first, second, slot_ref, code_ref, low_ref, rows, slots)
        sum_ref[...] += counts
        degree_ref[...] += degree
        return after

    lax.while_loop(lambda first: first >= 0, step, head_ref[t])
    put_counts(sum_ref[...], local_ref, remote_ref, 0, slots, locals_)


def build(tile_of, count, source, relation, target, *, node_rows, relations, remote_rows, resident):
    blocks, width = source.shape
    tiles, slots = node_rows // WIN, WIN * relations
    locals_, remotes = node_rows // CHUNK, remote_rows // CHUNK
    pieces = locals_ + remotes
    smem = pl.BlockSpec(memory_space=pltpu.SMEM)
    settings = dict(tiles=tiles, relations=relations, locals_=locals_, pieces=pieces, unroll=2)
    shapes = [
        ((tiles * slots, node_rows), jnp.bfloat16),
        ((tiles * slots, remote_rows), jnp.bfloat16),
        ((tiles * slots, 1), jnp.float32),
    ]
    scratch = [
        pltpu.SMEM((tiles,), jnp.int32),
        pltpu.SMEM((blocks,), jnp.int32),
        pltpu.VMEM((blocks, width), jnp.int32),
        pltpu.VMEM((blocks, width), jnp.int32),
        pltpu.VMEM((blocks, width), jnp.int32),
        pltpu.VMEM((pieces * slots, CHUNK), jnp.float32),
    ]
    cost = estimate(
        2 * (tiles + blocks // 4) * pieces * slots * CHUNK * 2 * width,
        2 * tiles * slots * pieces * CHUNK,
    )
    args = (tile_of, count, source, relation, target)
    if resident:
        vmem = pl.BlockSpec(memory_space=pltpu.VMEM)
        return pl.pallas_call(
            functools.partial(build_resident, **settings),
            out_shape=[pltpu.VMEM(s, d) for s, d in shapes],
            in_specs=[smem, smem, vmem, vmem, vmem],
            out_specs=[vmem, vmem, vmem],
            scratch_shapes=scratch,
            compiler_params=params(12),
            cost_estimate=cost,
            name="build",
        )(*args)
    whole = pl.BlockSpec((blocks, width), lambda t: (0, 0))
    return pl.pallas_call(
        functools.partial(build_streamed, **settings),
        grid=(tiles,),
        out_shape=[jax.ShapeDtypeStruct(s, d) for s, d in shapes],
        in_specs=[smem, smem, whole, whole, whole],
        out_specs=[pl.BlockSpec((slots, s[1]), lambda t: (t, 0)) for s, _ in shapes],
        scratch_shapes=scratch,
        compiler_params=params(40),
        cost_estimate=cost,
        name="build",
    )(*args)


def apply_local_body(counts_ref, table_ref, pooled_ref, *, group):
    def step(i, carry):
        rows = pl.ds(pl.multiple_of(i * group, group), group)
        pooled_ref[rows, :] = jnp.dot(
            counts_ref[rows, :], table_ref[...], preferred_element_type=jnp.float32
        )
        return carry

    lax.fori_loop(0, counts_ref.shape[0] // group, step, 0)


def apply_local(counts, table, *, resident, group=512):
    rows, depth = counts.shape
    width = table.shape[1]
    cost = estimate(2 * rows * depth * width, 2 * rows * depth)
    if resident:
        vmem = pl.BlockSpec(memory_space=pltpu.VMEM)
        return pl.pallas_call(
            functools.partial(apply_local_body, group=group),
            out_shape=pltpu.VMEM((rows, width), jnp.float32),
            in_specs=[vmem, vmem],
            out_specs=vmem,
            compiler_params=params(6),
            cost_estimate=cost,
            name="local",
        )(counts, table)
    return pl.pallas_call(
        functools.partial(apply_local_body, group=group),
        grid=(rows // group,),
        out_shape=jax.ShapeDtypeStruct((rows, width), jnp.float32),
        in_specs=[
            pl.BlockSpec((group, depth), lambda i: (i, 0)),
            pl.BlockSpec((depth, width), lambda i: (0, 0)),
        ],
        out_specs=pl.BlockSpec((group, width), lambda i: (i, 0)),
        compiler_params=params(40),
        cost_estimate=cost,
        name="local",
    )(counts, table)


def apply_remote_body(
    counts_ref, table_ref, pooled_ref, degree_ref, mean_ref, *, group, relations
):
    slots = WIN * relations
    width = table_ref.shape[1]

    def step(i, carry):
        rows = pl.ds(pl.multiple_of(i * group, group), group)
        total = pooled_ref[rows, :] + jnp.dot(
            counts_ref[rows, :], table_ref[...], preferred_element_type=jnp.float32
        )
        mean = (total * (1.0 / jnp.maximum(degree_ref[rows, :], 1.0))).astype(jnp.bfloat16)
        for tile in range(group // slots):
            at = i * (group // slots) + tile
            for relation in range(relations):
                start = tile * slots + relation * WIN
                mean_ref[
                    pl.ds(pl.multiple_of(at * WIN, WIN), WIN), pl.ds(relation * width, width)
                ] = mean[start : start + WIN]
        return carry

    lax.fori_loop(0, counts_ref.shape[0] // group, step, 0)


def apply_remote(counts, table, pooled, degree, *, relations, resident, group=512):
    rows, depth = counts.shape
    width = table.shape[1]
    nodes = rows // relations
    body = functools.partial(apply_remote_body, group=group, relations=relations)
    cost = estimate(2 * rows * depth * width, 2 * rows * depth)
    if resident:
        vmem = pl.BlockSpec(memory_space=pltpu.VMEM)
        return pl.pallas_call(
            body,
            out_shape=pltpu.VMEM((nodes, relations * width), jnp.bfloat16),
            in_specs=[vmem] * 4,
            out_specs=vmem,
            compiler_params=params(6),
            cost_estimate=cost,
            name="remote",
        )(counts, table, pooled, degree)
    return pl.pallas_call(
        body,
        grid=(rows // group,),
        out_shape=jax.ShapeDtypeStruct((nodes, relations * width), jnp.bfloat16),
        in_specs=[
            pl.BlockSpec((group, depth), lambda i: (i, 0)),
            pl.BlockSpec((depth, width), lambda i: (0, 0)),
            pl.BlockSpec((group, width), lambda i: (i, 0)),
            pl.BlockSpec((group, 1), lambda i: (i, 0)),
        ],
        out_specs=pl.BlockSpec((group // relations, relations * width), lambda i: (i, 0)),
        compiler_params=params(40),
        cost_estimate=cost,
        name="remote",
    )(counts, table, pooled, degree)


def dense_sum(side_ref, mean_ref, own_ref, mine_ref, other_ref, bias_ref):
    half = other_ref.shape[0]
    mine_at = pl.multiple_of(side_ref[0] * half, half)
    other_at = pl.multiple_of((1 - side_ref[0]) * half, half)
    total = jnp.dot(
        mean_ref[:, pl.ds(mine_at, half)], mine_ref[:half], preferred_element_type=jnp.float32
    )
    total += jnp.dot(
        mean_ref[:, pl.ds(other_at, half)], other_ref[...], preferred_element_type=jnp.float32
    )
    total += jnp.dot(own_ref[...], mine_ref[half:], preferred_element_type=jnp.float32)
    return total + bias_ref[...]


def dense_first_body(
    side_ref, mean_ref, own_ref, mine_ref, other_ref, bias_ref, send_ref, hidden_ref, out_ref
):
    total = dense_sum(side_ref, mean_ref, own_ref, mine_ref, other_ref, bias_ref)
    hidden_ref[...] = jnp.maximum(total, 0.0).astype(jnp.bfloat16)
    pick_body(send_ref, hidden_ref, out_ref)


def dense_second_body(side_ref, mean_ref, own_ref, mine_ref, other_ref, bias_ref, out_ref):
    total = dense_sum(side_ref, mean_ref, own_ref, mine_ref, other_ref, bias_ref)
    out_ref[...] = total.astype(jnp.bfloat16)


def pick_body(send_ref, rows_ref, out_ref):
    depth = rows_ref.shape[0]
    piece = 256

    def step(i, carry):
        rows = pl.ds(pl.multiple_of(i * piece, piece), piece)
        lanes = lax.broadcasted_iota(jnp.int32, (piece, depth), 1)
        chosen = jnp.where(send_ref[rows, :] == lanes, 1.0, 0.0).astype(jnp.bfloat16)
        out_ref[rows, :] = jnp.dot(
            chosen, rows_ref[...], preferred_element_type=jnp.float32
        ).astype(jnp.bfloat16)
        return carry

    lax.fori_loop(0, send_ref.shape[0] // piece, step, 0)


def pick(send, rows):
    vmem = pl.BlockSpec(memory_space=pltpu.VMEM)
    return pl.pallas_call(
        pick_body,
        out_shape=jax.ShapeDtypeStruct((send.shape[0], rows.shape[1]), rows.dtype),
        in_specs=[vmem, vmem],
        out_specs=vmem,
        compiler_params=params(16),
        cost_estimate=estimate(2 * send.shape[0] * rows.shape[0] * rows.shape[1], 0),
        name="pick",
    )(send, rows)


def dense(side, mean, own, mine, other, bias, send=None):
    nodes, width = own.shape
    vmem = pl.BlockSpec(memory_space=pltpu.VMEM)
    smem = pl.BlockSpec(memory_space=pltpu.SMEM)
    cost = estimate(2 * nodes * mean.shape[1] * width, 0)
    shape = jax.ShapeDtypeStruct((nodes, width), jnp.bfloat16)
    if send is None:
        return pl.pallas_call(
            dense_second_body,
            out_shape=shape,
            in_specs=[smem] + [vmem] * 5,
            out_specs=vmem,
            compiler_params=params(14),
            cost_estimate=cost,
            name="dense",
        )(side, mean, own, mine, other, bias)
    picked = jax.ShapeDtypeStruct((send.shape[0], width), jnp.bfloat16)
    return pl.pallas_call(
        dense_first_body,
        out_shape=[shape, picked],
        in_specs=[smem] + [vmem] * 6,
        out_specs=[vmem, vmem],
        compiler_params=params(16),
        cost_estimate=cost,
        name="dense",
    )(side, mean, own, mine, other, bias, send)


def weight_halves(bases, self_weight, coef):
    relations, width = coef.shape[0], bases.shape[2]
    mixed = jnp.einsum(
        "rb,bij->rij", coef, bases.astype(jnp.float32), precision=lax.Precision.HIGHEST
    ).astype(jnp.bfloat16)
    half = relations // 2
    halves = [
        jnp.concatenate([mixed[:half], self_weight[None]], axis=0),
        jnp.concatenate([mixed[half:], self_weight[None]], axis=0),
    ]
    return jnp.stack([h.reshape(-1, width) for h in halves])


def exchange(picked, halves, devices):
    width = picked.shape[1]
    rows = picked.reshape(devices, -1, width)
    weights = jnp.broadcast_to(halves[None], (devices // 2,) + halves.shape)
    outgoing = jnp.concatenate([rows, weights.reshape(devices, -1, width)], axis=1)
    return lax.all_to_all(outgoing, "dom", split_axis=0, concat_axis=0, tiled=True)


def split(incoming, slot, relations):
    devices, _, width = incoming.shape
    table = incoming[:, :slot].reshape(-1, width)
    mine = incoming[:, slot:].reshape(devices, relations // 2 + 1, -1, width)
    mine = jnp.swapaxes(mine, 0, 1).reshape(-1, width)
    swap = [(i, i ^ 1) for i in range(devices)]
    other = lax.ppermute(mine[: mine.shape[0] - width], "dom", swap)
    return table, mine, other


def shards(
    features,
    edge_source,
    edge_relation,
    edge_target,
    block_count,
    send_list,
    bases_first,
    self_first,
    coef_first,
    bias_first,
    bases_second,
    self_second,
    coef_second,
    bias_second,
):
    node_rows = features.shape[0]
    relations = coef_first.shape[0]
    devices, slot = send_list.shape[1:]
    remote_rows = devices * slot
    resident = 2 * node_rows * relations * (node_rows + remote_rows) <= RESIDENT_MAX
    side = (lax.axis_index("dom") & 1).astype(jnp.int32).reshape(1)
    send = send_list.reshape(-1, 1)
    halves_first = weight_halves(bases_first, self_first, coef_first)
    incoming = exchange(pick(send, features), halves_first, devices)
    halves_second = weight_halves(bases_second, self_second, coef_second)
    local, remote, degree = build(
        edge_target[0, :, 0],
        block_count,
        edge_source[0],
        edge_relation[0],
        edge_target[0],
        node_rows=node_rows,
        relations=relations,
        remote_rows=remote_rows,
        resident=resident,
    )
    pooled = apply_local(local, features, resident=resident)
    table, mine, other = split(incoming, slot, relations)
    mean = apply_remote(remote, table, pooled, degree, relations=relations, resident=resident)
    hidden, picked = dense(side, mean, features, mine, other, bias_first[None], send)
    incoming = exchange(picked, halves_second, devices)
    pooled = apply_local(local, hidden, resident=resident)
    table, mine, other = split(incoming, slot, relations)
    mean = apply_remote(remote, table, pooled, degree, relations=relations, resident=resident)
    return dense(side, mean, hidden, mine, other, bias_second[None])


def solution(mesh):
    placed = (
        P("dom", None),
        P("dom", None, None),
        P("dom", None, None),
        P("dom", None, None),
        P("dom"),
        P("dom", None, None),
        P(None, "dom", None),
        P("dom", None),
        P(),
        P(),
        P(None, "dom", None),
        P("dom", None),
        P(),
        P(),
    )
    return jax.shard_map(
        shards, mesh=mesh, in_specs=placed, out_specs=P("dom", None), check_vma=False
    )
```

```python
import functools

import jax
import jax.numpy as jnp
from jax import lax
from jax.experimental import pallas as pl
from jax.experimental.pallas import tpu as pltpu
from jax.sharding import PartitionSpec as P

WIN = 16
CHUNK = 512
GROUP = 8
MIB = 1 << 20
WHOLE_MAX = 36 * MIB
CONTRACT_LANES = (((1,), (1,)), ((), ()))


def estimate(flops, nbytes):
    return pl.CostEstimate(flops=int(flops), bytes_accessed=int(nbytes), transcendentals=0)


def params(mib, **more):
    return pltpu.CompilerParams(vmem_limit_bytes=mib * MIB, **more)


def hot(rows, lanes):
    row_ids = lax.broadcasted_iota(jnp.int32, (rows, lanes.shape[1]), 0)
    return jnp.where(row_ids == lanes, 1.0, 0.0)


def code_edges(source_ref, relation_ref, target_ref, slot_ref, code_ref, low_ref, relations):
    slot = relation_ref[...] * WIN + (target_ref[...] & (WIN - 1))
    slot_ref[...] = slot
    code_ref[...] = (source_ref[...] // CHUNK) * (WIN * relations) + slot
    low_ref[...] = source_ref[...] & (CHUNK - 1)


def link_blocks(tile_ref, count_ref, head_ref, next_ref, tiles):
    def clear(t, carry):
        head_ref[t] = -1
        return carry

    lax.fori_loop(0, tiles, clear, 0)

    def link(b, carry):
        t = tile_ref[b] // WIN
        next_ref[b] = head_ref[t]
        head_ref[t] = b
        return carry

    lax.fori_loop(0, count_ref[0], link, 0)


def pair_of(first, next_ref):
    second = jnp.where(first >= 0, next_ref[jnp.maximum(first, 0)], -1)
    after = jnp.where(second >= 0, next_ref[jnp.maximum(second, 0)], -1)
    return second, after


def pair_rows(ref, first, second):
    one = jnp.where(first >= 0, ref[pl.ds(jnp.maximum(first, 0), 1), :], -1)
    two = jnp.where(second >= 0, ref[pl.ds(jnp.maximum(second, 0), 1), :], -1)
    return jnp.concatenate([one, two], axis=1)


def pair_counts(first, second, slot_ref, code_ref, low_ref, rows, slots):
    left = hot(rows, pair_rows(code_ref, first, second)).astype(jnp.bfloat16)
    right = hot(CHUNK, pair_rows(low_ref, first, second)).astype(jnp.bfloat16)
    counts = lax.dot_general(left, right, CONTRACT_LANES, preferred_element_type=jnp.float32)
    degree = jnp.sum(hot(slots, pair_rows(slot_ref, first, second)), axis=1, keepdims=True)
    return counts, degree


def put_counts(counts, local_ref, remote_ref, row, slots, locals_):
    for piece in range(counts.shape[0] // slots):
        part = counts[piece * slots : (piece + 1) * slots].astype(jnp.bfloat16)
        if piece < locals_:
            local_ref[pl.ds(row, slots), pl.ds(piece * CHUNK, CHUNK)] = part
        else:
            remote_ref[pl.ds(row, slots), pl.ds((piece - locals_) * CHUNK, CHUNK)] = part


def build_streamed(
    tile_ref, count_ref, source_ref, relation_ref, target_ref,
    local_ref, remote_ref, degree_ref,
    head_ref, next_ref, slot_ref, code_ref, low_ref, sum_ref,
    *, tiles, relations, locals_, pieces,
):
    slots = WIN * relations
    rows = pieces * slots
    t = pl.program_id(0)

    @pl.when(t == 0)
    def _():
        code_edges(source_ref, relation_ref, target_ref, slot_ref, code_ref, low_ref, relations)
        link_blocks(tile_ref, count_ref, head_ref, next_ref, tiles)

    sum_ref[...] = jnp.zeros_like(sum_ref)
    degree_ref[...] = jnp.zeros_like(degree_ref)

    def step(first):
        second, after = pair_of(first, next_ref)
        counts, degree = pair_counts(first, second, slot_ref, code_ref, low_ref, rows, slots)
        sum_ref[...] += counts
        degree_ref[...] += degree
        return after

    lax.while_loop(lambda first: first >= 0, step, head_ref[t])
    put_counts(sum_ref[...], local_ref, remote_ref, 0, slots, locals_)


def build_streamed_call(tile_of, count, source, relation, target, *, node_rows, relations, remote_rows):
    blocks, width = source.shape
    tiles, slots = node_rows // WIN, WIN * relations
    locals_, remotes = node_rows // CHUNK, remote_rows // CHUNK
    pieces = locals_ + remotes
    smem = pl.BlockSpec(memory_space=pltpu.SMEM)
    shapes = [
        ((tiles * slots, node_rows), jnp.bfloat16),
        ((tiles * slots, remote_rows), jnp.bfloat16),
        ((tiles * slots, 1), jnp.float32),
    ]
    whole = pl.BlockSpec((blocks, width), lambda t: (0, 0))
    return pl.pallas_call(
        functools.partial(
            build_streamed, tiles=tiles, relations=relations, locals_=locals_, pieces=pieces
        ),
        grid=(tiles,),
        out_shape=[jax.ShapeDtypeStruct(s, d) for s, d in shapes],
        in_specs=[smem, smem, whole, whole, whole],
        out_specs=[pl.BlockSpec((slots, s[1]), lambda t: (t, 0)) for s, _ in shapes],
        scratch_shapes=[
            pltpu.SMEM((tiles,), jnp.int32),
            pltpu.SMEM((blocks,), jnp.int32),
            pltpu.VMEM((blocks, width), jnp.int32),
            pltpu.VMEM((blocks, width), jnp.int32),
            pltpu.VMEM((blocks, width), jnp.int32),
            pltpu.VMEM((pieces * slots, CHUNK), jnp.float32),
        ],
        compiler_params=params(40),
        cost_estimate=estimate(
            4 * (tiles + blocks // 4) * pieces * slots * CHUNK * width,
            2 * tiles * slots * pieces * CHUNK,
        ),
        name="build",
    )(tile_of, count, source, relation, target)


def local_streamed_body(counts_ref, table_ref, pooled_ref):
    pooled_ref[...] = jnp.dot(
        counts_ref[...], table_ref[...], preferred_element_type=jnp.float32
    )


def local_streamed(counts, table, *, group):
    rows, depth = counts.shape
    width = table.shape[1]
    return pl.pallas_call(
        local_streamed_body,
        grid=(rows // group,),
        out_shape=jax.ShapeDtypeStruct((rows, width), jnp.float32),
        in_specs=[
            pl.BlockSpec((group, depth), lambda i: (i, 0)),
            pl.BlockSpec((depth, width), lambda i: (0, 0)),
        ],
        out_specs=pl.BlockSpec((group, width), lambda i: (i, 0)),
        compiler_params=params(40),
        cost_estimate=estimate(2 * rows * depth * width, 2 * rows * depth),
        name="local",
    )(counts, table)


def put_means(mean, mean_ref, first_tile, relations):
    slots = WIN * relations
    width = mean.shape[1]
    for tile in range(mean.shape[0] // slots):
        at = pl.multiple_of((first_tile + tile) * WIN, WIN)
        for relation in range(relations):
            start = tile * slots + relation * WIN
            mean_ref[pl.ds(at, WIN), pl.ds(relation * width, width)] = mean[start : start + WIN]


def remote_streamed_body(counts_ref, table_ref, pooled_ref, degree_ref, mean_ref, *, relations):
    total = pooled_ref[...] + jnp.dot(
        counts_ref[...], table_ref[...], preferred_element_type=jnp.float32
    )
    mean = total * (1.0 / jnp.maximum(degree_ref[...], 1.0))
    put_means(mean.astype(jnp.bfloat16), mean_ref, 0, relations)


def remote_streamed(counts, table, pooled, degree, *, relations, group):
    rows, depth = counts.shape
    width = table.shape[1]
    return pl.pallas_call(
        functools.partial(remote_streamed_body, relations=relations),
        grid=(rows // group,),
        out_shape=jax.ShapeDtypeStruct((rows // relations, relations * width), jnp.bfloat16),
        in_specs=[
            pl.BlockSpec((group, depth), lambda i: (i, 0)),
            pl.BlockSpec((depth, width), lambda i: (0, 0)),
            pl.BlockSpec((group, width), lambda i: (i, 0)),
            pl.BlockSpec((group, 1), lambda i: (i, 0)),
        ],
        out_specs=pl.BlockSpec((group // relations, relations * width), lambda i: (i, 0)),
        compiler_params=params(40),
        cost_estimate=estimate(2 * rows * depth * width, 2 * rows * depth),
        name="remote",
    )(counts, table, pooled, degree)


def build_body(
    tile_ref, count_ref, source_ref, relation_ref, target_ref, own_ref,
    local_ref, remote_ref, pooled_ref, degree_ref,
    local_v, remote_v, pooled_v, head_ref, next_ref, list_ref, slot_ref, code_ref, low_ref, sum_ref,
    sems, *, tiles, relations, locals_, pieces,
):
    slots = WIN * relations
    rows = pieces * slots
    code_edges(source_ref, relation_ref, target_ref, slot_ref, code_ref, low_ref, relations)
    link_blocks(tile_ref, count_ref, head_ref, next_ref, tiles)
    head_ref[tiles] = -1
    counted = functools.partial(
        pair_counts, slot_ref=slot_ref, code_ref=code_ref, low_ref=low_ref, rows=rows, slots=slots
    )

    def place(t, piece):
        row = pl.multiple_of(t * slots, slots)
        ref, at = (local_v, piece) if piece < locals_ else (remote_v, piece - locals_)
        return ref, (pl.ds(row, slots), pl.ds(at * CHUNK, CHUNK))

    def part(counts, piece):
        return counts[piece * slots : (piece + 1) * slots]

    def add_degree(i, u, degree):
        lanes = lax.broadcasted_iota(jnp.int32, (slots, GROUP), 1)
        degree_ref[i] += jnp.where(lanes == u, degree, 0.0)

    def group(i, carry):
        for u in range(GROUP):
            t = i * GROUP + u
            first = head_ref[t]
            second, after = pair_of(first, next_ref)
            counts, degree = counted(first, second)
            for piece in range(pieces):
                ref, where = place(t, piece)
                ref[where] = part(counts, piece).astype(jnp.bfloat16)
            degree_ref[i, :, pl.ds(u, 1)] = degree
            head_ref[t] = after

        short = jnp.int32(0)
        for u in range(GROUP):
            t = i * GROUP + u
            first = head_ref[t]
            _, after = pair_of(first, next_ref)
            list_ref[short] = t
            short += jnp.where((first >= 0) & (after < 0), 1, 0)
        list_ref[short] = tiles

        def add_two(j, carry):
            for k in range(2):
                t = list_ref[2 * j + k]
                first = head_ref[t]
                second, _ = pair_of(first, next_ref)
                counts, degree = counted(first, second)
                for piece in range(pieces):
                    ref, where = place(t, piece)
                    total = ref[where].astype(jnp.float32) + part(counts, piece)
                    ref[where] = total.astype(jnp.bfloat16)
                add_degree(i, t - i * GROUP, degree)
            return carry

        lax.fori_loop(0, (short + 1) // 2, add_two, 0)

        def long(u, carry):
            t = i * GROUP + u
            first = head_ref[t]
            _, after = pair_of(first, next_ref)

            @pl.when(after >= 0)
            def _():
                for piece in range(pieces):
                    ref, where = place(t, piece)
                    sum_ref[pl.ds(piece * slots, slots), :] = ref[where].astype(jnp.float32)

                def step(first):
                    second, after = pair_of(first, next_ref)
                    counts, degree = counted(first, second)
                    sum_ref[...] += counts
                    add_degree(i, u, degree)
                    return after

                lax.while_loop(lambda first: first >= 0, step, first)
                for piece in range(pieces):
                    ref, where = place(t, piece)
                    ref[where] = sum_ref[pl.ds(piece * slots, slots), :].astype(jnp.bfloat16)

            return carry

        lax.fori_loop(0, GROUP, long, 0)
        some = pl.ds(pl.multiple_of(i * GROUP * slots, GROUP * slots), GROUP * slots)
        pooled_v[some, :] = jnp.dot(
            local_v[some, :], own_ref[...], preferred_element_type=jnp.float32
        )
        pltpu.make_async_copy(local_v.at[some], local_ref.at[some], sems.at[0]).start()
        pltpu.make_async_copy(remote_v.at[some], remote_ref.at[some], sems.at[1]).start()
        pltpu.make_async_copy(pooled_v.at[some], pooled_ref.at[some], sems.at[2]).start()
        return carry

    lax.fori_loop(0, tiles // GROUP, group, 0)
    every = pl.ds(0, tiles * slots)
    pltpu.make_async_copy(local_v.at[every], local_ref, sems.at[0]).wait()
    pltpu.make_async_copy(remote_v.at[every], remote_ref, sems.at[1]).wait()
    pltpu.make_async_copy(pooled_v, pooled_ref, sems.at[2]).wait()


def build(tile_of, count, source, relation, target, own, *, relations, remote_rows):
    blocks, block_width = source.shape
    node_rows, width = own.shape
    tiles, slots = node_rows // WIN, WIN * relations
    rows = tiles * slots
    locals_, remotes = node_rows // CHUNK, remote_rows // CHUNK
    pieces = locals_ + remotes
    vmem = pl.BlockSpec(memory_space=pltpu.VMEM)
    smem = pl.BlockSpec(memory_space=pltpu.SMEM)
    hbm = pl.BlockSpec(memory_space=pltpu.HBM)
    return pl.pallas_call(
        functools.partial(
            build_body, tiles=tiles, relations=relations, locals_=locals_, pieces=pieces
        ),
        out_shape=[
            jax.ShapeDtypeStruct((rows, node_rows), jnp.bfloat16),
            jax.ShapeDtypeStruct((rows, remote_rows), jnp.bfloat16),
            jax.ShapeDtypeStruct((rows, width), jnp.float32),
            jax.ShapeDtypeStruct((tiles // GROUP, slots, GROUP), jnp.float32),
        ],
        in_specs=[smem, smem, vmem, vmem, vmem, vmem],
        out_specs=[hbm, hbm, hbm, vmem],
        scratch_shapes=[
            pltpu.VMEM((rows + slots, node_rows), jnp.bfloat16),
            pltpu.VMEM((rows + slots, remote_rows), jnp.bfloat16),
            pltpu.VMEM((rows, width), jnp.float32),
            pltpu.SMEM((tiles + 1,), jnp.int32),
            pltpu.SMEM((blocks,), jnp.int32),
            pltpu.SMEM((GROUP + 1,), jnp.int32),
            pltpu.VMEM((blocks, block_width), jnp.int32),
            pltpu.VMEM((blocks, block_width), jnp.int32),
            pltpu.VMEM((blocks, block_width), jnp.int32),
            pltpu.VMEM((pieces * slots, CHUNK), jnp.float32),
            pltpu.SemaphoreType.DMA((3,)),
        ],
        compiler_params=params(58),
        cost_estimate=estimate(
            4 * (tiles + blocks // 4) * pieces * slots * CHUNK * block_width
            + 2 * rows * node_rows * width,
            2 * rows * pieces * CHUNK,
        ),
        name="build",
    )(tile_of, count, source, relation, target, own)


def pool_groups(counts_ref, counts_v, sems, table_ref, degree_ref, mean_ref, relations, extra=None):
    size = GROUP * WIN * relations
    groups = counts_ref.shape[0] // size

    def copies(i):
        some = pl.ds(pl.multiple_of(i * size, size), size)
        found = [pltpu.make_async_copy(counts_ref.at[some], counts_v.at[some], sems.at[0, i])]
        if extra is not None:
            found.append(pltpu.make_async_copy(extra[0].at[some], extra[1].at[some], sems.at[1, i]))
        return found

    def begin(i, carry):
        for copy in copies(i):
            copy.start()
        return carry

    def step(i, carry):
        for copy in copies(i):
            copy.wait()
        some = pl.ds(pl.multiple_of(i * size, size), size)
        total = jnp.dot(counts_v[some, :], table_ref[...], preferred_element_type=jnp.float32)
        if extra is not None:
            total += extra[1][some, :]
        share = 1.0 / jnp.maximum(degree_ref[i], 1.0)
        slots = WIN * relations
        for u in range(GROUP):
            mean = total[u * slots : (u + 1) * slots] * share[:, u : u + 1]
            put_means(mean.astype(jnp.bfloat16), mean_ref, i * GROUP + u, relations)
        return carry

    lax.fori_loop(0, groups, begin, 0)
    lax.fori_loop(0, groups, step, 0)


def pool_body(counts_ref, pooled_ref, table_ref, degree_ref, mean_ref, counts_v, pooled_v, sems, *, relations):
    pool_groups(
        counts_ref, counts_v, sems, table_ref, degree_ref, mean_ref, relations,
        extra=(pooled_ref, pooled_v),
    )


def pool(counts, pooled, table, degree, *, relations):
    rows, depth = counts.shape
    width = table.shape[1]
    vmem = pl.BlockSpec(memory_space=pltpu.VMEM)
    hbm = pl.BlockSpec(memory_space=pltpu.HBM)
    return pl.pallas_call(
        functools.partial(pool_body, relations=relations),
        out_shape=jax.ShapeDtypeStruct((rows // relations, relations * width), jnp.bfloat16),
        in_specs=[hbm, hbm, vmem, vmem],
        out_specs=vmem,
        scratch_shapes=[
            pltpu.VMEM(counts.shape, counts.dtype),
            pltpu.VMEM(pooled.shape, pooled.dtype),
            pltpu.SemaphoreType.DMA((2, degree.shape[0])),
        ],
        compiler_params=params(44),
        cost_estimate=estimate(2 * rows * depth * width, 2 * rows * depth),
        name="pool",
    )(counts, pooled, table, degree)


def part_body(
    side_ref, counts_ref, table_ref, degree_ref, mine_ref, other_ref, extra_ref,
    out_ref, counts_v, mean_v, sems, *, relations, last,
):
    pool_groups(counts_ref, counts_v, sems, table_ref, degree_ref, mean_v, relations)
    total = dense_sum(side_ref, mean_v, None if last else table_ref, mine_ref, other_ref, extra_ref)
    out_ref[...] = total.astype(out_ref.dtype)


def part(side, counts, table, degree, mine, other, extra, *, relations, last):
    rows, depth = counts.shape
    width = table.shape[1]
    nodes = rows // relations
    vmem = pl.BlockSpec(memory_space=pltpu.VMEM)
    smem = pl.BlockSpec(memory_space=pltpu.SMEM)
    hbm = pl.BlockSpec(memory_space=pltpu.HBM)
    return pl.pallas_call(
        functools.partial(part_body, relations=relations, last=last),
        out_shape=jax.ShapeDtypeStruct((nodes, width), jnp.bfloat16 if last else jnp.float32),
        in_specs=[smem, hbm, vmem, vmem, vmem, vmem, vmem],
        out_specs=vmem,
        scratch_shapes=[
            pltpu.VMEM(counts.shape, counts.dtype),
            pltpu.VMEM((nodes, relations * width), jnp.bfloat16),
            pltpu.SemaphoreType.DMA((1, degree.shape[0])),
        ],
        compiler_params=params(44),
        cost_estimate=estimate(
            2 * rows * depth * width + 2 * nodes * relations * width * width, 2 * rows * depth
        ),
        name="last" if last else "first",
    )(side, counts, table, degree, mine, other, extra)


def dense_sum(side_ref, mean_ref, own_ref, mine_ref, other_ref, bias_ref):
    half = other_ref.shape[0]
    mine_at = pl.multiple_of(side_ref[0] * half, half)
    other_at = pl.multiple_of((1 - side_ref[0]) * half, half)
    total = jnp.dot(
        mean_ref[:, pl.ds(mine_at, half)], mine_ref[:half], preferred_element_type=jnp.float32
    )
    total += jnp.dot(
        mean_ref[:, pl.ds(other_at, half)], other_ref[...], preferred_element_type=jnp.float32
    )
    if own_ref is not None:
        total += jnp.dot(own_ref[...], mine_ref[half:], preferred_element_type=jnp.float32)
    return total + bias_ref[...]


def dense_first_body(
    side_ref, mean_ref, own_ref, mine_ref, other_ref, bias_ref, send_ref, hidden_ref, out_ref
):
    total = dense_sum(side_ref, mean_ref, own_ref, mine_ref, other_ref, bias_ref)
    hidden_ref[...] = jnp.maximum(total, 0.0).astype(jnp.bfloat16)
    pick_body(send_ref, hidden_ref, out_ref)


def dense_second_body(side_ref, mean_ref, own_ref, mine_ref, other_ref, bias_ref, out_ref):
    total = dense_sum(side_ref, mean_ref, own_ref, mine_ref, other_ref, bias_ref)
    out_ref[...] = total.astype(jnp.bfloat16)


def pick_body(send_ref, rows_ref, out_ref):
    depth = rows_ref.shape[0]
    piece = 256

    def step(i, carry):
        rows = pl.ds(pl.multiple_of(i * piece, piece), piece)
        lanes = lax.broadcasted_iota(jnp.int32, (piece, depth), 1)
        chosen = jnp.where(send_ref[rows, :] == lanes, 1.0, 0.0).astype(jnp.bfloat16)
        out_ref[rows, :] = jnp.dot(
            chosen, rows_ref[...], preferred_element_type=jnp.float32
        ).astype(jnp.bfloat16)
        return carry

    lax.fori_loop(0, send_ref.shape[0] // piece, step, 0)


def pick(send, rows):
    vmem = pl.BlockSpec(memory_space=pltpu.VMEM)
    return pl.pallas_call(
        pick_body,
        out_shape=jax.ShapeDtypeStruct((send.shape[0], rows.shape[1]), rows.dtype),
        in_specs=[vmem, vmem],
        out_specs=vmem,
        compiler_params=params(16),
        cost_estimate=estimate(2 * send.shape[0] * rows.shape[0] * rows.shape[1], 0),
        name="pick",
    )(send, rows)


def dense(side, mean, own, mine, other, bias, send=None):
    nodes, width = own.shape
    vmem = pl.BlockSpec(memory_space=pltpu.VMEM)
    smem = pl.BlockSpec(memory_space=pltpu.SMEM)
    cost = estimate(2 * nodes * mean.shape[1] * width, 0)
    shape = jax.ShapeDtypeStruct((nodes, width), jnp.bfloat16)
    if send is None:
        return pl.pallas_call(
            dense_second_body,
            out_shape=shape,
            in_specs=[smem] + [vmem] * 5,
            out_specs=vmem,
            compiler_params=params(14),
            cost_estimate=cost,
            name="dense",
        )(side, mean, own, mine, other, bias)
    picked = jax.ShapeDtypeStruct((send.shape[0], width), jnp.bfloat16)
    return pl.pallas_call(
        dense_first_body,
        out_shape=[shape, picked],
        in_specs=[smem] + [vmem] * 6,
        out_specs=[vmem, vmem],
        compiler_params=params(16),
        cost_estimate=cost,
        name="dense",
    )(side, mean, own, mine, other, bias, send)


def weight_halves(bases, self_weight, coef):
    relations, width = coef.shape[0], bases.shape[2]
    mixed = jnp.einsum(
        "rb,bij->rij", coef, bases.astype(jnp.float32), precision=lax.Precision.HIGHEST
    ).astype(jnp.bfloat16)
    half = relations // 2
    halves = [
        jnp.concatenate([mixed[:half], self_weight[None]], axis=0),
        jnp.concatenate([mixed[half:], self_weight[None]], axis=0),
    ]
    return jnp.stack([h.reshape(-1, width) for h in halves])


def exchange(picked, weights, devices):
    rows = picked.reshape(devices, -1, picked.shape[1])
    if weights:
        halves = jnp.concatenate(weights, axis=1)
        halves = jnp.broadcast_to(halves[None], (devices // 2,) + halves.shape)
        rows = jnp.concatenate([rows, halves.reshape(devices, -1, rows.shape[2])], axis=1)
    return lax.all_to_all(rows, "dom", split_axis=0, concat_axis=0, tiled=True)


def join_weights(received, relations):
    devices, _, width = received.shape
    mine = received.reshape(devices, relations // 2 + 1, -1, width)
    mine = jnp.swapaxes(mine, 0, 1).reshape(-1, width)
    swap = [(i, i ^ 1) for i in range(devices)]
    return mine, lax.ppermute(mine[: mine.shape[0] - width], "dom", swap)


def shards(
    features,
    edge_source,
    edge_relation,
    edge_target,
    block_count,
    send_list,
    bases_first,
    self_first,
    coef_first,
    bias_first,
    bases_second,
    self_second,
    coef_second,
    bias_second,
):
    node_rows, width = features.shape
    relations = coef_first.shape[0]
    devices, slot = send_list.shape[1:]
    remote_rows = devices * slot
    side = (lax.axis_index("dom") & 1).astype(jnp.int32).reshape(1)
    send = send_list.reshape(-1, 1)
    halves = [
        weight_halves(bases_first, self_first, coef_first),
        weight_halves(bases_second, self_second, coef_second),
    ]
    incoming = exchange(pick(send, features), halves, devices)
    edges = (edge_target[0, :, 0], block_count, edge_source[0], edge_relation[0], edge_target[0])
    fits = 2 * node_rows * relations * (node_rows + remote_rows) <= WHOLE_MAX
    if fits:
        local, remote, pooled, degree = build(
            *edges, features, relations=relations, remote_rows=remote_rows
        )
    else:
        local, remote, degree = build_streamed_call(
            *edges, node_rows=node_rows, relations=relations, remote_rows=remote_rows
        )
        pooled = local_streamed(local, features, group=512)
    table = incoming[:, :slot].reshape(-1, width)
    rest = halves[0].shape[1]
    mine, other = join_weights(incoming[:, slot : slot + rest], relations)
    mine_next, other_next = join_weights(incoming[:, slot + rest :], relations)
    if fits:
        mean = pool(remote, pooled, table, degree, relations=relations)
    else:
        mean = remote_streamed(remote, table, pooled, degree, relations=relations, group=512)
    hidden, picked = dense(side, mean, features, mine, other, bias_first[None], send)
    table = exchange(picked, [], devices).reshape(-1, width)
    if fits:
        settings = dict(relations=relations)
        partial = part(
            side, local, hidden, degree, mine_next, other_next, bias_second[None], last=False, **settings
        )
        return part(
            side, remote, table, degree, mine_next, other_next, partial, last=True, **settings
        )
    pooled = local_streamed(local, hidden, group=512)
    mean = remote_streamed(remote, table, pooled, degree, relations=relations, group=512)
    return dense(side, mean, hidden, mine_next, other_next, bias_second[None])


def solution(mesh):
    placed = (
        P("dom", None),
        P("dom", None, None),
        P("dom", None, None),
        P("dom", None, None),
        P("dom"),
        P("dom", None, None),
        P(None, "dom", None),
        P("dom", None),
        P(),
        P(),
        P(None, "dom", None),
        P("dom", None),
        P(),
        P(),
    )
    return jax.shard_map(
        shards, mesh=mesh, in_specs=placed, out_specs=P("dom", None), check_vma=False
    )
```

```python
import functools

import jax
import jax.numpy as jnp
from jax import lax
from jax.experimental import pallas as pl
from jax.experimental.pallas import tpu as pltpu
from jax.sharding import PartitionSpec as P

WIN = 16
CHUNK = 512
GROUP = 8
MIB = 1 << 20
WHOLE_MAX = 36 * MIB
CONTRACT_LANES = (((1,), (1,)), ((), ()))


def estimate(flops, nbytes):
    return pl.CostEstimate(flops=int(flops), bytes_accessed=int(nbytes), transcendentals=0)


def params(mib, **more):
    return pltpu.CompilerParams(vmem_limit_bytes=mib * MIB, **more)


def hot(rows, lanes):
    row_ids = lax.broadcasted_iota(jnp.int32, (rows, lanes.shape[1]), 0)
    return jnp.where(row_ids == lanes, 1.0, 0.0)


def code_edges(source_ref, relation_ref, target_ref, slot_ref, code_ref, low_ref, relations):
    slot = relation_ref[...] * WIN + (target_ref[...] & (WIN - 1))
    slot_ref[...] = slot
    code_ref[...] = (source_ref[...] // CHUNK) * (WIN * relations) + slot
    low_ref[...] = source_ref[...] & (CHUNK - 1)


def link_blocks(tile_ref, count_ref, head_ref, next_ref, tiles):
    def clear(t, carry):
        head_ref[t] = -1
        return carry

    lax.fori_loop(0, tiles, clear, 0)

    def link(b, carry):
        t = tile_ref[b] // WIN
        next_ref[b] = head_ref[t]
        head_ref[t] = b
        return carry

    lax.fori_loop(0, count_ref[0], link, 0)


def pair_of(first, next_ref):
    second = jnp.where(first >= 0, next_ref[jnp.maximum(first, 0)], -1)
    after = jnp.where(second >= 0, next_ref[jnp.maximum(second, 0)], -1)
    return second, after


def pair_rows(ref, first, second):
    one = jnp.where(first >= 0, ref[pl.ds(jnp.maximum(first, 0), 1), :], -1)
    two = jnp.where(second >= 0, ref[pl.ds(jnp.maximum(second, 0), 1), :], -1)
    return jnp.concatenate([one, two], axis=1)


def pair_counts(first, second, slot_ref, code_ref, low_ref, rows, slots):
    left = hot(rows, pair_rows(code_ref, first, second)).astype(jnp.bfloat16)
    right = hot(CHUNK, pair_rows(low_ref, first, second)).astype(jnp.bfloat16)
    counts = lax.dot_general(left, right, CONTRACT_LANES, preferred_element_type=jnp.float32)
    degree = jnp.sum(hot(slots, pair_rows(slot_ref, first, second)), axis=1, keepdims=True)
    return counts, degree


def put_counts(counts, local_ref, remote_ref, row, slots, locals_):
    for piece in range(counts.shape[0] // slots):
        part = counts[piece * slots : (piece + 1) * slots].astype(jnp.bfloat16)
        if piece < locals_:
            local_ref[pl.ds(row, slots), pl.ds(piece * CHUNK, CHUNK)] = part
        else:
            remote_ref[pl.ds(row, slots), pl.ds((piece - locals_) * CHUNK, CHUNK)] = part


def build_streamed(
    tile_ref, count_ref, source_ref, relation_ref, target_ref,
    local_ref, remote_ref, degree_ref,
    head_ref, next_ref, slot_ref, code_ref, low_ref, sum_ref,
    *, tiles, relations, locals_, pieces,
):
    slots = WIN * relations
    rows = pieces * slots
    t = pl.program_id(0)

    @pl.when(t == 0)
    def _():
        code_edges(source_ref, relation_ref, target_ref, slot_ref, code_ref, low_ref, relations)
        link_blocks(tile_ref, count_ref, head_ref, next_ref, tiles)

    sum_ref[...] = jnp.zeros_like(sum_ref)
    degree_ref[...] = jnp.zeros_like(degree_ref)

    def step(first):
        second, after = pair_of(first, next_ref)
        counts, degree = pair_counts(first, second, slot_ref, code_ref, low_ref, rows, slots)
        sum_ref[...] += counts
        degree_ref[...] += degree
        return after

    lax.while_loop(lambda first: first >= 0, step, head_ref[t])
    put_counts(sum_ref[...], local_ref, remote_ref, 0, slots, locals_)


def build_streamed_call(tile_of, count, source, relation, target, *, node_rows, relations, remote_rows):
    blocks, width = source.shape
    tiles, slots = node_rows // WIN, WIN * relations
    locals_, remotes = node_rows // CHUNK, remote_rows // CHUNK
    pieces = locals_ + remotes
    smem = pl.BlockSpec(memory_space=pltpu.SMEM)
    shapes = [
        ((tiles * slots, node_rows), jnp.bfloat16),
        ((tiles * slots, remote_rows), jnp.bfloat16),
        ((tiles * slots, 1), jnp.float32),
    ]
    whole = pl.BlockSpec((blocks, width), lambda t: (0, 0))
    return pl.pallas_call(
        functools.partial(
            build_streamed, tiles=tiles, relations=relations, locals_=locals_, pieces=pieces
        ),
        grid=(tiles,),
        out_shape=[jax.ShapeDtypeStruct(s, d) for s, d in shapes],
        in_specs=[smem, smem, whole, whole, whole],
        out_specs=[pl.BlockSpec((slots, s[1]), lambda t: (t, 0)) for s, _ in shapes],
        scratch_shapes=[
            pltpu.SMEM((tiles,), jnp.int32),
            pltpu.SMEM((blocks,), jnp.int32),
            pltpu.VMEM((blocks, width), jnp.int32),
            pltpu.VMEM((blocks, width), jnp.int32),
            pltpu.VMEM((blocks, width), jnp.int32),
            pltpu.VMEM((pieces * slots, CHUNK), jnp.float32),
        ],
        compiler_params=params(40),
        cost_estimate=estimate(
            4 * (tiles + blocks // 4) * pieces * slots * CHUNK * width,
            2 * tiles * slots * pieces * CHUNK,
        ),
        name="build",
    )(tile_of, count, source, relation, target)


def local_streamed_body(counts_ref, table_ref, pooled_ref):
    pooled_ref[...] = jnp.dot(
        counts_ref[...], table_ref[...], preferred_element_type=jnp.float32
    )


def local_streamed(counts, table, *, group):
    rows, depth = counts.shape
    width = table.shape[1]
    return pl.pallas_call(
        local_streamed_body,
        grid=(rows // group,),
        out_shape=jax.ShapeDtypeStruct((rows, width), jnp.float32),
        in_specs=[
            pl.BlockSpec((group, depth), lambda i: (i, 0)),
            pl.BlockSpec((depth, width), lambda i: (0, 0)),
        ],
        out_specs=pl.BlockSpec((group, width), lambda i: (i, 0)),
        compiler_params=params(40),
        cost_estimate=estimate(2 * rows * depth * width, 2 * rows * depth),
        name="local",
    )(counts, table)


def put_means(mean, mean_ref, first_tile, relations):
    slots = WIN * relations
    width = mean.shape[1]
    for tile in range(mean.shape[0] // slots):
        at = pl.multiple_of((first_tile + tile) * WIN, WIN)
        for relation in range(relations):
            start = tile * slots + relation * WIN
            mean_ref[pl.ds(at, WIN), pl.ds(relation * width, width)] = mean[start : start + WIN]


def remote_streamed_body(counts_ref, table_ref, pooled_ref, degree_ref, mean_ref, *, relations):
    total = pooled_ref[...] + jnp.dot(
        counts_ref[...], table_ref[...], preferred_element_type=jnp.float32
    )
    mean = total * (1.0 / jnp.maximum(degree_ref[...], 1.0))
    put_means(mean.astype(jnp.bfloat16), mean_ref, 0, relations)


def remote_streamed(counts, table, pooled, degree, *, relations, group):
    rows, depth = counts.shape
    width = table.shape[1]
    return pl.pallas_call(
        functools.partial(remote_streamed_body, relations=relations),
        grid=(rows // group,),
        out_shape=jax.ShapeDtypeStruct((rows // relations, relations * width), jnp.bfloat16),
        in_specs=[
            pl.BlockSpec((group, depth), lambda i: (i, 0)),
            pl.BlockSpec((depth, width), lambda i: (0, 0)),
            pl.BlockSpec((group, width), lambda i: (i, 0)),
            pl.BlockSpec((group, 1), lambda i: (i, 0)),
        ],
        out_specs=pl.BlockSpec((group // relations, relations * width), lambda i: (i, 0)),
        compiler_params=params(40),
        cost_estimate=estimate(2 * rows * depth * width, 2 * rows * depth),
        name="remote",
    )(counts, table, pooled, degree)


def build_body(
    tile_ref, count_ref, source_ref, relation_ref, target_ref, own_ref,
    local_ref, remote_ref, pooled_ref, degree_ref,
    local_v, remote_v, pooled_v, head_ref, next_ref, list_ref, slot_ref, code_ref, low_ref, sum_ref,
    sems, *, tiles, relations, locals_, pieces,
):
    slots = WIN * relations
    rows = pieces * slots
    code_edges(source_ref, relation_ref, target_ref, slot_ref, code_ref, low_ref, relations)
    link_blocks(tile_ref, count_ref, head_ref, next_ref, tiles)
    head_ref[tiles] = -1
    counted = functools.partial(
        pair_counts, slot_ref=slot_ref, code_ref=code_ref, low_ref=low_ref, rows=rows, slots=slots
    )

    def place(t, piece):
        row = pl.multiple_of(t * slots, slots)
        ref, at = (local_v, piece) if piece < locals_ else (remote_v, piece - locals_)
        return ref, (pl.ds(row, slots), pl.ds(at * CHUNK, CHUNK))

    def part(counts, piece):
        return counts[piece * slots : (piece + 1) * slots]

    def add_degree(i, u, degree):
        lanes = lax.broadcasted_iota(jnp.int32, (slots, GROUP), 1)
        degree_ref[i] += jnp.where(lanes == u, degree, 0.0)

    def group(i, carry):
        for u in range(GROUP):
            t = i * GROUP + u
            first = head_ref[t]
            second, after = pair_of(first, next_ref)
            counts, degree = counted(first, second)
            for piece in range(pieces):
                ref, where = place(t, piece)
                ref[where] = part(counts, piece).astype(jnp.bfloat16)
            degree_ref[i, :, pl.ds(u, 1)] = degree
            head_ref[t] = after

        short = jnp.int32(0)
        for u in range(GROUP):
            t = i * GROUP + u
            first = head_ref[t]
            _, after = pair_of(first, next_ref)
            list_ref[short] = t
            short += jnp.where((first >= 0) & (after < 0), 1, 0)
        list_ref[short] = tiles

        def add_two(j, carry):
            for k in range(2):
                t = list_ref[2 * j + k]
                first = head_ref[t]
                second, _ = pair_of(first, next_ref)
                counts, degree = counted(first, second)
                for piece in range(pieces):
                    ref, where = place(t, piece)
                    total = ref[where].astype(jnp.float32) + part(counts, piece)
                    ref[where] = total.astype(jnp.bfloat16)
                add_degree(i, t - i * GROUP, degree)
            return carry

        lax.fori_loop(0, (short + 1) // 2, add_two, 0)

        def long(u, carry):
            t = i * GROUP + u
            first = head_ref[t]
            _, after = pair_of(first, next_ref)

            @pl.when(after >= 0)
            def _():
                for piece in range(pieces):
                    ref, where = place(t, piece)
                    sum_ref[pl.ds(piece * slots, slots), :] = ref[where].astype(jnp.float32)

                def step(first):
                    second, after = pair_of(first, next_ref)
                    counts, degree = counted(first, second)
                    sum_ref[...] += counts
                    add_degree(i, u, degree)
                    return after

                lax.while_loop(lambda first: first >= 0, step, first)
                for piece in range(pieces):
                    ref, where = place(t, piece)
                    ref[where] = sum_ref[pl.ds(piece * slots, slots), :].astype(jnp.bfloat16)

            return carry

        lax.fori_loop(0, GROUP, long, 0)
        some = pl.ds(pl.multiple_of(i * GROUP * slots, GROUP * slots), GROUP * slots)
        pooled_v[some, :] = jnp.dot(
            local_v[some, :], own_ref[...], preferred_element_type=jnp.float32
        )
        pltpu.make_async_copy(local_v.at[some], local_ref.at[some], sems.at[0]).start()
        pltpu.make_async_copy(remote_v.at[some], remote_ref.at[some], sems.at[1]).start()
        pltpu.make_async_copy(pooled_v.at[some], pooled_ref.at[some], sems.at[2]).start()
        return carry

    lax.fori_loop(0, tiles // GROUP, group, 0)
    every = pl.ds(0, tiles * slots)
    pltpu.make_async_copy(local_v.at[every], local_ref, sems.at[0]).wait()
    pltpu.make_async_copy(remote_v.at[every], remote_ref, sems.at[1]).wait()
    pltpu.make_async_copy(pooled_v, pooled_ref, sems.at[2]).wait()


def build(tile_of, count, source, relation, target, own, *, relations, remote_rows):
    blocks, block_width = source.shape
    node_rows, width = own.shape
    tiles, slots = node_rows // WIN, WIN * relations
    rows = tiles * slots
    locals_, remotes = node_rows // CHUNK, remote_rows // CHUNK
    pieces = locals_ + remotes
    vmem = pl.BlockSpec(memory_space=pltpu.VMEM)
    smem = pl.BlockSpec(memory_space=pltpu.SMEM)
    hbm = pl.BlockSpec(memory_space=pltpu.HBM)
    return pl.pallas_call(
        functools.partial(
            build_body, tiles=tiles, relations=relations, locals_=locals_, pieces=pieces
        ),
        out_shape=[
            jax.ShapeDtypeStruct((rows, node_rows), jnp.bfloat16),
            jax.ShapeDtypeStruct((rows, remote_rows), jnp.bfloat16),
            jax.ShapeDtypeStruct((rows, width), jnp.float32),
            jax.ShapeDtypeStruct((tiles // GROUP, slots, GROUP), jnp.float32),
        ],
        in_specs=[smem, smem, vmem, vmem, vmem, vmem],
        out_specs=[hbm, hbm, hbm, vmem],
        scratch_shapes=[
            pltpu.VMEM((rows + slots, node_rows), jnp.bfloat16),
            pltpu.VMEM((rows + slots, remote_rows), jnp.bfloat16),
            pltpu.VMEM((rows, width), jnp.float32),
            pltpu.SMEM((tiles + 1,), jnp.int32),
            pltpu.SMEM((blocks,), jnp.int32),
            pltpu.SMEM((GROUP + 1,), jnp.int32),
            pltpu.VMEM((blocks, block_width), jnp.int32),
            pltpu.VMEM((blocks, block_width), jnp.int32),
            pltpu.VMEM((blocks, block_width), jnp.int32),
            pltpu.VMEM((pieces * slots, CHUNK), jnp.float32),
            pltpu.SemaphoreType.DMA((3,)),
        ],
        compiler_params=params(58),
        cost_estimate=estimate(
            4 * (tiles + blocks // 4) * pieces * slots * CHUNK * block_width
            + 2 * rows * node_rows * width,
            2 * rows * pieces * CHUNK,
        ),
        name="build",
    )(tile_of, count, source, relation, target, own)


def pool_groups(
    counts_ref, counts_v, sems, table_ref, degree_ref, mean_ref, relations, ready=None, extra=None
):
    size = GROUP * WIN * relations
    groups = counts_ref.shape[0] // size

    def copies(i):
        some = pl.ds(pl.multiple_of(i * size, size), size)
        found = [pltpu.make_async_copy(counts_ref.at[some], counts_v.at[some], sems.at[0, i])]
        if extra is not None:
            found.append(pltpu.make_async_copy(extra[0].at[some], extra[1].at[some], sems.at[1, i]))
        return found

    def begin(i, carry):
        for copy in copies(i):
            copy.start()
        return carry

    def step(i, carry):
        for copy in copies(i):
            copy.wait()
        some = pl.ds(pl.multiple_of(i * size, size), size)
        total = jnp.dot(counts_v[some, :], table_ref[...], preferred_element_type=jnp.float32)
        if extra is not None:
            total += extra[1][some, :]
        share = 1.0 / jnp.maximum(degree_ref[i], 1.0)
        slots = WIN * relations
        for u in range(GROUP):
            mean = total[u * slots : (u + 1) * slots] * share[:, u : u + 1]
            put_means(mean.astype(jnp.bfloat16), mean_ref, i * GROUP + u, relations)
        return carry

    lax.fori_loop(0, groups, begin, 0)
    if ready is not None:
        ready()
    lax.fori_loop(0, groups, step, 0)


def copy_table(incoming_ref, table_ref, slot):
    for device in range(incoming_ref.shape[0]):
        table_ref[device * slot : (device + 1) * slot, :] = incoming_ref[device, :slot, :]


def pool_body(
    counts_ref, pooled_ref, incoming_ref, degree_ref, mean_ref,
    counts_v, pooled_v, table_v, sems, *, relations, slot,
):
    def ready():
        copy_table(incoming_ref, table_v, slot)

    pool_groups(
        counts_ref, counts_v, sems, table_v, degree_ref, mean_ref, relations, ready,
        extra=(pooled_ref, pooled_v),
    )


def pool(counts, pooled, incoming, degree, *, relations, slot):
    rows, depth = counts.shape
    width = incoming.shape[2]
    vmem = pl.BlockSpec(memory_space=pltpu.VMEM)
    hbm = pl.BlockSpec(memory_space=pltpu.HBM)
    return pl.pallas_call(
        functools.partial(pool_body, relations=relations, slot=slot),
        out_shape=jax.ShapeDtypeStruct((rows // relations, relations * width), jnp.bfloat16),
        in_specs=[hbm, hbm, vmem, vmem],
        out_specs=vmem,
        scratch_shapes=[
            pltpu.VMEM(counts.shape, counts.dtype),
            pltpu.VMEM(pooled.shape, pooled.dtype),
            pltpu.VMEM((depth, width), jnp.bfloat16),
            pltpu.SemaphoreType.DMA((2, degree.shape[0])),
        ],
        compiler_params=params(44),
        cost_estimate=estimate(2 * rows * depth * width, 2 * rows * depth),
        name="pool",
    )(counts, pooled, incoming, degree)


def pick_rows(send_ref, rows_ref, emit):
    devices, slot = send_ref.shape
    depth = rows_ref.shape[0]
    columns = send_ref[...].astype(jnp.float32).T.astype(jnp.int32)
    lanes = lax.broadcasted_iota(jnp.int32, (slot, depth), 1)
    step = 8
    for start in range(0, devices, step):
        chosen = jnp.concatenate(
            [
                jnp.where(columns[:, device : device + 1] == lanes, 1.0, 0.0).astype(jnp.bfloat16)
                for device in range(start, start + step)
            ],
            axis=0,
        )
        picked = jnp.dot(chosen, rows_ref[...], preferred_element_type=jnp.float32)
        for k in range(step):
            emit(start + k, picked[k * slot : (k + 1) * slot].astype(jnp.bfloat16))


def middle_body(
    side_ref, mean_ref, own_ref, incoming_ref, swapped_ref, bias_ref, send_ref,
    hidden_ref, out_ref, self_ref, weights_v, *, relations, slot,
):
    width = own_ref.shape[1]
    half = relations // 2
    devices = incoming_ref.shape[0]
    piece = width // devices
    block = (half + 1) * width
    for device in range(devices):
        for m in range(half + 1):
            at = m * width + device * piece
            weights_v[at : at + piece, :] = incoming_ref[
                device, slot + m * piece : slot + (m + 1) * piece, :
            ]
            weights_v[block + at : block + at + piece, :] = swapped_ref[
                device, m * piece : (m + 1) * piece, :
            ]
    side = side_ref[0]
    mine_at = pl.multiple_of(side * (half * width), width)
    other_at = pl.multiple_of((1 - side) * (half * width), width)
    own_at = pl.multiple_of(half * width + side * block, width)
    next_at = pl.multiple_of(half * width + (1 - side) * block, width)
    self_ref[...] = weights_v[pl.ds(next_at, width), :]
    total = jnp.dot(
        mean_ref[:, pl.ds(mine_at, half * width)],
        weights_v[: half * width, :],
        preferred_element_type=jnp.float32,
    )
    total += jnp.dot(
        mean_ref[:, pl.ds(other_at, half * width)],
        weights_v[block : block + half * width, :],
        preferred_element_type=jnp.float32,
    )
    total += jnp.dot(
        own_ref[...], weights_v[pl.ds(own_at, width), :], preferred_element_type=jnp.float32
    )
    hidden_ref[...] = jnp.maximum(total + bias_ref[...], 0.0).astype(jnp.bfloat16)

    def emit(device, picked):
        out_ref[device, :, :] = picked

    pick_rows(send_ref, hidden_ref, emit)


def middle(side, mean, own, incoming, swapped, bias, send, *, relations):
    nodes, width = own.shape
    devices, slot = send.shape
    vmem = pl.BlockSpec(memory_space=pltpu.VMEM)
    smem = pl.BlockSpec(memory_space=pltpu.SMEM)
    return pl.pallas_call(
        functools.partial(middle_body, relations=relations, slot=slot),
        out_shape=[
            jax.ShapeDtypeStruct((nodes, width), jnp.bfloat16),
            jax.ShapeDtypeStruct((devices, slot, width), jnp.bfloat16),
            jax.ShapeDtypeStruct((width, width), jnp.bfloat16),
        ],
        in_specs=[smem] + [vmem] * 6,
        out_specs=[vmem] * 3,
        scratch_shapes=[pltpu.VMEM(((relations + 2) * width, width), jnp.bfloat16)],
        compiler_params=params(20),
        cost_estimate=estimate(2 * nodes * mean.shape[1] * width, 0),
        name="middle",
    )(side, mean, own, incoming, swapped, bias, send)


def first_body(
    class_ref, counts_ref, own_ref, degree_ref, self_ref, bias_ref, *refs, relations
):
    pieces, (out_ref, weights_ref, counts_v, mean_v, sems) = refs[:relations], refs[relations:]
    width = own_ref.shape[1]

    def ready():
        for k, piece in enumerate(pieces):
            at = pl.multiple_of((class_ref[0] ^ k) * width, width)
            weights_ref[pl.ds(at, width), :] = piece[...]

    pool_groups(counts_ref, counts_v, sems, own_ref, degree_ref, mean_v, relations, ready)
    total = jnp.dot(mean_v[...], weights_ref[...], preferred_element_type=jnp.float32)
    total += jnp.dot(own_ref[...], self_ref[...], preferred_element_type=jnp.float32)
    out_ref[...] = total + bias_ref[...]


def first(class_, counts, own, degree, self_weight, bias, pieces, *, relations):
    rows, depth = counts.shape
    nodes, width = own.shape
    vmem = pl.BlockSpec(memory_space=pltpu.VMEM)
    smem = pl.BlockSpec(memory_space=pltpu.SMEM)
    hbm = pl.BlockSpec(memory_space=pltpu.HBM)
    return pl.pallas_call(
        functools.partial(first_body, relations=relations),
        out_shape=[
            jax.ShapeDtypeStruct((nodes, width), jnp.float32),
            jax.ShapeDtypeStruct((relations * width, width), jnp.bfloat16),
        ],
        in_specs=[smem, hbm] + [vmem] * (4 + relations),
        out_specs=[vmem, vmem],
        scratch_shapes=[
            pltpu.VMEM(counts.shape, counts.dtype),
            pltpu.VMEM((nodes, relations * width), jnp.bfloat16),
            pltpu.SemaphoreType.DMA((1, degree.shape[0])),
        ],
        compiler_params=params(44),
        cost_estimate=estimate(
            2 * rows * depth * width + 2 * nodes * relations * width * width, 2 * rows * depth
        ),
        name="first",
    )(class_, counts, own, degree, self_weight, bias, *pieces)


def last_body(
    counts_ref, table_ref, degree_ref, weights_ref, partial_ref, out_ref,
    counts_v, mean_v, sems, *, relations,
):
    pool_groups(counts_ref, counts_v, sems, table_ref, degree_ref, mean_v, relations)
    total = jnp.dot(mean_v[...], weights_ref[...], preferred_element_type=jnp.float32)
    out_ref[...] = (total + partial_ref[...]).astype(out_ref.dtype)


def last(counts, table, degree, weights, partial, *, relations):
    rows, depth = counts.shape
    width = table.shape[1]
    nodes = rows // relations
    vmem = pl.BlockSpec(memory_space=pltpu.VMEM)
    hbm = pl.BlockSpec(memory_space=pltpu.HBM)
    return pl.pallas_call(
        functools.partial(last_body, relations=relations),
        out_shape=jax.ShapeDtypeStruct((nodes, width), jnp.bfloat16),
        in_specs=[hbm] + [vmem] * 4,
        out_specs=vmem,
        scratch_shapes=[
            pltpu.VMEM(counts.shape, counts.dtype),
            pltpu.VMEM((nodes, relations * width), jnp.bfloat16),
            pltpu.SemaphoreType.DMA((1, degree.shape[0])),
        ],
        compiler_params=params(44),
        cost_estimate=estimate(
            2 * rows * depth * width + 2 * nodes * relations * width * width, 2 * rows * depth
        ),
        name="last",
    )(counts, table, degree, weights, partial)


def pack_body(
    coef_first_ref, coef_second_ref, features_ref, send_ref, bases_first_ref, self_first_ref,
    bases_second_ref, self_second_ref, out_ref,
):
    relations, bases = coef_first_ref.shape
    devices, slot = send_ref.shape
    piece = self_first_ref.shape[0]
    half = relations // 2

    def mix(coef_ref, bases_ref):
        mixed = []
        for relation in range(relations):
            total = coef_ref[relation, 0] * bases_ref[0].astype(jnp.float32)
            for base in range(1, bases):
                total += coef_ref[relation, base] * bases_ref[base].astype(jnp.float32)
            mixed.append(total.astype(jnp.bfloat16))
        return mixed

    first = mix(coef_first_ref, bases_first_ref)
    second = mix(coef_second_ref, bases_second_ref)
    own = [self_first_ref[...], self_second_ref[...]]
    for device in range(devices):
        side = device % 2
        rows = first[side * half : (side + 1) * half] + [own[side], second[device % relations]]
        for k, value in enumerate(rows):
            at = slot + k * piece
            out_ref[device, at : at + piece, :] = value

    def emit(device, picked):
        out_ref[device, :slot, :] = picked

    pick_rows(send_ref, features_ref, emit)


def pack(features, send, bases_first, self_first, coef_first, bases_second, self_second, coef_second):
    devices, slot = send.shape
    relations = coef_first.shape[0]
    piece, width = self_first.shape
    vmem = pl.BlockSpec(memory_space=pltpu.VMEM)
    smem = pl.BlockSpec(memory_space=pltpu.SMEM)
    return pl.pallas_call(
        pack_body,
        out_shape=jax.ShapeDtypeStruct(
            (devices, slot + (relations // 2 + 2) * piece, width), jnp.bfloat16
        ),
        in_specs=[smem, smem] + [vmem] * 6,
        out_specs=vmem,
        compiler_params=params(24),
        cost_estimate=estimate(2 * devices * slot * features.size, 0),
        name="pack",
    )(coef_first, coef_second, features, send, bases_first, self_first, bases_second, self_second)


def dense_body(mean_ref, own_ref, weights_ref, bias_ref, out_ref, *, last):
    depth = mean_ref.shape[1]
    total = jnp.dot(mean_ref[...], weights_ref[:depth], preferred_element_type=jnp.float32)
    total += jnp.dot(own_ref[...], weights_ref[depth:], preferred_element_type=jnp.float32)
    total += bias_ref[...]
    out_ref[...] = (total if last else jnp.maximum(total, 0.0)).astype(jnp.bfloat16)


def dense(mean, own, weights, bias, *, last):
    nodes, width = own.shape
    vmem = pl.BlockSpec(memory_space=pltpu.VMEM)
    return pl.pallas_call(
        functools.partial(dense_body, last=last),
        out_shape=jax.ShapeDtypeStruct((nodes, width), jnp.bfloat16),
        in_specs=[vmem] * 4,
        out_specs=vmem,
        compiler_params=params(16),
        cost_estimate=estimate(2 * nodes * mean.shape[1] * width, 0),
        name="dense",
    )(mean, own, weights, bias)


def mix_weights(bases, self_weight, coef):
    mixed = jnp.einsum(
        "rb,bij->rij", coef, bases.astype(jnp.float32), precision=lax.Precision.HIGHEST
    ).astype(jnp.bfloat16)
    return jnp.concatenate([mixed, self_weight[None]], axis=0)


def general_layers(
    features, edges, send, weights_first, weights_second, bias_first, bias_second, relations
):
    node_rows, width = features.shape
    devices, slot = send.shape
    half = relations // 2
    swap = [(i, i ^ 1) for i in range(devices)]
    side = lax.axis_index("dom") & 1

    def send_all(rows, weights):
        rows = rows[send]
        halves = [
            jnp.concatenate([weights[:half], weights[relations:]], axis=0).reshape(-1, width),
            jnp.concatenate([weights[half:relations], weights[relations:]], axis=0).reshape(-1, width),
        ]
        halves = jnp.broadcast_to(jnp.stack(halves)[None], (devices // 2, 2) + halves[0].shape)
        rows = jnp.concatenate([rows, halves.reshape(devices, -1, width)], axis=1)
        return lax.all_to_all(rows, "dom", split_axis=0, concat_axis=0, tiled=True)

    def take_all(incoming):
        mine = jnp.swapaxes(incoming[:, slot:].reshape(devices, half + 1, -1, width), 0, 1)
        mine = mine.reshape(-1, width)
        other = lax.ppermute(mine[: half * width], "dom", swap)
        mine, own = mine[: half * width], mine[half * width :]
        low, high = jnp.where(side == 0, mine, other), jnp.where(side == 0, other, mine)
        return incoming[:, :slot].reshape(-1, width), jnp.concatenate([low, high, own], axis=0)

    local, remote, degree = build_streamed_call(
        *edges, node_rows=node_rows, relations=relations, remote_rows=devices * slot
    )

    def layer(rows, weights, bias, last):
        incoming = send_all(rows, weights)
        pooled = local_streamed(local, rows, group=512)
        table, full = take_all(incoming)
        mean = remote_streamed(remote, table, pooled, degree, relations=relations, group=512)
        return dense(mean, rows, full, bias[None], last=last)

    hidden = layer(features, weights_first, bias_first, False)
    return layer(hidden, weights_second, bias_second, True)


def shards(
    features,
    edge_source,
    edge_relation,
    edge_target,
    block_count,
    send_list,
    bases_first,
    self_first,
    coef_first,
    bias_first,
    bases_second,
    self_second,
    coef_second,
    bias_second,
):
    node_rows, width = features.shape
    relations = coef_first.shape[0]
    devices, slot = send_list.shape[1:]
    remote_rows = devices * slot
    send = send_list[0]
    edges = (edge_target[0, :, 0], block_count, edge_source[0], edge_relation[0], edge_target[0])
    if 2 * node_rows * relations * (node_rows + remote_rows) > WHOLE_MAX:
        return general_layers(
            features,
            edges,
            send,
            mix_weights(bases_first, self_first, coef_first),
            mix_weights(bases_second, self_second, coef_second),
            bias_first,
            bias_second,
            relations,
        )
    here = lax.axis_index("dom").astype(jnp.int32).reshape(1)
    side, class_ = here & 1, here & (relations - 1)
    outgoing = pack(
        features, send, bases_first, self_first, coef_first, bases_second, self_second, coef_second
    )
    incoming = lax.all_to_all(outgoing, "dom", split_axis=0, concat_axis=0, tiled=True)
    local, remote, pooled, degree = build(
        *edges, features, relations=relations, remote_rows=remote_rows
    )
    incoming, degree = lax.optimization_barrier((incoming, degree))

    def from_peer(array, mask):
        return lax.ppermute(array, "dom", [(i, i ^ mask) for i in range(devices)])

    next_at = slot + (relations // 2 + 1) * self_first.shape[0]
    swapped = from_peer(incoming[:, slot:next_at], 1)
    pieces = {0: incoming[:, next_at:].reshape(width, width)}
    mask = relations // 2
    while mask:
        pieces.update({k | mask: from_peer(piece, mask) for k, piece in sorted(pieces.items())})
        mask //= 2
    pieces = [pieces[k] for k in range(relations)]
    mean = pool(remote, pooled, incoming, degree, relations=relations, slot=slot)
    hidden, picked, self_next = middle(
        side, mean, features, incoming, swapped, bias_first[None], send, relations=relations
    )
    table = lax.all_to_all(picked, "dom", split_axis=0, concat_axis=0, tiled=True)
    partial, weights = first(
        class_, local, hidden, degree, self_next, bias_second[None], pieces, relations=relations
    )
    table, partial = lax.optimization_barrier((table, partial))
    return last(
        remote, table.reshape(-1, width), degree, weights, partial, relations=relations
    )


def solution(mesh):
    placed = (
        P("dom", None),
        P("dom", None, None),
        P("dom", None, None),
        P("dom", None, None),
        P("dom"),
        P("dom", None, None),
        P(None, "dom", None),
        P("dom", None),
        P(),
        P(),
        P(None, "dom", None),
        P("dom", None),
        P(),
        P(),
    )
    return jax.shard_map(
        shards, mesh=mesh, in_specs=placed, out_specs=P("dom", None), check_vma=False
    )
```

```python
import functools

import jax
import jax.numpy as jnp
from jax import lax
from jax.experimental import pallas as pl
from jax.experimental.pallas import tpu as pltpu
from jax.sharding import PartitionSpec as P

WIN = 16
CHUNK = 512
GROUP = 8
MIB = 1 << 20
WHOLE_MAX = 36 * MIB
CONTRACT_LANES = (((1,), (1,)), ((), ()))


def estimate(flops, nbytes):
    return pl.CostEstimate(flops=int(flops), bytes_accessed=int(nbytes), transcendentals=0)


def params(mib, **more):
    return pltpu.CompilerParams(vmem_limit_bytes=mib * MIB, **more)


def hot(rows, lanes):
    row_ids = lax.broadcasted_iota(jnp.int32, (rows, lanes.shape[1]), 0)
    return jnp.where(row_ids == lanes, 1.0, 0.0)


def code_edges(source_ref, relation_ref, target_ref, slot_ref, code_ref, low_ref, relations):
    slot = relation_ref[...] * WIN + (target_ref[...] & (WIN - 1))
    slot_ref[...] = slot
    code_ref[...] = (source_ref[...] // CHUNK) * (WIN * relations) + slot
    low_ref[...] = source_ref[...] & (CHUNK - 1)


def link_blocks(tile_ref, count_ref, head_ref, next_ref, tiles):
    def clear(t, carry):
        head_ref[t] = -1
        return carry

    lax.fori_loop(0, tiles, clear, 0)

    def link(b, carry):
        t = tile_ref[b] // WIN
        next_ref[b] = head_ref[t]
        head_ref[t] = b
        return carry

    lax.fori_loop(0, count_ref[0], link, 0)


def pair_of(first, next_ref):
    second = jnp.where(first >= 0, next_ref[jnp.maximum(first, 0)], -1)
    after = jnp.where(second >= 0, next_ref[jnp.maximum(second, 0)], -1)
    return second, after


def pair_rows(ref, first, second):
    one = jnp.where(first >= 0, ref[pl.ds(jnp.maximum(first, 0), 1), :], -1)
    two = jnp.where(second >= 0, ref[pl.ds(jnp.maximum(second, 0), 1), :], -1)
    return jnp.concatenate([one, two], axis=1)


def pair_counts(first, second, slot_ref, code_ref, low_ref, rows, slots):
    left = hot(rows, pair_rows(code_ref, first, second)).astype(jnp.bfloat16)
    right = hot(CHUNK, pair_rows(low_ref, first, second)).astype(jnp.bfloat16)
    counts = lax.dot_general(left, right, CONTRACT_LANES, preferred_element_type=jnp.float32)
    degree = jnp.sum(hot(slots, pair_rows(slot_ref, first, second)), axis=1, keepdims=True)
    return counts, degree


def put_counts(counts, local_ref, remote_ref, row, slots, locals_):
    for piece in range(counts.shape[0] // slots):
        part = counts[piece * slots : (piece + 1) * slots].astype(jnp.bfloat16)
        if piece < locals_:
            local_ref[pl.ds(row, slots), pl.ds(piece * CHUNK, CHUNK)] = part
        else:
            remote_ref[pl.ds(row, slots), pl.ds((piece - locals_) * CHUNK, CHUNK)] = part


def build_streamed(
    tile_ref, count_ref, source_ref, relation_ref, target_ref,
    local_ref, remote_ref, degree_ref,
    head_ref, next_ref, slot_ref, code_ref, low_ref, sum_ref,
    *, tiles, relations, locals_, pieces,
):
    slots = WIN * relations
    rows = pieces * slots
    t = pl.program_id(0)

    @pl.when(t == 0)
    def _():
        code_edges(source_ref, relation_ref, target_ref, slot_ref, code_ref, low_ref, relations)
        link_blocks(tile_ref, count_ref, head_ref, next_ref, tiles)

    sum_ref[...] = jnp.zeros_like(sum_ref)
    degree_ref[...] = jnp.zeros_like(degree_ref)

    def step(first):
        second, after = pair_of(first, next_ref)
        counts, degree = pair_counts(first, second, slot_ref, code_ref, low_ref, rows, slots)
        sum_ref[...] += counts
        degree_ref[...] += degree
        return after

    lax.while_loop(lambda first: first >= 0, step, head_ref[t])
    put_counts(sum_ref[...], local_ref, remote_ref, 0, slots, locals_)


def build_streamed_call(tile_of, count, source, relation, target, *, node_rows, relations, remote_rows):
    blocks, width = source.shape
    tiles, slots = node_rows // WIN, WIN * relations
    locals_, remotes = node_rows // CHUNK, remote_rows // CHUNK
    pieces = locals_ + remotes
    smem = pl.BlockSpec(memory_space=pltpu.SMEM)
    shapes = [
        ((tiles * slots, node_rows), jnp.bfloat16),
        ((tiles * slots, remote_rows), jnp.bfloat16),
        ((tiles * slots, 1), jnp.float32),
    ]
    whole = pl.BlockSpec((blocks, width), lambda t: (0, 0))
    return pl.pallas_call(
        functools.partial(
            build_streamed, tiles=tiles, relations=relations, locals_=locals_, pieces=pieces
        ),
        grid=(tiles,),
        out_shape=[jax.ShapeDtypeStruct(s, d) for s, d in shapes],
        in_specs=[smem, smem, whole, whole, whole],
        out_specs=[pl.BlockSpec((slots, s[1]), lambda t: (t, 0)) for s, _ in shapes],
        scratch_shapes=[
            pltpu.SMEM((tiles,), jnp.int32),
            pltpu.SMEM((blocks,), jnp.int32),
            pltpu.VMEM((blocks, width), jnp.int32),
            pltpu.VMEM((blocks, width), jnp.int32),
            pltpu.VMEM((blocks, width), jnp.int32),
            pltpu.VMEM((pieces * slots, CHUNK), jnp.float32),
        ],
        compiler_params=params(40),
        cost_estimate=estimate(
            4 * (tiles + blocks // 4) * pieces * slots * CHUNK * width,
            2 * tiles * slots * pieces * CHUNK,
        ),
        name="build",
    )(tile_of, count, source, relation, target)


def local_streamed_body(counts_ref, table_ref, pooled_ref):
    pooled_ref[...] = jnp.dot(
        counts_ref[...], table_ref[...], preferred_element_type=jnp.float32
    )


def local_streamed(counts, table, *, group):
    rows, depth = counts.shape
    width = table.shape[1]
    return pl.pallas_call(
        local_streamed_body,
        grid=(rows // group,),
        out_shape=jax.ShapeDtypeStruct((rows, width), jnp.float32),
        in_specs=[
            pl.BlockSpec((group, depth), lambda i: (i, 0)),
            pl.BlockSpec((depth, width), lambda i: (0, 0)),
        ],
        out_specs=pl.BlockSpec((group, width), lambda i: (i, 0)),
        compiler_params=params(40),
        cost_estimate=estimate(2 * rows * depth * width, 2 * rows * depth),
        name="local",
    )(counts, table)


def put_means(mean, mean_ref, first_tile, relations):
    slots = WIN * relations
    width = mean.shape[1]
    for tile in range(mean.shape[0] // slots):
        at = pl.multiple_of((first_tile + tile) * WIN, WIN)
        for relation in range(relations):
            start = tile * slots + relation * WIN
            mean_ref[pl.ds(at, WIN), pl.ds(relation * width, width)] = mean[start : start + WIN]


def remote_streamed_body(counts_ref, table_ref, pooled_ref, degree_ref, mean_ref, *, relations):
    total = pooled_ref[...] + jnp.dot(
        counts_ref[...], table_ref[...], preferred_element_type=jnp.float32
    )
    mean = total * (1.0 / jnp.maximum(degree_ref[...], 1.0))
    put_means(mean.astype(jnp.bfloat16), mean_ref, 0, relations)


def remote_streamed(counts, table, pooled, degree, *, relations, group):
    rows, depth = counts.shape
    width = table.shape[1]
    return pl.pallas_call(
        functools.partial(remote_streamed_body, relations=relations),
        grid=(rows // group,),
        out_shape=jax.ShapeDtypeStruct((rows // relations, relations * width), jnp.bfloat16),
        in_specs=[
            pl.BlockSpec((group, depth), lambda i: (i, 0)),
            pl.BlockSpec((depth, width), lambda i: (0, 0)),
            pl.BlockSpec((group, width), lambda i: (i, 0)),
            pl.BlockSpec((group, 1), lambda i: (i, 0)),
        ],
        out_specs=pl.BlockSpec((group // relations, relations * width), lambda i: (i, 0)),
        compiler_params=params(40),
        cost_estimate=estimate(2 * rows * depth * width, 2 * rows * depth),
        name="remote",
    )(counts, table, pooled, degree)


def in_hbm(*arrays):
    return [pltpu.with_memory_space_constraint(array, pltpu.HBM) for array in arrays]


def start_all(sems, *pairs):
    copies = [pltpu.make_async_copy(a, b, sems.at[i]) for i, (a, b) in enumerate(pairs)]
    for copy in copies:
        copy.start()
    return copies


def wait_all(copies):
    for copy in copies:
        copy.wait()


def build_body(
    tile_ref, count_ref, source_hbm, relation_hbm, target_hbm, own_hbm,
    local_ref, remote_ref, pooled_ref, degree_hbm,
    source_ref, relation_ref, target_ref, own_ref, degree_ref,
    local_v, remote_v, pooled_v, head_ref, next_ref, list_ref, slot_ref, code_ref, low_ref, sum_ref,
    sems, in_sems, *, tiles, relations, locals_, pieces,
):
    slots = WIN * relations
    rows = pieces * slots
    inputs = start_all(
        in_sems,
        (source_hbm, source_ref),
        (relation_hbm, relation_ref),
        (target_hbm, target_ref),
        (own_hbm, own_ref),
    )
    wait_all(inputs)
    code_edges(source_ref, relation_ref, target_ref, slot_ref, code_ref, low_ref, relations)
    link_blocks(tile_ref, count_ref, head_ref, next_ref, tiles)
    head_ref[tiles] = -1
    counted = functools.partial(
        pair_counts, slot_ref=slot_ref, code_ref=code_ref, low_ref=low_ref, rows=rows, slots=slots
    )

    def place(t, piece):
        row = pl.multiple_of(t * slots, slots)
        ref, at = (local_v, piece) if piece < locals_ else (remote_v, piece - locals_)
        return ref, (pl.ds(row, slots), pl.ds(at * CHUNK, CHUNK))

    def part(counts, piece):
        return counts[piece * slots : (piece + 1) * slots]

    def add_degree(i, u, degree):
        lanes = lax.broadcasted_iota(jnp.int32, (slots, GROUP), 1)
        degree_ref[i] += jnp.where(lanes == u, degree, 0.0)

    def group(i, carry):
        for u in range(GROUP):
            t = i * GROUP + u
            first = head_ref[t]
            second, after = pair_of(first, next_ref)
            counts, degree = counted(first, second)
            for piece in range(pieces):
                ref, where = place(t, piece)
                ref[where] = part(counts, piece).astype(jnp.bfloat16)
            degree_ref[i, :, pl.ds(u, 1)] = degree
            head_ref[t] = after

        short = jnp.int32(0)
        for u in range(GROUP):
            t = i * GROUP + u
            first = head_ref[t]
            _, after = pair_of(first, next_ref)
            list_ref[short] = t
            short += jnp.where((first >= 0) & (after < 0), 1, 0)
        list_ref[short] = tiles

        def add_two(j, carry):
            for k in range(2):
                t = list_ref[2 * j + k]
                first = head_ref[t]
                second, _ = pair_of(first, next_ref)
                counts, degree = counted(first, second)
                for piece in range(pieces):
                    ref, where = place(t, piece)
                    total = ref[where].astype(jnp.float32) + part(counts, piece)
                    ref[where] = total.astype(jnp.bfloat16)
                add_degree(i, t - i * GROUP, degree)
            return carry

        lax.fori_loop(0, (short + 1) // 2, add_two, 0)

        def long(u, carry):
            t = i * GROUP + u
            first = head_ref[t]
            _, after = pair_of(first, next_ref)

            @pl.when(after >= 0)
            def _():
                for piece in range(pieces):
                    ref, where = place(t, piece)
                    sum_ref[pl.ds(piece * slots, slots), :] = ref[where].astype(jnp.float32)

                def step(first):
                    second, after = pair_of(first, next_ref)
                    counts, degree = counted(first, second)
                    sum_ref[...] += counts
                    add_degree(i, u, degree)
                    return after

                lax.while_loop(lambda first: first >= 0, step, first)
                for piece in range(pieces):
                    ref, where = place(t, piece)
                    ref[where] = sum_ref[pl.ds(piece * slots, slots), :].astype(jnp.bfloat16)

            return carry

        lax.fori_loop(0, GROUP, long, 0)
        some = pl.ds(pl.multiple_of(i * GROUP * slots, GROUP * slots), GROUP * slots)
        pooled_v[some, :] = jnp.dot(
            local_v[some, :], own_ref[...], preferred_element_type=jnp.float32
        )
        pltpu.make_async_copy(local_v.at[some], local_ref.at[some], sems.at[0]).start()
        pltpu.make_async_copy(remote_v.at[some], remote_ref.at[some], sems.at[1]).start()
        pltpu.make_async_copy(pooled_v.at[some], pooled_ref.at[some], sems.at[2]).start()
        return carry

    lax.fori_loop(0, tiles // GROUP, group, 0)
    every = pl.ds(0, tiles * slots)
    pltpu.make_async_copy(local_v.at[every], local_ref, sems.at[0]).wait()
    pltpu.make_async_copy(remote_v.at[every], remote_ref, sems.at[1]).wait()
    pltpu.make_async_copy(pooled_v, pooled_ref, sems.at[2]).wait()
    pltpu.sync_copy(degree_ref, degree_hbm)


def build(tile_of, count, source, relation, target, own, *, relations, remote_rows):
    blocks, block_width = source.shape
    node_rows, width = own.shape
    tiles, slots = node_rows // WIN, WIN * relations
    rows = tiles * slots
    locals_, remotes = node_rows // CHUNK, remote_rows // CHUNK
    pieces = locals_ + remotes
    vmem = pl.BlockSpec(memory_space=pltpu.VMEM)
    smem = pl.BlockSpec(memory_space=pltpu.SMEM)
    hbm = pl.BlockSpec(memory_space=pltpu.HBM)
    return pl.pallas_call(
        functools.partial(
            build_body, tiles=tiles, relations=relations, locals_=locals_, pieces=pieces
        ),
        out_shape=[
            pltpu.HBM((rows, node_rows), jnp.bfloat16),
            pltpu.HBM((rows, remote_rows), jnp.bfloat16),
            pltpu.HBM((rows, width), jnp.float32),
            pltpu.HBM((tiles // GROUP, slots, GROUP), jnp.float32),
        ],
        in_specs=[smem, smem] + [hbm] * 4,
        out_specs=[hbm] * 4,
        scratch_shapes=[
            pltpu.VMEM((blocks, block_width), jnp.int32),
            pltpu.VMEM((blocks, block_width), jnp.int32),
            pltpu.VMEM((blocks, block_width), jnp.int32),
            pltpu.VMEM((node_rows, width), jnp.bfloat16),
            pltpu.VMEM((tiles // GROUP, slots, GROUP), jnp.float32),
            pltpu.VMEM((rows + slots, node_rows), jnp.bfloat16),
            pltpu.VMEM((rows + slots, remote_rows), jnp.bfloat16),
            pltpu.VMEM((rows, width), jnp.float32),
            pltpu.SMEM((tiles + 1,), jnp.int32),
            pltpu.SMEM((blocks,), jnp.int32),
            pltpu.SMEM((GROUP + 1,), jnp.int32),
            pltpu.VMEM((blocks, block_width), jnp.int32),
            pltpu.VMEM((blocks, block_width), jnp.int32),
            pltpu.VMEM((blocks, block_width), jnp.int32),
            pltpu.VMEM((pieces * slots, CHUNK), jnp.float32),
            pltpu.SemaphoreType.DMA((3,)),
            pltpu.SemaphoreType.DMA((4,)),
        ],
        compiler_params=params(58),
        cost_estimate=estimate(
            4 * (tiles + blocks // 4) * pieces * slots * CHUNK * block_width
            + 2 * rows * node_rows * width,
            2 * rows * pieces * CHUNK,
        ),
        name="build",
    )(tile_of, count, *in_hbm(source, relation, target, own))


def pool_groups(
    counts_ref, counts_v, sems, table_ref, degree_ref, mean_ref, relations, ready=None, extra=None
):
    size = GROUP * WIN * relations
    groups = counts_ref.shape[0] // size

    def copies(i):
        some = pl.ds(pl.multiple_of(i * size, size), size)
        found = [pltpu.make_async_copy(counts_ref.at[some], counts_v.at[some], sems.at[0, i])]
        if extra is not None:
            found.append(pltpu.make_async_copy(extra[0].at[some], extra[1].at[some], sems.at[1, i]))
        return found

    def begin(i, carry):
        for copy in copies(i):
            copy.start()
        return carry

    def step(i, carry):
        for copy in copies(i):
            copy.wait()
        some = pl.ds(pl.multiple_of(i * size, size), size)
        total = jnp.dot(counts_v[some, :], table_ref[...], preferred_element_type=jnp.float32)
        if extra is not None:
            total += extra[1][some, :]
        share = 1.0 / jnp.maximum(degree_ref[i], 1.0)
        slots = WIN * relations
        for u in range(GROUP):
            mean = total[u * slots : (u + 1) * slots] * share[:, u : u + 1]
            put_means(mean.astype(jnp.bfloat16), mean_ref, i * GROUP + u, relations)
        return carry

    lax.fori_loop(0, groups, begin, 0)
    if ready is not None:
        ready()
    lax.fori_loop(0, groups, step, 0)


def copy_table(incoming_ref, table_ref, slot):
    for device in range(incoming_ref.shape[0]):
        table_ref[device * slot : (device + 1) * slot, :] = incoming_ref[device, :slot, :]


def pool_body(
    counts_ref, pooled_ref, incoming_ref, degree_hbm, mean_ref,
    counts_v, pooled_v, table_v, degree_v, sems, in_sems, *, relations, slot,
):
    inputs = start_all(in_sems, (degree_hbm, degree_v))

    def ready():
        copy_table(incoming_ref, table_v, slot)
        wait_all(inputs)

    pool_groups(
        counts_ref, counts_v, sems, table_v, degree_v, mean_ref, relations, ready,
        extra=(pooled_ref, pooled_v),
    )


def pool(counts, pooled, incoming, degree, *, relations, slot):
    rows, depth = counts.shape
    width = incoming.shape[2]
    vmem = pl.BlockSpec(memory_space=pltpu.VMEM)
    hbm = pl.BlockSpec(memory_space=pltpu.HBM)
    return pl.pallas_call(
        functools.partial(pool_body, relations=relations, slot=slot),
        out_shape=jax.ShapeDtypeStruct((rows // relations, relations * width), jnp.bfloat16),
        in_specs=[hbm, hbm, vmem, hbm],
        out_specs=vmem,
        scratch_shapes=[
            pltpu.VMEM(counts.shape, counts.dtype),
            pltpu.VMEM(pooled.shape, pooled.dtype),
            pltpu.VMEM((depth, width), jnp.bfloat16),
            pltpu.VMEM(degree.shape, degree.dtype),
            pltpu.SemaphoreType.DMA((2, degree.shape[0])),
            pltpu.SemaphoreType.DMA((1,)),
        ],
        compiler_params=params(44),
        cost_estimate=estimate(2 * rows * depth * width, 2 * rows * depth),
        name="pool",
    )(*in_hbm(counts, pooled), incoming, *in_hbm(degree))


def pick_rows(send_ref, rows_ref, emit, done):
    devices, slot = send_ref.shape
    depth = rows_ref.shape[0]
    columns = send_ref[...].astype(jnp.float32).T.astype(jnp.int32)
    lanes = lax.broadcasted_iota(jnp.int32, (slot, depth), 1)
    step = 8
    for start in range(0, devices, step):
        chosen = jnp.concatenate(
            [
                jnp.where(columns[:, device : device + 1] == lanes, 1.0, 0.0).astype(jnp.bfloat16)
                for device in range(start, start + step)
            ],
            axis=0,
        )
        picked = jnp.dot(chosen, rows_ref[...], preferred_element_type=jnp.float32)
        for k in range(step):
            emit(start + k, picked[k * slot : (k + 1) * slot].astype(jnp.bfloat16))
        done(start, step)


def send_out(out_v, out_ref, sems, start, count):
    some = pl.ds(start, count)
    pltpu.make_async_copy(out_v.at[some], out_ref.at[some], sems.at[0]).start()


def middle_body(
    mean_ref, own_hbm, incoming_ref, swapped_ref, bias_hbm, send_hbm,
    hidden_hbm, out_ref, self_hbm,
    own_v, bias_v, send_v, hidden_v, out_v, self_v, weights_v, sems, in_sems,
    *, relations, slot,
):
    inputs = start_all(in_sems, (own_hbm, own_v), (bias_hbm, bias_v), (send_hbm, send_v))
    width = own_v.shape[1]
    half = relations // 2
    devices = incoming_ref.shape[0]
    piece = width // devices
    block = (half + 1) * width
    for device in range(devices):
        for m in range(half + 1):
            at = m * width + device * piece
            weights_v[at : at + piece, :] = incoming_ref[
                device, slot + m * piece : slot + (m + 1) * piece, :
            ]
            weights_v[block + at : block + at + piece, :] = swapped_ref[
                device, m * piece : (m + 1) * piece, :
            ]
    side = lax.axis_index("dom") & 1
    mine_at = pl.multiple_of(side * (half * width), width)
    other_at = pl.multiple_of((1 - side) * (half * width), width)
    own_at = pl.multiple_of(half * width + side * block, width)
    next_at = pl.multiple_of(half * width + (1 - side) * block, width)
    self_v[...] = weights_v[pl.ds(next_at, width), :]
    total = jnp.dot(
        mean_ref[:, pl.ds(mine_at, half * width)],
        weights_v[: half * width, :],
        preferred_element_type=jnp.float32,
    )
    total += jnp.dot(
        mean_ref[:, pl.ds(other_at, half * width)],
        weights_v[block : block + half * width, :],
        preferred_element_type=jnp.float32,
    )
    wait_all(inputs)
    total += jnp.dot(
        own_v[...], weights_v[pl.ds(own_at, width), :], preferred_element_type=jnp.float32
    )
    hidden_v[...] = jnp.maximum(total + bias_v[...], 0.0).astype(jnp.bfloat16)
    outputs = [
        pltpu.make_async_copy(hidden_v, hidden_hbm, sems.at[1]),
        pltpu.make_async_copy(self_v, self_hbm, sems.at[2]),
    ]
    for copy in outputs:
        copy.start()

    def emit(device, picked):
        out_v[device, :, :] = picked

    pick_rows(send_v, hidden_v, emit, functools.partial(send_out, out_v, out_ref, sems))
    pltpu.make_async_copy(out_v, out_ref, sems.at[0]).wait()
    wait_all(outputs)


def middle(mean, own, incoming, swapped, bias, send, *, relations):
    nodes, width = own.shape
    devices, slot = send.shape
    vmem = pl.BlockSpec(memory_space=pltpu.VMEM)
    hbm = pl.BlockSpec(memory_space=pltpu.HBM)
    return pl.pallas_call(
        functools.partial(middle_body, relations=relations, slot=slot),
        out_shape=[
            pltpu.HBM((nodes, width), jnp.bfloat16),
            pltpu.HBM((devices, slot, width), jnp.bfloat16),
            pltpu.HBM((width, width), jnp.bfloat16),
        ],
        in_specs=[vmem, hbm, vmem, vmem, hbm, hbm],
        out_specs=[hbm] * 3,
        scratch_shapes=[
            pltpu.VMEM(own.shape, own.dtype),
            pltpu.VMEM(bias.shape, bias.dtype),
            pltpu.VMEM(send.shape, send.dtype),
            pltpu.VMEM((nodes, width), jnp.bfloat16),
            pltpu.VMEM((devices, slot, width), jnp.bfloat16),
            pltpu.VMEM((width, width), jnp.bfloat16),
            pltpu.VMEM(((relations + 2) * width, width), jnp.bfloat16),
            pltpu.SemaphoreType.DMA((3,)),
            pltpu.SemaphoreType.DMA((3,)),
        ],
        compiler_params=params(24),
        cost_estimate=estimate(2 * nodes * mean.shape[1] * width, 0),
        name="middle",
    )(mean, *in_hbm(own), incoming, swapped, *in_hbm(bias, send))


def weight_copies(pieces, weights_v, relations):
    width = weights_v.shape[1]
    class_ = lax.axis_index("dom") & (relations - 1)
    return [
        (piece, weights_v.at[pl.ds(pl.multiple_of((class_ ^ k) * width, width), width)])
        for k, piece in enumerate(pieces)
    ]


def first_body(
    counts_ref, own_hbm, degree_hbm, self_hbm, bias_hbm, *refs, relations
):
    pieces, refs = refs[:relations], refs[relations:]
    out_hbm, own_v, degree_v, self_v, bias_v, out_v, weights_v, counts_v, mean_v, sems, in_sems = refs
    inputs = start_all(
        in_sems,
        (own_hbm, own_v),
        (degree_hbm, degree_v),
        (self_hbm, self_v),
        (bias_hbm, bias_v),
        *weight_copies(pieces, weights_v, relations),
    )
    pool_groups(
        counts_ref, counts_v, sems, own_v, degree_v, mean_v, relations, lambda: wait_all(inputs)
    )
    total = jnp.dot(mean_v[...], weights_v[...], preferred_element_type=jnp.float32)
    total += jnp.dot(own_v[...], self_v[...], preferred_element_type=jnp.float32)
    out_v[...] = total + bias_v[...]
    pltpu.sync_copy(out_v, out_hbm)


def first(counts, own, degree, self_weight, bias, pieces, *, relations):
    rows, depth = counts.shape
    nodes, width = own.shape
    hbm = pl.BlockSpec(memory_space=pltpu.HBM)
    return pl.pallas_call(
        functools.partial(first_body, relations=relations),
        out_shape=pltpu.HBM((nodes, width), jnp.float32),
        in_specs=[hbm] * (5 + relations),
        out_specs=hbm,
        scratch_shapes=[
            pltpu.VMEM(own.shape, own.dtype),
            pltpu.VMEM(degree.shape, degree.dtype),
            pltpu.VMEM(self_weight.shape, self_weight.dtype),
            pltpu.VMEM(bias.shape, bias.dtype),
            pltpu.VMEM((nodes, width), jnp.float32),
            pltpu.VMEM((relations * width, width), jnp.bfloat16),
            pltpu.VMEM(counts.shape, counts.dtype),
            pltpu.VMEM((nodes, relations * width), jnp.bfloat16),
            pltpu.SemaphoreType.DMA((1, degree.shape[0])),
            pltpu.SemaphoreType.DMA((4 + relations,)),
        ],
        compiler_params=params(44),
        cost_estimate=estimate(
            2 * rows * depth * width + 2 * nodes * relations * width * width, 2 * rows * depth
        ),
        name="first",
    )(*in_hbm(counts, own, degree, self_weight, bias, *pieces))


def last_body(counts_ref, table_ref, degree_hbm, partial_hbm, *refs, relations):
    pieces, refs = refs[:relations], refs[relations:]
    out_ref, degree_v, partial_v, weights_v, counts_v, mean_v, sems, in_sems = refs
    inputs = start_all(
        in_sems,
        (degree_hbm, degree_v),
        (partial_hbm, partial_v),
        *weight_copies(pieces, weights_v, relations),
    )
    pool_groups(
        counts_ref, counts_v, sems, table_ref, degree_v, mean_v, relations, lambda: wait_all(inputs)
    )
    total = jnp.dot(mean_v[...], weights_v[...], preferred_element_type=jnp.float32)
    out_ref[...] = (total + partial_v[...]).astype(out_ref.dtype)


def last(counts, table, degree, partial, pieces, *, relations):
    rows, depth = counts.shape
    width = table.shape[1]
    nodes = rows // relations
    vmem = pl.BlockSpec(memory_space=pltpu.VMEM)
    hbm = pl.BlockSpec(memory_space=pltpu.HBM)
    return pl.pallas_call(
        functools.partial(last_body, relations=relations),
        out_shape=jax.ShapeDtypeStruct((nodes, width), jnp.bfloat16),
        in_specs=[hbm, vmem] + [hbm] * (2 + relations),
        out_specs=vmem,
        scratch_shapes=[
            pltpu.VMEM(degree.shape, degree.dtype),
            pltpu.VMEM(partial.shape, partial.dtype),
            pltpu.VMEM((relations * width, width), jnp.bfloat16),
            pltpu.VMEM(counts.shape, counts.dtype),
            pltpu.VMEM((nodes, relations * width), jnp.bfloat16),
            pltpu.SemaphoreType.DMA((1, degree.shape[0])),
            pltpu.SemaphoreType.DMA((2 + relations,)),
        ],
        compiler_params=params(44),
        cost_estimate=estimate(
            2 * rows * depth * width + 2 * nodes * relations * width * width, 2 * rows * depth
        ),
        name="last",
    )(*in_hbm(counts), table, *in_hbm(degree, partial, *pieces))


def pack_body(*refs):
    inputs_hbm, out_ref, inputs_v, (out_v, sems, in_sems) = refs[:8], refs[8], refs[9:17], refs[17:]
    inputs = start_all(in_sems, *zip(inputs_hbm, inputs_v))
    coef_first, coef_second, bases_first, bases_second, self_first, self_second, features, send = (
        inputs_v
    )
    relations, bases = coef_first.shape
    devices, slot = send.shape
    piece = self_first.shape[0]
    half = relations // 2
    wait_all(inputs)

    def mix(coef_ref, bases_ref):
        mixed = []
        for relation in range(relations):
            total = coef_ref[relation, 0] * bases_ref[0].astype(jnp.float32)
            for base in range(1, bases):
                total += coef_ref[relation, base] * bases_ref[base].astype(jnp.float32)
            mixed.append(total.astype(jnp.bfloat16))
        return mixed

    first = mix(coef_first, bases_first)
    second = mix(coef_second, bases_second)
    own = [self_first[...], self_second[...]]
    for device in range(devices):
        side = device % 2
        rows = first[side * half : (side + 1) * half] + [own[side], second[device % relations]]
        for k, value in enumerate(rows):
            at = slot + k * piece
            out_v[device, at : at + piece, :] = value

    def emit(device, picked):
        out_v[device, :slot, :] = picked

    pick_rows(send, features, emit, functools.partial(send_out, out_v, out_ref, sems))
    pltpu.make_async_copy(out_v, out_ref, sems.at[0]).wait()


def pack(features, send, bases_first, self_first, coef_first, bases_second, self_second, coef_second):
    devices, slot = send.shape
    relations = coef_first.shape[0]
    piece, width = self_first.shape
    hbm = pl.BlockSpec(memory_space=pltpu.HBM)
    shape = (devices, slot + (relations // 2 + 2) * piece, width)
    args = (
        coef_first, coef_second, bases_first, bases_second, self_first, self_second, features, send,
    )
    return pl.pallas_call(
        pack_body,
        out_shape=pltpu.HBM(shape, jnp.bfloat16),
        in_specs=[hbm] * 8,
        out_specs=hbm,
        scratch_shapes=[
            *[pltpu.SMEM(a.shape, a.dtype) for a in args[:2]],
            *[pltpu.VMEM(a.shape, a.dtype) for a in args[2:]],
            pltpu.VMEM(shape, jnp.bfloat16),
            pltpu.SemaphoreType.DMA((1,)),
            pltpu.SemaphoreType.DMA((8,)),
        ],
        compiler_params=params(24),
        cost_estimate=estimate(2 * devices * slot * features.size, 0),
        name="pack",
    )(*in_hbm(*args))


def dense_body(mean_ref, own_ref, weights_ref, bias_ref, out_ref, *, last):
    depth = mean_ref.shape[1]
    total = jnp.dot(mean_ref[...], weights_ref[:depth], preferred_element_type=jnp.float32)
    total += jnp.dot(own_ref[...], weights_ref[depth:], preferred_element_type=jnp.float32)
    total += bias_ref[...]
    out_ref[...] = (total if last else jnp.maximum(total, 0.0)).astype(jnp.bfloat16)


def dense(mean, own, weights, bias, *, last):
    nodes, width = own.shape
    vmem = pl.BlockSpec(memory_space=pltpu.VMEM)
    return pl.pallas_call(
        functools.partial(dense_body, last=last),
        out_shape=jax.ShapeDtypeStruct((nodes, width), jnp.bfloat16),
        in_specs=[vmem] * 4,
        out_specs=vmem,
        compiler_params=params(16),
        cost_estimate=estimate(2 * nodes * mean.shape[1] * width, 0),
        name="dense",
    )(mean, own, weights, bias)


def mix_weights(bases, self_weight, coef):
    mixed = jnp.einsum(
        "rb,bij->rij", coef, bases.astype(jnp.float32), precision=lax.Precision.HIGHEST
    ).astype(jnp.bfloat16)
    return jnp.concatenate([mixed, self_weight[None]], axis=0)


def general_layers(
    features, edges, send, weights_first, weights_second, bias_first, bias_second, relations
):
    node_rows, width = features.shape
    devices, slot = send.shape
    half = relations // 2
    swap = [(i, i ^ 1) for i in range(devices)]
    side = lax.axis_index("dom") & 1

    def send_all(rows, weights):
        rows = rows[send]
        halves = [
            jnp.concatenate([weights[:half], weights[relations:]], axis=0).reshape(-1, width),
            jnp.concatenate([weights[half:relations], weights[relations:]], axis=0).reshape(-1, width),
        ]
        halves = jnp.broadcast_to(jnp.stack(halves)[None], (devices // 2, 2) + halves[0].shape)
        rows = jnp.concatenate([rows, halves.reshape(devices, -1, width)], axis=1)
        return lax.all_to_all(rows, "dom", split_axis=0, concat_axis=0, tiled=True)

    def take_all(incoming):
        mine = jnp.swapaxes(incoming[:, slot:].reshape(devices, half + 1, -1, width), 0, 1)
        mine = mine.reshape(-1, width)
        other = lax.ppermute(mine[: half * width], "dom", swap)
        mine, own = mine[: half * width], mine[half * width :]
        low, high = jnp.where(side == 0, mine, other), jnp.where(side == 0, other, mine)
        return incoming[:, :slot].reshape(-1, width), jnp.concatenate([low, high, own], axis=0)

    local, remote, degree = build_streamed_call(
        *edges, node_rows=node_rows, relations=relations, remote_rows=devices * slot
    )

    def layer(rows, weights, bias, last):
        incoming = send_all(rows, weights)
        pooled = local_streamed(local, rows, group=512)
        table, full = take_all(incoming)
        mean = remote_streamed(remote, table, pooled, degree, relations=relations, group=512)
        return dense(mean, rows, full, bias[None], last=last)

    hidden = layer(features, weights_first, bias_first, False)
    return layer(hidden, weights_second, bias_second, True)


def shards(
    features,
    edge_source,
    edge_relation,
    edge_target,
    block_count,
    send_list,
    bases_first,
    self_first,
    coef_first,
    bias_first,
    bases_second,
    self_second,
    coef_second,
    bias_second,
):
    node_rows, width = features.shape
    relations = coef_first.shape[0]
    devices, slot = send_list.shape[1:]
    remote_rows = devices * slot
    send = send_list[0]
    edges = (edge_target[0, :, 0], block_count, edge_source[0], edge_relation[0], edge_target[0])
    if 2 * node_rows * relations * (node_rows + remote_rows) > WHOLE_MAX:
        return general_layers(
            features,
            edges,
            send,
            mix_weights(bases_first, self_first, coef_first),
            mix_weights(bases_second, self_second, coef_second),
            bias_first,
            bias_second,
            relations,
        )
    outgoing = pack(
        features, send, bases_first, self_first, coef_first, bases_second, self_second, coef_second
    )
    incoming = lax.all_to_all(outgoing, "dom", split_axis=0, concat_axis=0, tiled=True)
    local, remote, pooled, degree = build(
        *edges, features, relations=relations, remote_rows=remote_rows
    )
    incoming, degree = lax.optimization_barrier((incoming, degree))

    def from_peer(array, mask):
        return lax.ppermute(array, "dom", [(i, i ^ mask) for i in range(devices)])

    next_at = slot + (relations // 2 + 1) * self_first.shape[0]
    swapped = from_peer(incoming[:, slot:next_at], 1)
    pieces = {0: incoming[:, next_at:].reshape(width, width)}

    def widen(mask):
        pieces.update({k | mask: from_peer(piece, mask) for k, piece in sorted(pieces.items())})

    mask = relations // 2
    widen(mask)
    mean = pool(remote, pooled, incoming, degree, relations=relations, slot=slot)
    pieces, mean = lax.optimization_barrier((pieces, mean))
    while mask > 2:
        mask //= 2
        widen(mask)
    hidden, picked, self_next = middle(
        mean, features, incoming, swapped, bias_first[None], send, relations=relations
    )
    pieces, picked = lax.optimization_barrier((pieces, picked))
    while mask > 1:
        mask //= 2
        widen(mask)
    pieces = [pieces[k] for k in range(relations)]
    table = lax.all_to_all(picked, "dom", split_axis=0, concat_axis=0, tiled=True)
    partial = first(
        local, hidden, degree, self_next, bias_second[None], pieces, relations=relations
    )
    table, partial = lax.optimization_barrier((table, partial))
    return last(remote, table.reshape(-1, width), degree, partial, pieces, relations=relations)


def solution(mesh):
    placed = (
        P("dom", None),
        P("dom", None, None),
        P("dom", None, None),
        P("dom", None, None),
        P("dom"),
        P("dom", None, None),
        P(None, "dom", None),
        P("dom", None),
        P(),
        P(),
        P(None, "dom", None),
        P("dom", None),
        P(),
        P(),
    )
    return jax.shard_map(
        shards, mesh=mesh, in_specs=placed, out_specs=P("dom", None), check_vma=False
    )
```

```python
import functools

import jax
import jax.numpy as jnp
from jax import lax
from jax.experimental import pallas as pl
from jax.experimental.pallas import tpu as pltpu
from jax.sharding import PartitionSpec as P

WIN = 16
CHUNK = 512
GROUP = 8
EACH = 2
MIB = 1 << 20
WHOLE_MAX = 36 * MIB
CONTRACT_LANES = (((1,), (1,)), ((), ()))


def estimate(flops, nbytes):
    return pl.CostEstimate(flops=int(flops), bytes_accessed=int(nbytes), transcendentals=0)


def params(mib, **more):
    return pltpu.CompilerParams(vmem_limit_bytes=mib * MIB, **more)


def hot(rows, lanes):
    row_ids = lax.broadcasted_iota(jnp.int32, (rows, lanes.shape[1]), 0)
    return jnp.where(row_ids == lanes, 1.0, 0.0)


def code_edges(source_ref, relation_ref, target_ref, slot_ref, code_ref, low_ref, relations):
    slot = relation_ref[...] * WIN + (target_ref[...] & (WIN - 1))
    slot_ref[...] = slot
    code_ref[...] = (source_ref[...] // CHUNK) * (WIN * relations) + slot
    low_ref[...] = source_ref[...] & (CHUNK - 1)


def link_blocks(tile_ref, count_ref, head_ref, next_ref, tiles):
    def clear(t, carry):
        head_ref[t] = -1
        return carry

    lax.fori_loop(0, tiles, clear, 0)

    def link(b, carry):
        t = tile_ref[b] // WIN
        next_ref[b] = head_ref[t]
        head_ref[t] = b
        return carry

    lax.fori_loop(0, count_ref[0], link, 0)


def pair_of(first, next_ref):
    second = jnp.where(first >= 0, next_ref[jnp.maximum(first, 0)], -1)
    after = jnp.where(second >= 0, next_ref[jnp.maximum(second, 0)], -1)
    return second, after


def some_rows(ref, blocks):
    return jnp.concatenate(
        [jnp.where(b >= 0, ref[pl.ds(jnp.maximum(b, 0), 1), :], -1) for b in blocks], axis=1
    )


def count_blocks(blocks, slot_ref, code_ref, low_ref, rows, slots):
    left = hot(rows, some_rows(code_ref, blocks)).astype(jnp.bfloat16)
    right = hot(CHUNK, some_rows(low_ref, blocks)).astype(jnp.bfloat16)
    counts = lax.dot_general(left, right, CONTRACT_LANES, preferred_element_type=jnp.float32)
    degree = jnp.sum(hot(slots, some_rows(slot_ref, blocks)), axis=1, keepdims=True)
    return counts, degree


def put_counts(counts, local_ref, remote_ref, row, slots, locals_):
    for piece in range(counts.shape[0] // slots):
        part = counts[piece * slots : (piece + 1) * slots].astype(jnp.bfloat16)
        if piece < locals_:
            local_ref[pl.ds(row, slots), pl.ds(piece * CHUNK, CHUNK)] = part
        else:
            remote_ref[pl.ds(row, slots), pl.ds((piece - locals_) * CHUNK, CHUNK)] = part


def build_streamed(
    tile_ref, count_ref, source_ref, relation_ref, target_ref,
    local_ref, remote_ref, degree_ref,
    head_ref, next_ref, slot_ref, code_ref, low_ref, sum_ref,
    *, tiles, relations, locals_, pieces,
):
    slots = WIN * relations
    rows = pieces * slots
    t = pl.program_id(0)

    @pl.when(t == 0)
    def _():
        code_edges(source_ref, relation_ref, target_ref, slot_ref, code_ref, low_ref, relations)
        link_blocks(tile_ref, count_ref, head_ref, next_ref, tiles)

    sum_ref[...] = jnp.zeros_like(sum_ref)
    degree_ref[...] = jnp.zeros_like(degree_ref)

    def step(first):
        second, after = pair_of(first, next_ref)
        counts, degree = count_blocks([first, second], slot_ref, code_ref, low_ref, rows, slots)
        sum_ref[...] += counts
        degree_ref[...] += degree
        return after

    lax.while_loop(lambda first: first >= 0, step, head_ref[t])
    put_counts(sum_ref[...], local_ref, remote_ref, 0, slots, locals_)


def build_streamed_call(tile_of, count, source, relation, target, *, node_rows, relations, remote_rows):
    blocks, width = source.shape
    tiles, slots = node_rows // WIN, WIN * relations
    locals_, remotes = node_rows // CHUNK, remote_rows // CHUNK
    pieces = locals_ + remotes
    smem = pl.BlockSpec(memory_space=pltpu.SMEM)
    shapes = [
        ((tiles * slots, node_rows), jnp.bfloat16),
        ((tiles * slots, remote_rows), jnp.bfloat16),
        ((tiles * slots, 1), jnp.float32),
    ]
    whole = pl.BlockSpec((blocks, width), lambda t: (0, 0))
    return pl.pallas_call(
        functools.partial(
            build_streamed, tiles=tiles, relations=relations, locals_=locals_, pieces=pieces
        ),
        grid=(tiles,),
        out_shape=[jax.ShapeDtypeStruct(s, d) for s, d in shapes],
        in_specs=[smem, smem, whole, whole, whole],
        out_specs=[pl.BlockSpec((slots, s[1]), lambda t: (t, 0)) for s, _ in shapes],
        scratch_shapes=[
            pltpu.SMEM((tiles,), jnp.int32),
            pltpu.SMEM((blocks,), jnp.int32),
            pltpu.VMEM((blocks, width), jnp.int32),
            pltpu.VMEM((blocks, width), jnp.int32),
            pltpu.VMEM((blocks, width), jnp.int32),
            pltpu.VMEM((pieces * slots, CHUNK), jnp.float32),
        ],
        compiler_params=params(40),
        cost_estimate=estimate(
            4 * (tiles + blocks // 4) * pieces * slots * CHUNK * width,
            2 * tiles * slots * pieces * CHUNK,
        ),
        name="build",
    )(tile_of, count, source, relation, target)


def local_streamed_body(counts_ref, table_ref, pooled_ref):
    pooled_ref[...] = jnp.dot(
        counts_ref[...], table_ref[...], preferred_element_type=jnp.float32
    )


def local_streamed(counts, table, *, group):
    rows, depth = counts.shape
    width = table.shape[1]
    return pl.pallas_call(
        local_streamed_body,
        grid=(rows // group,),
        out_shape=jax.ShapeDtypeStruct((rows, width), jnp.float32),
        in_specs=[
            pl.BlockSpec((group, depth), lambda i: (i, 0)),
            pl.BlockSpec((depth, width), lambda i: (0, 0)),
        ],
        out_specs=pl.BlockSpec((group, width), lambda i: (i, 0)),
        compiler_params=params(40),
        cost_estimate=estimate(2 * rows * depth * width, 2 * rows * depth),
        name="local",
    )(counts, table)


def put_means(mean, mean_ref, first_tile, relations):
    slots = WIN * relations
    width = mean.shape[1]
    for tile in range(mean.shape[0] // slots):
        at = pl.multiple_of((first_tile + tile) * WIN, WIN)
        for relation in range(relations):
            start = tile * slots + relation * WIN
            mean_ref[pl.ds(at, WIN), pl.ds(relation * width, width)] = mean[start : start + WIN]


def remote_streamed_body(counts_ref, table_ref, pooled_ref, degree_ref, mean_ref, *, relations):
    total = pooled_ref[...] + jnp.dot(
        counts_ref[...], table_ref[...], preferred_element_type=jnp.float32
    )
    mean = total * (1.0 / jnp.maximum(degree_ref[...], 1.0))
    put_means(mean.astype(jnp.bfloat16), mean_ref, 0, relations)


def remote_streamed(counts, table, pooled, degree, *, relations, group):
    rows, depth = counts.shape
    width = table.shape[1]
    return pl.pallas_call(
        functools.partial(remote_streamed_body, relations=relations),
        grid=(rows // group,),
        out_shape=jax.ShapeDtypeStruct((rows // relations, relations * width), jnp.bfloat16),
        in_specs=[
            pl.BlockSpec((group, depth), lambda i: (i, 0)),
            pl.BlockSpec((depth, width), lambda i: (0, 0)),
            pl.BlockSpec((group, width), lambda i: (i, 0)),
            pl.BlockSpec((group, 1), lambda i: (i, 0)),
        ],
        out_specs=pl.BlockSpec((group // relations, relations * width), lambda i: (i, 0)),
        compiler_params=params(40),
        cost_estimate=estimate(2 * rows * depth * width, 2 * rows * depth),
        name="remote",
    )(counts, table, pooled, degree)


def in_hbm(*arrays):
    return [pltpu.with_memory_space_constraint(array, pltpu.HBM) for array in arrays]


def start_all(sems, *pairs):
    copies = [pltpu.make_async_copy(a, b, sems.at[i]) for i, (a, b) in enumerate(pairs)]
    for copy in copies:
        copy.start()
    return copies


def wait_all(copies):
    for copy in copies:
        copy.wait()


def build_body(
    tile_ref, count_ref, source_hbm, relation_hbm, target_hbm, own_hbm,
    local_ref, remote_ref, pooled_ref, degree_hbm,
    source_ref, relation_ref, target_ref, own_ref, degree_ref,
    local_v, remote_v, pooled_v, head_ref, next_ref, list_ref, slot_ref, code_ref, low_ref, sum_ref,
    sems, in_sems, *, tiles, relations, locals_, pieces,
):
    slots = WIN * relations
    rows = pieces * slots
    inputs = start_all(
        in_sems,
        (source_hbm, source_ref),
        (relation_hbm, relation_ref),
        (target_hbm, target_ref),
        (own_hbm, own_ref),
    )
    wait_all(inputs)
    code_edges(source_ref, relation_ref, target_ref, slot_ref, code_ref, low_ref, relations)
    link_blocks(tile_ref, count_ref, head_ref, next_ref, tiles)
    head_ref[tiles] = -1
    degree_ref[tiles // GROUP] = jnp.zeros((slots, GROUP), jnp.float32)
    counted = functools.partial(
        count_blocks, slot_ref=slot_ref, code_ref=code_ref, low_ref=low_ref, rows=rows, slots=slots
    )

    def place(t, piece):
        row = pl.multiple_of(t * slots, slots)
        ref, at = (local_v, piece) if piece < locals_ else (remote_v, piece - locals_)
        return ref, (pl.ds(row, slots), pl.ds(at * CHUNK, CHUNK))

    def part(counts, piece):
        return counts[piece * slots : (piece + 1) * slots]

    def add(t, blocks):
        counts, degree = counted(blocks)
        for piece in range(pieces):
            ref, where = place(t, piece)
            total = ref[where].astype(jnp.float32) + part(counts, piece)
            ref[where] = total.astype(jnp.bfloat16)
        add_degree(t, degree)

    def add_degree(t, degree):
        lanes = lax.broadcasted_iota(jnp.int32, (slots, GROUP), 1)
        degree_ref[t // GROUP] += jnp.where(lanes == t % GROUP, degree, 0.0)

    def copy_tile(t):
        some = pl.ds(pl.multiple_of(t * slots, slots), slots)
        pltpu.make_async_copy(local_v.at[some], local_ref.at[some], sems.at[0]).start()
        pltpu.make_async_copy(remote_v.at[some], remote_ref.at[some], sems.at[1]).start()

    def base(i, carry):
        afters = []
        for u in range(GROUP):
            t = i * GROUP + u
            first = head_ref[t]
            second, after = pair_of(first, next_ref)
            counts, degree = counted([first, second])
            for piece in range(pieces):
                ref, where = place(t, piece)
                ref[where] = part(counts, piece).astype(jnp.bfloat16)
            degree_ref[i, :, pl.ds(u, 1)] = degree
            head_ref[t] = after
            afters.append(after)
        for u, after in enumerate(afters):

            @pl.when(after < 0)
            def _():
                copy_tile(i * GROUP + u)

        return carry

    lax.fori_loop(0, tiles // GROUP, base, 0)

    def sort_tile(t, sizes):
        short, mid, long = sizes
        first = head_ref[t]
        _, third = pair_of(first, next_ref)
        _, fifth = pair_of(third, next_ref)
        list_ref[0, short] = t
        list_ref[1, mid] = t
        list_ref[2, long] = t
        more = first >= 0
        return (
            short + jnp.where(more & (third < 0), 1, 0),
            mid + jnp.where(more & (third >= 0) & (fifth < 0), 1, 0),
            long + jnp.where(more & (fifth >= 0), 1, 0),
        )

    zero = jnp.int32(0)
    short, mid, long = lax.fori_loop(0, tiles, sort_tile, (zero, zero, zero))
    for k in range(4):
        list_ref[0, short + k] = tiles
        list_ref[1, mid + k] = tiles

    def add_short(j, carry):
        for k in range(4):
            t = list_ref[0, 4 * j + k]
            first = head_ref[t]
            second, _ = pair_of(first, next_ref)
            add(t, [first, second])
        for k in range(4):
            t = list_ref[0, 4 * j + k]

            @pl.when(t < tiles)
            def _():
                copy_tile(t)

        return carry

    def add_mid(j, carry):
        for k in range(2):
            t = list_ref[1, 2 * j + k]
            first = head_ref[t]
            second, third = pair_of(first, next_ref)
            fourth, _ = pair_of(third, next_ref)
            add(t, [first, second, third, fourth])
        for k in range(2):
            t = list_ref[1, 2 * j + k]

            @pl.when(t < tiles)
            def _():
                copy_tile(t)

        return carry

    def add_long(j, carry):
        t = list_ref[2, j]
        for piece in range(pieces):
            ref, where = place(t, piece)
            sum_ref[pl.ds(piece * slots, slots), :] = ref[where].astype(jnp.float32)

        def step(first):
            second, after = pair_of(first, next_ref)
            counts, degree = counted([first, second])
            sum_ref[...] += counts
            add_degree(t, degree)
            return after

        lax.while_loop(lambda first: first >= 0, step, head_ref[t])
        for piece in range(pieces):
            ref, where = place(t, piece)
            ref[where] = sum_ref[pl.ds(piece * slots, slots), :].astype(jnp.bfloat16)
        copy_tile(t)
        return carry

    lax.fori_loop(0, (short + 3) // 4, add_short, 0)
    lax.fori_loop(0, (mid + 1) // 2, add_mid, 0)
    lax.fori_loop(0, long, add_long, 0)

    def pool_own(i, carry):
        some = pl.ds(pl.multiple_of(i * GROUP * slots, GROUP * slots), GROUP * slots)
        pooled_v[some, :] = jnp.dot(
            local_v[some, :], own_ref[...], preferred_element_type=jnp.float32
        )
        pltpu.make_async_copy(pooled_v.at[some], pooled_ref.at[some], sems.at[2]).start()
        return carry

    lax.fori_loop(0, tiles // GROUP, pool_own, 0)
    every = pl.ds(0, tiles * slots)
    pltpu.make_async_copy(local_v.at[every], local_ref, sems.at[0]).wait()
    pltpu.make_async_copy(remote_v.at[every], remote_ref, sems.at[1]).wait()
    pltpu.make_async_copy(pooled_v, pooled_ref, sems.at[2]).wait()
    pltpu.sync_copy(degree_ref.at[pl.ds(0, tiles // GROUP)], degree_hbm)


def build(tile_of, count, source, relation, target, own, *, relations, remote_rows):
    blocks, block_width = source.shape
    node_rows, width = own.shape
    tiles, slots = node_rows // WIN, WIN * relations
    rows = tiles * slots
    locals_, remotes = node_rows // CHUNK, remote_rows // CHUNK
    pieces = locals_ + remotes
    vmem = pl.BlockSpec(memory_space=pltpu.VMEM)
    smem = pl.BlockSpec(memory_space=pltpu.SMEM)
    hbm = pl.BlockSpec(memory_space=pltpu.HBM)
    return pl.pallas_call(
        functools.partial(
            build_body, tiles=tiles, relations=relations, locals_=locals_, pieces=pieces
        ),
        out_shape=[
            pltpu.HBM((rows, node_rows), jnp.bfloat16),
            pltpu.HBM((rows, remote_rows), jnp.bfloat16),
            pltpu.HBM((rows, width), jnp.float32),
            pltpu.HBM((tiles // GROUP, slots, GROUP), jnp.float32),
        ],
        in_specs=[smem, smem] + [hbm] * 4,
        out_specs=[hbm] * 4,
        scratch_shapes=[
            pltpu.VMEM((blocks, block_width), jnp.int32),
            pltpu.VMEM((blocks, block_width), jnp.int32),
            pltpu.VMEM((blocks, block_width), jnp.int32),
            pltpu.VMEM((node_rows, width), jnp.bfloat16),
            pltpu.VMEM((tiles // GROUP + 1, slots, GROUP), jnp.float32),
            pltpu.VMEM((rows + slots, node_rows), jnp.bfloat16),
            pltpu.VMEM((rows + slots, remote_rows), jnp.bfloat16),
            pltpu.VMEM((rows, width), jnp.float32),
            pltpu.SMEM((tiles + 1,), jnp.int32),
            pltpu.SMEM((blocks,), jnp.int32),
            pltpu.SMEM((3, tiles + 8), jnp.int32),
            pltpu.VMEM((blocks, block_width), jnp.int32),
            pltpu.VMEM((blocks, block_width), jnp.int32),
            pltpu.VMEM((blocks, block_width), jnp.int32),
            pltpu.VMEM((pieces * slots, CHUNK), jnp.float32),
            pltpu.SemaphoreType.DMA((3,)),
            pltpu.SemaphoreType.DMA((4,)),
        ],
        compiler_params=params(58),
        cost_estimate=estimate(
            4 * (tiles + blocks // 4) * pieces * slots * CHUNK * block_width
            + 2 * rows * node_rows * width,
            2 * rows * pieces * CHUNK,
        ),
        name="build",
    )(tile_of, count, *in_hbm(source, relation, target, own))


def pool_groups(
    counts_ref, counts_v, sems, table_ref, degree_ref, mean_ref, relations, begun, extra=None
):
    size = GROUP * WIN * relations
    groups = counts_ref.shape[0] // size

    def copies(i):
        some = pl.ds(pl.multiple_of(i * size, size), size)
        found = [pltpu.make_async_copy(counts_ref.at[some], counts_v.at[some], sems.at[0, i])]
        if extra is not None:
            found.append(pltpu.make_async_copy(extra[0].at[some], extra[1].at[some], sems.at[1, i]))
        return found

    def begin(i, carry):
        for copy in copies(i):
            copy.start()
        return carry

    def step(i, carry):
        for copy in copies(i):
            copy.wait()
        some = pl.ds(pl.multiple_of(i * size, size), size)
        total = jnp.dot(counts_v[some, :], table_ref[...], preferred_element_type=jnp.float32)
        if extra is not None:
            total += extra[1][some, :]
        share = 1.0 / jnp.maximum(degree_ref[i], 1.0)
        slots = WIN * relations
        for u in range(GROUP):
            mean = total[u * slots : (u + 1) * slots] * share[:, u : u + 1]
            put_means(mean.astype(jnp.bfloat16), mean_ref, i * GROUP + u, relations)
        return carry

    lax.fori_loop(0, groups, begin, 0)
    begun()
    lax.fori_loop(0, groups, step, 0)


def copy_table(incoming_ref, table_ref, slot):
    for device in range(incoming_ref.shape[0]):
        table_ref[device * slot : (device + 1) * slot, :] = incoming_ref[device, :slot, :]


def pool_body(
    counts_ref, pooled_ref, incoming_ref, degree_hbm, mean_ref,
    counts_v, pooled_v, table_v, degree_v, sems, in_sems, *, relations, slot,
):
    inputs = start_all(in_sems, (degree_hbm, degree_v))

    def begun():
        copy_table(incoming_ref, table_v, slot)
        wait_all(inputs)

    pool_groups(
        counts_ref, counts_v, sems, table_v, degree_v, mean_ref, relations, begun,
        extra=(pooled_ref, pooled_v),
    )


def pool(counts, pooled, incoming, degree, *, relations, slot):
    rows, depth = counts.shape
    width = incoming.shape[2]
    vmem = pl.BlockSpec(memory_space=pltpu.VMEM)
    hbm = pl.BlockSpec(memory_space=pltpu.HBM)
    return pl.pallas_call(
        functools.partial(pool_body, relations=relations, slot=slot),
        out_shape=jax.ShapeDtypeStruct((rows // relations, relations * width), jnp.bfloat16),
        in_specs=[hbm, hbm, vmem, hbm],
        out_specs=vmem,
        scratch_shapes=[
            pltpu.VMEM(counts.shape, counts.dtype),
            pltpu.VMEM(pooled.shape, pooled.dtype),
            pltpu.VMEM((depth, width), jnp.bfloat16),
            pltpu.VMEM(degree.shape, degree.dtype),
            pltpu.SemaphoreType.DMA((2, degree.shape[0])),
            pltpu.SemaphoreType.DMA((1,)),
        ],
        compiler_params=params(44),
        cost_estimate=estimate(2 * rows * depth * width, 2 * rows * depth),
        name="pool",
    )(*in_hbm(counts, pooled), incoming, *in_hbm(degree))


def pick_rows(send_ref, rows_ref, emit, done):
    devices, slot = send_ref.shape
    depth = rows_ref.shape[0]
    columns = send_ref[...].astype(jnp.float32).T.astype(jnp.int32)
    lanes = lax.broadcasted_iota(jnp.int32, (slot, depth), 1)
    step = 8
    for start in range(0, devices, step):
        chosen = jnp.concatenate(
            [
                jnp.where(columns[:, device : device + 1] == lanes, 1.0, 0.0).astype(jnp.bfloat16)
                for device in range(start, start + step)
            ],
            axis=0,
        )
        picked = jnp.dot(chosen, rows_ref[...], preferred_element_type=jnp.float32)
        for k in range(step):
            emit(start + k, picked[k * slot : (k + 1) * slot].astype(jnp.bfloat16))
        done(start, step)


def send_out(out_v, out_ref, sems, start, count):
    some = pl.ds(start, count)
    pltpu.make_async_copy(out_v.at[some], out_ref.at[some], sems.at[0]).start()


def middle_body(
    mean_ref, own_hbm, incoming_ref, swapped_ref, bias_hbm, send_hbm,
    hidden_hbm, out_ref, self_hbm,
    own_v, bias_v, send_v, hidden_v, out_v, self_v, weights_v, sems, in_sems,
    *, relations, slot,
):
    inputs = start_all(in_sems, (own_hbm, own_v), (bias_hbm, bias_v), (send_hbm, send_v))
    width = own_v.shape[1]
    half = relations // 2
    devices = incoming_ref.shape[0]
    piece = width // devices
    block = (half + 1) * width
    for device in range(devices):
        for m in range(half + 1):
            at = m * width + device * piece
            weights_v[at : at + piece, :] = incoming_ref[
                device, slot + m * piece : slot + (m + 1) * piece, :
            ]
            weights_v[block + at : block + at + piece, :] = swapped_ref[
                device, m * piece : (m + 1) * piece, :
            ]
    side = lax.axis_index("dom") & 1
    mine_at = pl.multiple_of(side * (half * width), width)
    other_at = pl.multiple_of((1 - side) * (half * width), width)
    own_at = pl.multiple_of(half * width + side * block, width)
    next_at = pl.multiple_of(half * width + (1 - side) * block, width)
    self_v[...] = weights_v[pl.ds(next_at, width), :]
    total = jnp.dot(
        mean_ref[:, pl.ds(mine_at, half * width)],
        weights_v[: half * width, :],
        preferred_element_type=jnp.float32,
    )
    total += jnp.dot(
        mean_ref[:, pl.ds(other_at, half * width)],
        weights_v[block : block + half * width, :],
        preferred_element_type=jnp.float32,
    )
    wait_all(inputs)
    total += jnp.dot(
        own_v[...], weights_v[pl.ds(own_at, width), :], preferred_element_type=jnp.float32
    )
    hidden_v[...] = jnp.maximum(total + bias_v[...], 0.0).astype(jnp.bfloat16)
    outputs = [
        pltpu.make_async_copy(hidden_v, hidden_hbm, sems.at[1]),
        pltpu.make_async_copy(self_v, self_hbm, sems.at[2]),
    ]
    for copy in outputs:
        copy.start()

    def emit(device, picked):
        out_v[device, :, :] = picked

    pick_rows(send_v, hidden_v, emit, functools.partial(send_out, out_v, out_ref, sems))
    pltpu.make_async_copy(out_v, out_ref, sems.at[0]).wait()
    wait_all(outputs)


def middle(mean, own, incoming, swapped, bias, send, *, relations):
    nodes, width = own.shape
    devices, slot = send.shape
    vmem = pl.BlockSpec(memory_space=pltpu.VMEM)
    hbm = pl.BlockSpec(memory_space=pltpu.HBM)
    return pl.pallas_call(
        functools.partial(middle_body, relations=relations, slot=slot),
        out_shape=[
            pltpu.HBM((nodes, width), jnp.bfloat16),
            pltpu.HBM((devices, slot, width), jnp.bfloat16),
            pltpu.HBM((width, width), jnp.bfloat16),
        ],
        in_specs=[vmem, hbm, vmem, vmem, hbm, hbm],
        out_specs=[hbm] * 3,
        scratch_shapes=[
            pltpu.VMEM(own.shape, own.dtype),
            pltpu.VMEM(bias.shape, bias.dtype),
            pltpu.VMEM(send.shape, send.dtype),
            pltpu.VMEM((nodes, width), jnp.bfloat16),
            pltpu.VMEM((devices, slot, width), jnp.bfloat16),
            pltpu.VMEM((width, width), jnp.bfloat16),
            pltpu.VMEM(((relations + 2) * width, width), jnp.bfloat16),
            pltpu.SemaphoreType.DMA((3,)),
            pltpu.SemaphoreType.DMA((3,)),
        ],
        compiler_params=params(24),
        cost_estimate=estimate(2 * nodes * mean.shape[1] * width, 0),
        name="middle",
    )(mean, *in_hbm(own), incoming, swapped, *in_hbm(bias, send))


def weight_copies(pieces, weights_v, relations):
    width = weights_v.shape[1]
    ways = relations // EACH
    class_ = lax.axis_index("dom") & (ways - 1)

    def rows(k):
        relation = (class_ ^ (k // EACH)) + ways * (k % EACH)
        return weights_v.at[pl.ds(pl.multiple_of(relation * width, width), width)]

    return [(piece, rows(k)) for k, piece in enumerate(pieces)]


def first_body(
    counts_ref, own_hbm, degree_hbm, self_hbm, bias_hbm, *refs, relations
):
    pieces, refs = refs[:relations], refs[relations:]
    out_hbm, own_v, degree_v, self_v, bias_v, out_v, weights_v, counts_v, mean_v, sems, in_sems = refs
    inputs = start_all(in_sems, (own_hbm, own_v), (degree_hbm, degree_v))
    later = []

    def begun():
        later.extend(
            start_all(
                in_sems.at[pl.ds(2, 2 + relations)],
                (self_hbm, self_v),
                (bias_hbm, bias_v),
                *weight_copies(pieces, weights_v, relations),
            )
        )
        wait_all(inputs)

    pool_groups(counts_ref, counts_v, sems, own_v, degree_v, mean_v, relations, begun)
    wait_all(later)
    total = jnp.dot(mean_v[...], weights_v[...], preferred_element_type=jnp.float32)
    total += jnp.dot(own_v[...], self_v[...], preferred_element_type=jnp.float32)
    out_v[...] = total + bias_v[...]
    pltpu.sync_copy(out_v, out_hbm)


def first(counts, own, degree, self_weight, bias, pieces, *, relations):
    rows, depth = counts.shape
    nodes, width = own.shape
    hbm = pl.BlockSpec(memory_space=pltpu.HBM)
    return pl.pallas_call(
        functools.partial(first_body, relations=relations),
        out_shape=pltpu.HBM((nodes, width), jnp.float32),
        in_specs=[hbm] * (5 + relations),
        out_specs=hbm,
        scratch_shapes=[
            pltpu.VMEM(own.shape, own.dtype),
            pltpu.VMEM(degree.shape, degree.dtype),
            pltpu.VMEM(self_weight.shape, self_weight.dtype),
            pltpu.VMEM(bias.shape, bias.dtype),
            pltpu.VMEM((nodes, width), jnp.float32),
            pltpu.VMEM((relations * width, width), jnp.bfloat16),
            pltpu.VMEM(counts.shape, counts.dtype),
            pltpu.VMEM((nodes, relations * width), jnp.bfloat16),
            pltpu.SemaphoreType.DMA((1, degree.shape[0])),
            pltpu.SemaphoreType.DMA((4 + relations,)),
        ],
        compiler_params=params(44),
        cost_estimate=estimate(
            2 * rows * depth * width + 2 * nodes * relations * width * width, 2 * rows * depth
        ),
        name="first",
    )(*in_hbm(counts, own, degree, self_weight, bias, *pieces))


def last_body(counts_ref, table_ref, degree_hbm, partial_hbm, *refs, relations):
    pieces, refs = refs[:relations], refs[relations:]
    out_ref, degree_v, partial_v, weights_v, counts_v, mean_v, sems, in_sems = refs
    inputs = start_all(in_sems, (degree_hbm, degree_v))
    later = []

    def begun():
        later.extend(
            start_all(
                in_sems.at[pl.ds(1, 1 + relations)],
                (partial_hbm, partial_v),
                *weight_copies(pieces, weights_v, relations),
            )
        )
        wait_all(inputs)

    pool_groups(counts_ref, counts_v, sems, table_ref, degree_v, mean_v, relations, begun)
    wait_all(later)
    total = jnp.dot(mean_v[...], weights_v[...], preferred_element_type=jnp.float32)
    out_ref[...] = (total + partial_v[...]).astype(out_ref.dtype)


def last(counts, table, degree, partial, pieces, *, relations):
    rows, depth = counts.shape
    width = table.shape[1]
    nodes = rows // relations
    vmem = pl.BlockSpec(memory_space=pltpu.VMEM)
    hbm = pl.BlockSpec(memory_space=pltpu.HBM)
    return pl.pallas_call(
        functools.partial(last_body, relations=relations),
        out_shape=jax.ShapeDtypeStruct((nodes, width), jnp.bfloat16),
        in_specs=[hbm, vmem] + [hbm] * (2 + relations),
        out_specs=vmem,
        scratch_shapes=[
            pltpu.VMEM(degree.shape, degree.dtype),
            pltpu.VMEM(partial.shape, partial.dtype),
            pltpu.VMEM((relations * width, width), jnp.bfloat16),
            pltpu.VMEM(counts.shape, counts.dtype),
            pltpu.VMEM((nodes, relations * width), jnp.bfloat16),
            pltpu.SemaphoreType.DMA((1, degree.shape[0])),
            pltpu.SemaphoreType.DMA((2 + relations,)),
        ],
        compiler_params=params(44),
        cost_estimate=estimate(
            2 * rows * depth * width + 2 * nodes * relations * width * width, 2 * rows * depth
        ),
        name="last",
    )(*in_hbm(counts), table, *in_hbm(degree, partial, *pieces))


def pack_body(*refs):
    inputs_hbm, out_ref, inputs_v, (out_v, sems, in_sems) = refs[:8], refs[8], refs[9:17], refs[17:]
    inputs = start_all(in_sems, *zip(inputs_hbm, inputs_v))
    coef_first, coef_second, bases_first, bases_second, self_first, self_second, features, send = (
        inputs_v
    )
    relations, bases = coef_first.shape
    devices, slot = send.shape
    piece = self_first.shape[0]
    half = relations // 2
    wait_all(inputs)

    def mix(coef_ref, bases_ref):
        mixed = []
        for relation in range(relations):
            total = coef_ref[relation, 0] * bases_ref[0].astype(jnp.float32)
            for base in range(1, bases):
                total += coef_ref[relation, base] * bases_ref[base].astype(jnp.float32)
            mixed.append(total.astype(jnp.bfloat16))
        return mixed

    first = mix(coef_first, bases_first)
    second = mix(coef_second, bases_second)
    own = [self_first[...], self_second[...]]
    for device in range(devices):
        side = device % 2
        ways = relations // EACH
        rows = first[side * half : (side + 1) * half] + [own[side]] + second[device % ways :: ways]
        for k, value in enumerate(rows):
            at = slot + k * piece
            out_v[device, at : at + piece, :] = value

    def emit(device, picked):
        out_v[device, :slot, :] = picked

    pick_rows(send, features, emit, functools.partial(send_out, out_v, out_ref, sems))
    pltpu.make_async_copy(out_v, out_ref, sems.at[0]).wait()


def pack(features, send, bases_first, self_first, coef_first, bases_second, self_second, coef_second):
    devices, slot = send.shape
    relations = coef_first.shape[0]
    piece, width = self_first.shape
    hbm = pl.BlockSpec(memory_space=pltpu.HBM)
    shape = (devices, slot + (relations // 2 + 1 + EACH) * piece, width)
    args = (
        coef_first, coef_second, bases_first, bases_second, self_first, self_second, features, send,
    )
    return pl.pallas_call(
        pack_body,
        out_shape=pltpu.HBM(shape, jnp.bfloat16),
        in_specs=[hbm] * 8,
        out_specs=hbm,
        scratch_shapes=[
            *[pltpu.SMEM(a.shape, a.dtype) for a in args[:2]],
            *[pltpu.VMEM(a.shape, a.dtype) for a in args[2:]],
            pltpu.VMEM(shape, jnp.bfloat16),
            pltpu.SemaphoreType.DMA((1,)),
            pltpu.SemaphoreType.DMA((8,)),
        ],
        compiler_params=params(24),
        cost_estimate=estimate(2 * devices * slot * features.size, 0),
        name="pack",
    )(*in_hbm(*args))


def dense_body(mean_ref, own_ref, weights_ref, bias_ref, out_ref, *, last):
    depth = mean_ref.shape[1]
    total = jnp.dot(mean_ref[...], weights_ref[:depth], preferred_element_type=jnp.float32)
    total += jnp.dot(own_ref[...], weights_ref[depth:], preferred_element_type=jnp.float32)
    total += bias_ref[...]
    out_ref[...] = (total if last else jnp.maximum(total, 0.0)).astype(jnp.bfloat16)


def dense(mean, own, weights, bias, *, last):
    nodes, width = own.shape
    vmem = pl.BlockSpec(memory_space=pltpu.VMEM)
    return pl.pallas_call(
        functools.partial(dense_body, last=last),
        out_shape=jax.ShapeDtypeStruct((nodes, width), jnp.bfloat16),
        in_specs=[vmem] * 4,
        out_specs=vmem,
        compiler_params=params(16),
        cost_estimate=estimate(2 * nodes * mean.shape[1] * width, 0),
        name="dense",
    )(mean, own, weights, bias)


def mix_weights(bases, self_weight, coef):
    mixed = jnp.einsum(
        "rb,bij->rij", coef, bases.astype(jnp.float32), precision=lax.Precision.HIGHEST
    ).astype(jnp.bfloat16)
    return jnp.concatenate([mixed, self_weight[None]], axis=0)


def general_layers(
    features, edges, send, weights_first, weights_second, bias_first, bias_second, relations
):
    node_rows, width = features.shape
    devices, slot = send.shape
    half = relations // 2
    swap = [(i, i ^ 1) for i in range(devices)]
    side = lax.axis_index("dom") & 1

    def send_all(rows, weights):
        rows = rows[send]
        halves = [
            jnp.concatenate([weights[:half], weights[relations:]], axis=0).reshape(-1, width),
            jnp.concatenate([weights[half:relations], weights[relations:]], axis=0).reshape(-1, width),
        ]
        halves = jnp.broadcast_to(jnp.stack(halves)[None], (devices // 2, 2) + halves[0].shape)
        rows = jnp.concatenate([rows, halves.reshape(devices, -1, width)], axis=1)
        return lax.all_to_all(rows, "dom", split_axis=0, concat_axis=0, tiled=True)

    def take_all(incoming):
        mine = jnp.swapaxes(incoming[:, slot:].reshape(devices, half + 1, -1, width), 0, 1)
        mine = mine.reshape(-1, width)
        other = lax.ppermute(mine[: half * width], "dom", swap)
        mine, own = mine[: half * width], mine[half * width :]
        low, high = jnp.where(side == 0, mine, other), jnp.where(side == 0, other, mine)
        return incoming[:, :slot].reshape(-1, width), jnp.concatenate([low, high, own], axis=0)

    local, remote, degree = build_streamed_call(
        *edges, node_rows=node_rows, relations=relations, remote_rows=devices * slot
    )

    def layer(rows, weights, bias, last):
        incoming = send_all(rows, weights)
        pooled = local_streamed(local, rows, group=512)
        table, full = take_all(incoming)
        mean = remote_streamed(remote, table, pooled, degree, relations=relations, group=512)
        return dense(mean, rows, full, bias[None], last=last)

    hidden = layer(features, weights_first, bias_first, False)
    return layer(hidden, weights_second, bias_second, True)


def shards(
    features,
    edge_source,
    edge_relation,
    edge_target,
    block_count,
    send_list,
    bases_first,
    self_first,
    coef_first,
    bias_first,
    bases_second,
    self_second,
    coef_second,
    bias_second,
):
    node_rows, width = features.shape
    relations = coef_first.shape[0]
    devices, slot = send_list.shape[1:]
    remote_rows = devices * slot
    send = send_list[0]
    edges = (edge_target[0, :, 0], block_count, edge_source[0], edge_relation[0], edge_target[0])
    if 2 * node_rows * relations * (node_rows + remote_rows) > WHOLE_MAX:
        return general_layers(
            features,
            edges,
            send,
            mix_weights(bases_first, self_first, coef_first),
            mix_weights(bases_second, self_second, coef_second),
            bias_first,
            bias_second,
            relations,
        )
    outgoing = pack(
        features, send, bases_first, self_first, coef_first, bases_second, self_second, coef_second
    )
    incoming = lax.all_to_all(outgoing, "dom", split_axis=0, concat_axis=0, tiled=True)
    local, remote, pooled, degree = build(
        *edges, features, relations=relations, remote_rows=remote_rows
    )
    incoming, degree = lax.optimization_barrier((incoming, degree))

    def from_peer(array, mask):
        return lax.ppermute(array, "dom", [(i, i ^ mask) for i in range(devices)])

    next_at = slot + (relations // 2 + 1) * self_first.shape[0]
    swapped = from_peer(incoming[:, slot:next_at], 1)
    row = self_first.shape[0]
    pieces = {
        (0, e): incoming[:, next_at + e * row : next_at + (e + 1) * row].reshape(width, width)
        for e in range(EACH)
    }

    def widen(mask):
        pieces.update(
            {(k | mask, e): from_peer(piece, mask) for (k, e), piece in sorted(pieces.items())}
        )

    mask = relations // EACH // 2
    widen(mask)
    mean = pool(remote, pooled, incoming, degree, relations=relations, slot=slot)
    pieces, mean = lax.optimization_barrier((pieces, mean))
    while mask > 1:
        mask //= 2
        widen(mask)
    hidden, picked, self_next = middle(
        mean, features, incoming, swapped, bias_first[None], send, relations=relations
    )
    pieces, picked = lax.optimization_barrier((pieces, picked))
    pieces = [piece for _, piece in sorted(pieces.items())]
    table = lax.all_to_all(picked, "dom", split_axis=0, concat_axis=0, tiled=True)
    partial = first(
        local, hidden, degree, self_next, bias_second[None], pieces, relations=relations
    )
    table, partial = lax.optimization_barrier((table, partial))
    return last(remote, table.reshape(-1, width), degree, partial, pieces, relations=relations)


def solution(mesh):
    placed = (
        P("dom", None),
        P("dom", None, None),
        P("dom", None, None),
        P("dom", None, None),
        P("dom"),
        P("dom", None, None),
        P(None, "dom", None),
        P("dom", None),
        P(),
        P(),
        P(None, "dom", None),
        P("dom", None),
        P(),
        P(),
    )
    return jax.shard_map(
        shards, mesh=mesh, in_specs=placed, out_specs=P("dom", None), check_vma=False
    )
```

```python
import functools

import jax
import jax.numpy as jnp
from jax import lax
from jax.experimental import pallas as pl
from jax.experimental.pallas import tpu as pltpu
from jax.sharding import PartitionSpec as P

WIN = 16
CHUNK = 512
GROUP = 8
EACH = 1
MIB = 1 << 20
WHOLE_MAX = 36 * MIB
CONTRACT_LANES = (((1,), (1,)), ((), ()))


def estimate(flops, nbytes):
    return pl.CostEstimate(flops=int(flops), bytes_accessed=int(nbytes), transcendentals=0)


def params(mib, **more):
    return pltpu.CompilerParams(vmem_limit_bytes=mib * MIB, **more)


def hot(rows, lanes):
    row_ids = lax.broadcasted_iota(jnp.int32, (rows, lanes.shape[1]), 0)
    return jnp.where(row_ids == lanes, 1.0, 0.0)


def code_edges(source_ref, relation_ref, target_ref, slot_ref, code_ref, low_ref, relations):
    slot = relation_ref[...] * WIN + (target_ref[...] & (WIN - 1))
    slot_ref[...] = slot
    code_ref[...] = (source_ref[...] // CHUNK) * (WIN * relations) + slot
    low_ref[...] = source_ref[...] & (CHUNK - 1)


def link_blocks(tile_ref, count_ref, head_ref, next_ref, tiles):
    def clear(t, carry):
        head_ref[t] = -1
        return carry

    lax.fori_loop(0, tiles, clear, 0)

    def link(b, carry):
        t = tile_ref[b] // WIN
        next_ref[b] = head_ref[t]
        head_ref[t] = b
        return carry

    lax.fori_loop(0, count_ref[0], link, 0)


def pair_of(first, next_ref):
    second = jnp.where(first >= 0, next_ref[jnp.maximum(first, 0)], -1)
    after = jnp.where(second >= 0, next_ref[jnp.maximum(second, 0)], -1)
    return second, after


def some_rows(ref, blocks):
    return jnp.concatenate(
        [jnp.where(b >= 0, ref[pl.ds(jnp.maximum(b, 0), 1), :], -1) for b in blocks], axis=1
    )


def count_blocks(blocks, slot_ref, code_ref, low_ref, rows, slots):
    left = hot(rows, some_rows(code_ref, blocks)).astype(jnp.bfloat16)
    right = hot(CHUNK, some_rows(low_ref, blocks)).astype(jnp.bfloat16)
    counts = lax.dot_general(left, right, CONTRACT_LANES, preferred_element_type=jnp.float32)
    degree = jnp.sum(hot(slots, some_rows(slot_ref, blocks)), axis=1, keepdims=True)
    return counts, degree


def put_counts(counts, local_ref, remote_ref, row, slots, locals_):
    for piece in range(counts.shape[0] // slots):
        part = counts[piece * slots : (piece + 1) * slots].astype(jnp.bfloat16)
        if piece < locals_:
            local_ref[pl.ds(row, slots), pl.ds(piece * CHUNK, CHUNK)] = part
        else:
            remote_ref[pl.ds(row, slots), pl.ds((piece - locals_) * CHUNK, CHUNK)] = part


def build_streamed(
    tile_ref, count_ref, source_ref, relation_ref, target_ref,
    local_ref, remote_ref, degree_ref,
    head_ref, next_ref, slot_ref, code_ref, low_ref, sum_ref,
    *, tiles, relations, locals_, pieces,
):
    slots = WIN * relations
    rows = pieces * slots
    t = pl.program_id(0)

    @pl.when(t == 0)
    def _():
        code_edges(source_ref, relation_ref, target_ref, slot_ref, code_ref, low_ref, relations)
        link_blocks(tile_ref, count_ref, head_ref, next_ref, tiles)

    sum_ref[...] = jnp.zeros_like(sum_ref)
    degree_ref[...] = jnp.zeros_like(degree_ref)

    def step(first):
        second, after = pair_of(first, next_ref)
        counts, degree = count_blocks([first, second], slot_ref, code_ref, low_ref, rows, slots)
        sum_ref[...] += counts
        degree_ref[...] += degree
        return after

    lax.while_loop(lambda first: first >= 0, step, head_ref[t])
    put_counts(sum_ref[...], local_ref, remote_ref, 0, slots, locals_)


def build_streamed_call(tile_of, count, source, relation, target, *, node_rows, relations, remote_rows):
    blocks, width = source.shape
    tiles, slots = node_rows // WIN, WIN * relations
    locals_, remotes = node_rows // CHUNK, remote_rows // CHUNK
    pieces = locals_ + remotes
    smem = pl.BlockSpec(memory_space=pltpu.SMEM)
    shapes = [
        ((tiles * slots, node_rows), jnp.bfloat16),
        ((tiles * slots, remote_rows), jnp.bfloat16),
        ((tiles * slots, 1), jnp.float32),
    ]
    whole = pl.BlockSpec((blocks, width), lambda t: (0, 0))
    return pl.pallas_call(
        functools.partial(
            build_streamed, tiles=tiles, relations=relations, locals_=locals_, pieces=pieces
        ),
        grid=(tiles,),
        out_shape=[jax.ShapeDtypeStruct(s, d) for s, d in shapes],
        in_specs=[smem, smem, whole, whole, whole],
        out_specs=[pl.BlockSpec((slots, s[1]), lambda t: (t, 0)) for s, _ in shapes],
        scratch_shapes=[
            pltpu.SMEM((tiles,), jnp.int32),
            pltpu.SMEM((blocks,), jnp.int32),
            pltpu.VMEM((blocks, width), jnp.int32),
            pltpu.VMEM((blocks, width), jnp.int32),
            pltpu.VMEM((blocks, width), jnp.int32),
            pltpu.VMEM((pieces * slots, CHUNK), jnp.float32),
        ],
        compiler_params=params(40),
        cost_estimate=estimate(
            4 * (tiles + blocks // 4) * pieces * slots * CHUNK * width,
            2 * tiles * slots * pieces * CHUNK,
        ),
        name="build",
    )(tile_of, count, source, relation, target)


def local_streamed_body(counts_ref, table_ref, pooled_ref):
    pooled_ref[...] = jnp.dot(
        counts_ref[...], table_ref[...], preferred_element_type=jnp.float32
    )


def local_streamed(counts, table, *, group):
    rows, depth = counts.shape
    width = table.shape[1]
    return pl.pallas_call(
        local_streamed_body,
        grid=(rows // group,),
        out_shape=jax.ShapeDtypeStruct((rows, width), jnp.float32),
        in_specs=[
            pl.BlockSpec((group, depth), lambda i: (i, 0)),
            pl.BlockSpec((depth, width), lambda i: (0, 0)),
        ],
        out_specs=pl.BlockSpec((group, width), lambda i: (i, 0)),
        compiler_params=params(40),
        cost_estimate=estimate(2 * rows * depth * width, 2 * rows * depth),
        name="local",
    )(counts, table)


def put_means(mean, mean_ref, first_tile, relations):
    slots = WIN * relations
    width = mean.shape[1]
    for tile in range(mean.shape[0] // slots):
        at = pl.multiple_of((first_tile + tile) * WIN, WIN)
        for relation in range(relations):
            start = tile * slots + relation * WIN
            mean_ref[pl.ds(at, WIN), pl.ds(relation * width, width)] = mean[start : start + WIN]


def remote_streamed_body(counts_ref, table_ref, pooled_ref, degree_ref, mean_ref, *, relations):
    total = pooled_ref[...] + jnp.dot(
        counts_ref[...], table_ref[...], preferred_element_type=jnp.float32
    )
    mean = total * (1.0 / jnp.maximum(degree_ref[...], 1.0))
    put_means(mean.astype(jnp.bfloat16), mean_ref, 0, relations)


def remote_streamed(counts, table, pooled, degree, *, relations, group):
    rows, depth = counts.shape
    width = table.shape[1]
    return pl.pallas_call(
        functools.partial(remote_streamed_body, relations=relations),
        grid=(rows // group,),
        out_shape=jax.ShapeDtypeStruct((rows // relations, relations * width), jnp.bfloat16),
        in_specs=[
            pl.BlockSpec((group, depth), lambda i: (i, 0)),
            pl.BlockSpec((depth, width), lambda i: (0, 0)),
            pl.BlockSpec((group, width), lambda i: (i, 0)),
            pl.BlockSpec((group, 1), lambda i: (i, 0)),
        ],
        out_specs=pl.BlockSpec((group // relations, relations * width), lambda i: (i, 0)),
        compiler_params=params(40),
        cost_estimate=estimate(2 * rows * depth * width, 2 * rows * depth),
        name="remote",
    )(counts, table, pooled, degree)


def in_hbm(*arrays):
    return [pltpu.with_memory_space_constraint(array, pltpu.HBM) for array in arrays]


def start_all(sems, *pairs):
    copies = [pltpu.make_async_copy(a, b, sems.at[i]) for i, (a, b) in enumerate(pairs)]
    for copy in copies:
        copy.start()
    return copies


def wait_all(copies):
    for copy in copies:
        copy.wait()


def build_body(
    tile_ref, count_ref, source_hbm, relation_hbm, target_hbm, own_hbm,
    local_ref, remote_ref, pooled_ref, degree_hbm,
    source_ref, relation_ref, target_ref, own_ref, degree_ref,
    local_v, remote_v, pooled_v, head_ref, next_ref, list_ref, slot_ref, code_ref, low_ref, sum_ref,
    sems, in_sems, *, tiles, relations, locals_, pieces,
):
    slots = WIN * relations
    rows = pieces * slots
    inputs = start_all(
        in_sems,
        (source_hbm, source_ref),
        (relation_hbm, relation_ref),
        (target_hbm, target_ref),
        (own_hbm, own_ref),
    )
    wait_all(inputs)
    code_edges(source_ref, relation_ref, target_ref, slot_ref, code_ref, low_ref, relations)
    link_blocks(tile_ref, count_ref, head_ref, next_ref, tiles)
    head_ref[tiles] = -1
    degree_ref[tiles // GROUP] = jnp.zeros((slots, GROUP), jnp.float32)
    counted = functools.partial(
        count_blocks, slot_ref=slot_ref, code_ref=code_ref, low_ref=low_ref, rows=rows, slots=slots
    )

    def place(t, piece):
        row = pl.multiple_of(t * slots, slots)
        ref, at = (local_v, piece) if piece < locals_ else (remote_v, piece - locals_)
        return ref, (pl.ds(row, slots), pl.ds(at * CHUNK, CHUNK))

    def part(counts, piece):
        return counts[piece * slots : (piece + 1) * slots]

    def add(t, blocks):
        counts, degree = counted(blocks)
        for piece in range(pieces):
            ref, where = place(t, piece)
            total = ref[where].astype(jnp.float32) + part(counts, piece)
            ref[where] = total.astype(jnp.bfloat16)
        add_degree(t, degree)

    def add_degree(t, degree):
        lanes = lax.broadcasted_iota(jnp.int32, (slots, GROUP), 1)
        degree_ref[t // GROUP] += jnp.where(lanes == t % GROUP, degree, 0.0)

    def copy_tile(t):
        some = pl.ds(pl.multiple_of(t * slots, slots), slots)
        pltpu.make_async_copy(local_v.at[some], local_ref.at[some], sems.at[0]).start()
        pltpu.make_async_copy(remote_v.at[some], remote_ref.at[some], sems.at[1]).start()

    def base(i, carry):
        afters = []
        for u in range(GROUP):
            t = i * GROUP + u
            first = head_ref[t]
            second, after = pair_of(first, next_ref)
            counts, degree = counted([first, second])
            for piece in range(pieces):
                ref, where = place(t, piece)
                ref[where] = part(counts, piece).astype(jnp.bfloat16)
            degree_ref[i, :, pl.ds(u, 1)] = degree
            head_ref[t] = after
            afters.append(after)
        for u, after in enumerate(afters):

            @pl.when(after < 0)
            def _():
                copy_tile(i * GROUP + u)

        return carry

    lax.fori_loop(0, tiles // GROUP, base, 0)

    def sort_tile(t, sizes):
        short, mid, long = sizes
        first = head_ref[t]
        _, third = pair_of(first, next_ref)
        _, fifth = pair_of(third, next_ref)
        list_ref[0, short] = t
        list_ref[1, mid] = t
        list_ref[2, long] = t
        more = first >= 0
        return (
            short + jnp.where(more & (third < 0), 1, 0),
            mid + jnp.where(more & (third >= 0) & (fifth < 0), 1, 0),
            long + jnp.where(more & (fifth >= 0), 1, 0),
        )

    zero = jnp.int32(0)
    short, mid, long = lax.fori_loop(0, tiles, sort_tile, (zero, zero, zero))
    for k in range(4):
        list_ref[0, short + k] = tiles
        list_ref[1, mid + k] = tiles

    def add_short(j, carry):
        for k in range(4):
            t = list_ref[0, 4 * j + k]
            first = head_ref[t]
            second, _ = pair_of(first, next_ref)
            add(t, [first, second])
        for k in range(4):
            t = list_ref[0, 4 * j + k]

            @pl.when(t < tiles)
            def _():
                copy_tile(t)

        return carry

    def add_mid(j, carry):
        for k in range(2):
            t = list_ref[1, 2 * j + k]
            first = head_ref[t]
            second, third = pair_of(first, next_ref)
            fourth, _ = pair_of(third, next_ref)
            add(t, [first, second, third, fourth])
        for k in range(2):
            t = list_ref[1, 2 * j + k]

            @pl.when(t < tiles)
            def _():
                copy_tile(t)

        return carry

    def add_long(j, carry):
        t = list_ref[2, j]
        for piece in range(pieces):
            ref, where = place(t, piece)
            sum_ref[pl.ds(piece * slots, slots), :] = ref[where].astype(jnp.float32)

        def step(first):
            second, after = pair_of(first, next_ref)
            counts, degree = counted([first, second])
            sum_ref[...] += counts
            add_degree(t, degree)
            return after

        lax.while_loop(lambda first: first >= 0, step, head_ref[t])
        for piece in range(pieces):
            ref, where = place(t, piece)
            ref[where] = sum_ref[pl.ds(piece * slots, slots), :].astype(jnp.bfloat16)
        copy_tile(t)
        return carry

    lax.fori_loop(0, (short + 3) // 4, add_short, 0)
    lax.fori_loop(0, (mid + 1) // 2, add_mid, 0)
    lax.fori_loop(0, long, add_long, 0)

    def pool_own(i, carry):
        some = pl.ds(pl.multiple_of(i * GROUP * slots, GROUP * slots), GROUP * slots)
        pooled_v[some, :] = jnp.dot(
            local_v[some, :], own_ref[...], preferred_element_type=jnp.float32
        ).astype(jnp.bfloat16)
        pltpu.make_async_copy(pooled_v.at[some], pooled_ref.at[some], sems.at[2]).start()
        return carry

    lax.fori_loop(0, tiles // GROUP, pool_own, 0)
    every = pl.ds(0, tiles * slots)
    pltpu.make_async_copy(local_v.at[every], local_ref, sems.at[0]).wait()
    pltpu.make_async_copy(remote_v.at[every], remote_ref, sems.at[1]).wait()
    pltpu.make_async_copy(pooled_v, pooled_ref, sems.at[2]).wait()
    pltpu.sync_copy(degree_ref.at[pl.ds(0, tiles // GROUP)], degree_hbm)


def build(tile_of, count, source, relation, target, own, *, relations, remote_rows):
    blocks, block_width = source.shape
    node_rows, width = own.shape
    tiles, slots = node_rows // WIN, WIN * relations
    rows = tiles * slots
    locals_, remotes = node_rows // CHUNK, remote_rows // CHUNK
    pieces = locals_ + remotes
    vmem = pl.BlockSpec(memory_space=pltpu.VMEM)
    smem = pl.BlockSpec(memory_space=pltpu.SMEM)
    hbm = pl.BlockSpec(memory_space=pltpu.HBM)
    return pl.pallas_call(
        functools.partial(
            build_body, tiles=tiles, relations=relations, locals_=locals_, pieces=pieces
        ),
        out_shape=[
            pltpu.HBM((rows, node_rows), jnp.bfloat16),
            pltpu.HBM((rows, remote_rows), jnp.bfloat16),
            pltpu.HBM((rows, width), jnp.bfloat16),
            pltpu.HBM((tiles // GROUP, slots, GROUP), jnp.float32),
        ],
        in_specs=[smem, smem] + [hbm] * 4,
        out_specs=[hbm] * 4,
        scratch_shapes=[
            pltpu.VMEM((blocks, block_width), jnp.int32),
            pltpu.VMEM((blocks, block_width), jnp.int32),
            pltpu.VMEM((blocks, block_width), jnp.int32),
            pltpu.VMEM((node_rows, width), jnp.bfloat16),
            pltpu.VMEM((tiles // GROUP + 1, slots, GROUP), jnp.float32),
            pltpu.VMEM((rows + slots, node_rows), jnp.bfloat16),
            pltpu.VMEM((rows + slots, remote_rows), jnp.bfloat16),
            pltpu.VMEM((rows, width), jnp.bfloat16),
            pltpu.SMEM((tiles + 1,), jnp.int32),
            pltpu.SMEM((blocks,), jnp.int32),
            pltpu.SMEM((3, tiles + 8), jnp.int32),
            pltpu.VMEM((blocks, block_width), jnp.int32),
            pltpu.VMEM((blocks, block_width), jnp.int32),
            pltpu.VMEM((blocks, block_width), jnp.int32),
            pltpu.VMEM((pieces * slots, CHUNK), jnp.float32),
            pltpu.SemaphoreType.DMA((3,)),
            pltpu.SemaphoreType.DMA((4,)),
        ],
        compiler_params=params(58),
        cost_estimate=estimate(
            4 * (tiles + blocks // 4) * pieces * slots * CHUNK * block_width
            + 2 * rows * node_rows * width,
            2 * rows * pieces * CHUNK,
        ),
        name="build",
    )(tile_of, count, *in_hbm(source, relation, target, own))


def pool_groups(
    counts_ref, counts_v, sems, table_ref, degree_ref, mean_ref, relations, begun, extra=None
):
    size = GROUP * WIN * relations
    groups = counts_ref.shape[0] // size

    def copies(i):
        some = pl.ds(pl.multiple_of(i * size, size), size)
        found = [pltpu.make_async_copy(counts_ref.at[some], counts_v.at[some], sems.at[0, i])]
        if extra is not None:
            found.append(pltpu.make_async_copy(extra[0].at[some], extra[1].at[some], sems.at[1, i]))
        return found

    def begin(i, carry):
        for copy in copies(i):
            copy.start()
        return carry

    def step(i, carry):
        for copy in copies(i):
            copy.wait()
        some = pl.ds(pl.multiple_of(i * size, size), size)
        total = jnp.dot(counts_v[some, :], table_ref[...], preferred_element_type=jnp.float32)
        if extra is not None:
            total += extra[1][some, :].astype(jnp.float32)
        share = 1.0 / jnp.maximum(degree_ref[i], 1.0)
        slots = WIN * relations
        for u in range(GROUP):
            mean = total[u * slots : (u + 1) * slots] * share[:, u : u + 1]
            put_means(mean.astype(jnp.bfloat16), mean_ref, i * GROUP + u, relations)
        return carry

    lax.fori_loop(0, groups, begin, 0)
    begun()
    lax.fori_loop(0, groups, step, 0)


def copy_table(incoming_ref, table_ref, slot):
    for device in range(incoming_ref.shape[0]):
        table_ref[device * slot : (device + 1) * slot, :] = incoming_ref[device, :slot, :]


def pool_body(
    counts_ref, pooled_ref, incoming_ref, degree_hbm, mean_ref,
    counts_v, pooled_v, table_v, degree_v, sems, in_sems, *, relations, slot,
):
    inputs = start_all(in_sems, (degree_hbm, degree_v))

    def begun():
        copy_table(incoming_ref, table_v, slot)
        wait_all(inputs)

    pool_groups(
        counts_ref, counts_v, sems, table_v, degree_v, mean_ref, relations, begun,
        extra=(pooled_ref, pooled_v),
    )


def pool(counts, pooled, incoming, degree, *, relations, slot):
    rows, depth = counts.shape
    width = incoming.shape[2]
    vmem = pl.BlockSpec(memory_space=pltpu.VMEM)
    hbm = pl.BlockSpec(memory_space=pltpu.HBM)
    return pl.pallas_call(
        functools.partial(pool_body, relations=relations, slot=slot),
        out_shape=jax.ShapeDtypeStruct((rows // relations, relations * width), jnp.bfloat16),
        in_specs=[hbm, hbm, vmem, hbm],
        out_specs=vmem,
        scratch_shapes=[
            pltpu.VMEM(counts.shape, counts.dtype),
            pltpu.VMEM(pooled.shape, pooled.dtype),
            pltpu.VMEM((depth, width), jnp.bfloat16),
            pltpu.VMEM(degree.shape, degree.dtype),
            pltpu.SemaphoreType.DMA((2, degree.shape[0])),
            pltpu.SemaphoreType.DMA((1,)),
        ],
        compiler_params=params(44),
        cost_estimate=estimate(2 * rows * depth * width, 2 * rows * depth),
        name="pool",
    )(*in_hbm(counts, pooled), incoming, *in_hbm(degree))


def pick_rows(send_ref, rows_ref, emit, done):
    devices, slot = send_ref.shape
    depth = rows_ref.shape[0]
    columns = send_ref[...].astype(jnp.float32).T.astype(jnp.int32)
    lanes = lax.broadcasted_iota(jnp.int32, (slot, depth), 1)
    step = 8
    for start in range(0, devices, step):
        chosen = jnp.concatenate(
            [
                jnp.where(columns[:, device : device + 1] == lanes, 1.0, 0.0).astype(jnp.bfloat16)
                for device in range(start, start + step)
            ],
            axis=0,
        )
        picked = jnp.dot(chosen, rows_ref[...], preferred_element_type=jnp.float32)
        for k in range(step):
            emit(start + k, picked[k * slot : (k + 1) * slot].astype(jnp.bfloat16))
        done(start, step)


def send_out(out_v, out_ref, sems, start, count):
    some = pl.ds(start, count)
    pltpu.make_async_copy(out_v.at[some], out_ref.at[some], sems.at[0]).start()


def middle_body(
    mean_ref, own_hbm, incoming_ref, swapped_ref, bias_hbm, send_hbm,
    hidden_hbm, out_ref, self_hbm,
    own_v, bias_v, send_v, hidden_v, out_v, self_v, weights_v, sems, in_sems,
    *, relations, slot,
):
    inputs = start_all(in_sems, (own_hbm, own_v), (bias_hbm, bias_v), (send_hbm, send_v))
    width = own_v.shape[1]
    half = relations // 2
    devices = incoming_ref.shape[0]
    piece = width // devices
    block = (half + 1) * width
    for device in range(devices):
        for m in range(half + 1):
            at = m * width + device * piece
            weights_v[at : at + piece, :] = incoming_ref[
                device, slot + m * piece : slot + (m + 1) * piece, :
            ]
            weights_v[block + at : block + at + piece, :] = swapped_ref[
                device, m * piece : (m + 1) * piece, :
            ]
    side = lax.axis_index("dom") & 1
    mine_at = pl.multiple_of(side * (half * width), width)
    other_at = pl.multiple_of((1 - side) * (half * width), width)
    own_at = pl.multiple_of(half * width + side * block, width)
    next_at = pl.multiple_of(half * width + (1 - side) * block, width)
    self_v[...] = weights_v[pl.ds(next_at, width), :]
    total = jnp.dot(
        mean_ref[:, pl.ds(mine_at, half * width)],
        weights_v[: half * width, :],
        preferred_element_type=jnp.float32,
    )
    total += jnp.dot(
        mean_ref[:, pl.ds(other_at, half * width)],
        weights_v[block : block + half * width, :],
        preferred_element_type=jnp.float32,
    )
    wait_all(inputs)
    total += jnp.dot(
        own_v[...], weights_v[pl.ds(own_at, width), :], preferred_element_type=jnp.float32
    )
    hidden_v[...] = jnp.maximum(total + bias_v[...], 0.0).astype(jnp.bfloat16)
    outputs = [
        pltpu.make_async_copy(hidden_v, hidden_hbm, sems.at[1]),
        pltpu.make_async_copy(self_v, self_hbm, sems.at[2]),
    ]
    for copy in outputs:
        copy.start()

    def emit(device, picked):
        out_v[device, :, :] = picked

    pick_rows(send_v, hidden_v, emit, functools.partial(send_out, out_v, out_ref, sems))
    pltpu.make_async_copy(out_v, out_ref, sems.at[0]).wait()
    wait_all(outputs)


def middle(mean, own, incoming, swapped, bias, send, *, relations):
    nodes, width = own.shape
    devices, slot = send.shape
    vmem = pl.BlockSpec(memory_space=pltpu.VMEM)
    hbm = pl.BlockSpec(memory_space=pltpu.HBM)
    return pl.pallas_call(
        functools.partial(middle_body, relations=relations, slot=slot),
        out_shape=[
            pltpu.HBM((nodes, width), jnp.bfloat16),
            pltpu.HBM((devices, slot, width), jnp.bfloat16),
            pltpu.HBM((width, width), jnp.bfloat16),
        ],
        in_specs=[vmem, hbm, vmem, vmem, hbm, hbm],
        out_specs=[hbm] * 3,
        scratch_shapes=[
            pltpu.VMEM(own.shape, own.dtype),
            pltpu.VMEM(bias.shape, bias.dtype),
            pltpu.VMEM(send.shape, send.dtype),
            pltpu.VMEM((nodes, width), jnp.bfloat16),
            pltpu.VMEM((devices, slot, width), jnp.bfloat16),
            pltpu.VMEM((width, width), jnp.bfloat16),
            pltpu.VMEM(((relations + 2) * width, width), jnp.bfloat16),
            pltpu.SemaphoreType.DMA((3,)),
            pltpu.SemaphoreType.DMA((3,)),
        ],
        compiler_params=params(24),
        cost_estimate=estimate(2 * nodes * mean.shape[1] * width, 0),
        name="middle",
    )(mean, *in_hbm(own), incoming, swapped, *in_hbm(bias, send))


def weight_copies(pieces, weights_v, relations):
    width = weights_v.shape[1]
    ways = relations // EACH
    class_ = lax.axis_index("dom") & (ways - 1)

    def rows(k):
        relation = (class_ ^ (k // EACH)) + ways * (k % EACH)
        return weights_v.at[pl.ds(pl.multiple_of(relation * width, width), width)]

    return [(piece, rows(k)) for k, piece in enumerate(pieces)]


def first_body(
    counts_ref, own_hbm, degree_hbm, self_hbm, bias_hbm, *refs, relations
):
    pieces, refs = refs[:relations], refs[relations:]
    out_hbm, own_v, degree_v, self_v, bias_v, out_v, weights_v, counts_v, mean_v, sems, in_sems = refs
    inputs = start_all(in_sems, (own_hbm, own_v), (degree_hbm, degree_v))
    later = []

    def begun():
        later.extend(
            start_all(
                in_sems.at[pl.ds(2, 2 + relations)],
                (self_hbm, self_v),
                (bias_hbm, bias_v),
                *weight_copies(pieces, weights_v, relations),
            )
        )
        wait_all(inputs)

    pool_groups(counts_ref, counts_v, sems, own_v, degree_v, mean_v, relations, begun)
    wait_all(later)
    total = jnp.dot(mean_v[...], weights_v[...], preferred_element_type=jnp.float32)
    total += jnp.dot(own_v[...], self_v[...], preferred_element_type=jnp.float32)
    out_v[...] = total + bias_v[...]
    pltpu.sync_copy(out_v, out_hbm)


def first(counts, own, degree, self_weight, bias, pieces, *, relations):
    rows, depth = counts.shape
    nodes, width = own.shape
    hbm = pl.BlockSpec(memory_space=pltpu.HBM)
    return pl.pallas_call(
        functools.partial(first_body, relations=relations),
        out_shape=pltpu.HBM((nodes, width), jnp.float32),
        in_specs=[hbm] * (5 + relations),
        out_specs=hbm,
        scratch_shapes=[
            pltpu.VMEM(own.shape, own.dtype),
            pltpu.VMEM(degree.shape, degree.dtype),
            pltpu.VMEM(self_weight.shape, self_weight.dtype),
            pltpu.VMEM(bias.shape, bias.dtype),
            pltpu.VMEM((nodes, width), jnp.float32),
            pltpu.VMEM((relations * width, width), jnp.bfloat16),
            pltpu.VMEM(counts.shape, counts.dtype),
            pltpu.VMEM((nodes, relations * width), jnp.bfloat16),
            pltpu.SemaphoreType.DMA((1, degree.shape[0])),
            pltpu.SemaphoreType.DMA((4 + relations,)),
        ],
        compiler_params=params(44),
        cost_estimate=estimate(
            2 * rows * depth * width + 2 * nodes * relations * width * width, 2 * rows * depth
        ),
        name="first",
    )(*in_hbm(counts, own, degree, self_weight, bias, *pieces))


def last_body(counts_ref, table_ref, degree_hbm, partial_hbm, *refs, relations):
    pieces, refs = refs[:relations], refs[relations:]
    out_ref, degree_v, partial_v, weights_v, counts_v, mean_v, sems, in_sems = refs
    inputs = start_all(in_sems, (degree_hbm, degree_v))
    later = []

    def begun():
        later.extend(
            start_all(
                in_sems.at[pl.ds(1, 1 + relations)],
                (partial_hbm, partial_v),
                *weight_copies(pieces, weights_v, relations),
            )
        )
        wait_all(inputs)

    pool_groups(counts_ref, counts_v, sems, table_ref, degree_v, mean_v, relations, begun)
    wait_all(later)
    total = jnp.dot(mean_v[...], weights_v[...], preferred_element_type=jnp.float32)
    out_ref[...] = (total + partial_v[...]).astype(out_ref.dtype)


def last(counts, table, degree, partial, pieces, *, relations):
    rows, depth = counts.shape
    width = table.shape[1]
    nodes = rows // relations
    vmem = pl.BlockSpec(memory_space=pltpu.VMEM)
    hbm = pl.BlockSpec(memory_space=pltpu.HBM)
    return pl.pallas_call(
        functools.partial(last_body, relations=relations),
        out_shape=jax.ShapeDtypeStruct((nodes, width), jnp.bfloat16),
        in_specs=[hbm, vmem] + [hbm] * (2 + relations),
        out_specs=vmem,
        scratch_shapes=[
            pltpu.VMEM(degree.shape, degree.dtype),
            pltpu.VMEM(partial.shape, partial.dtype),
            pltpu.VMEM((relations * width, width), jnp.bfloat16),
            pltpu.VMEM(counts.shape, counts.dtype),
            pltpu.VMEM((nodes, relations * width), jnp.bfloat16),
            pltpu.SemaphoreType.DMA((1, degree.shape[0])),
            pltpu.SemaphoreType.DMA((2 + relations,)),
        ],
        compiler_params=params(44),
        cost_estimate=estimate(
            2 * rows * depth * width + 2 * nodes * relations * width * width, 2 * rows * depth
        ),
        name="last",
    )(*in_hbm(counts), table, *in_hbm(degree, partial, *pieces))


def pack_body(*refs):
    inputs_hbm, out_ref, inputs_v, (out_v, sems, in_sems) = refs[:8], refs[8], refs[9:17], refs[17:]
    inputs = start_all(in_sems, *zip(inputs_hbm, inputs_v))
    coef_first, coef_second, bases_first, bases_second, self_first, self_second, features, send = (
        inputs_v
    )
    relations, bases = coef_first.shape
    devices, slot = send.shape
    piece = self_first.shape[0]
    half = relations // 2
    wait_all(inputs)

    def mix(coef_ref, bases_ref):
        mixed = []
        for relation in range(relations):
            total = coef_ref[relation, 0] * bases_ref[0].astype(jnp.float32)
            for base in range(1, bases):
                total += coef_ref[relation, base] * bases_ref[base].astype(jnp.float32)
            mixed.append(total.astype(jnp.bfloat16))
        return mixed

    first = mix(coef_first, bases_first)
    second = mix(coef_second, bases_second)
    own = [self_first[...], self_second[...]]
    for device in range(devices):
        side = device % 2
        ways = relations // EACH
        rows = first[side * half : (side + 1) * half] + [own[side]] + second[device % ways :: ways]
        for k, value in enumerate(rows):
            at = slot + k * piece
            out_v[device, at : at + piece, :] = value

    def emit(device, picked):
        out_v[device, :slot, :] = picked

    pick_rows(send, features, emit, functools.partial(send_out, out_v, out_ref, sems))
    pltpu.make_async_copy(out_v, out_ref, sems.at[0]).wait()


def pack(features, send, bases_first, self_first, coef_first, bases_second, self_second, coef_second):
    devices, slot = send.shape
    relations = coef_first.shape[0]
    piece, width = self_first.shape
    hbm = pl.BlockSpec(memory_space=pltpu.HBM)
    shape = (devices, slot + (relations // 2 + 1 + EACH) * piece, width)
    args = (
        coef_first, coef_second, bases_first, bases_second, self_first, self_second, features, send,
    )
    return pl.pallas_call(
        pack_body,
        out_shape=pltpu.HBM(shape, jnp.bfloat16),
        in_specs=[hbm] * 8,
        out_specs=hbm,
        scratch_shapes=[
            *[pltpu.SMEM(a.shape, a.dtype) for a in args[:2]],
            *[pltpu.VMEM(a.shape, a.dtype) for a in args[2:]],
            pltpu.VMEM(shape, jnp.bfloat16),
            pltpu.SemaphoreType.DMA((1,)),
            pltpu.SemaphoreType.DMA((8,)),
        ],
        compiler_params=params(24),
        cost_estimate=estimate(2 * devices * slot * features.size, 0),
        name="pack",
    )(*in_hbm(*args))


def dense_body(mean_ref, own_ref, weights_ref, bias_ref, out_ref, *, last):
    depth = mean_ref.shape[1]
    total = jnp.dot(mean_ref[...], weights_ref[:depth], preferred_element_type=jnp.float32)
    total += jnp.dot(own_ref[...], weights_ref[depth:], preferred_element_type=jnp.float32)
    total += bias_ref[...]
    out_ref[...] = (total if last else jnp.maximum(total, 0.0)).astype(jnp.bfloat16)


def dense(mean, own, weights, bias, *, last):
    nodes, width = own.shape
    vmem = pl.BlockSpec(memory_space=pltpu.VMEM)
    return pl.pallas_call(
        functools.partial(dense_body, last=last),
        out_shape=jax.ShapeDtypeStruct((nodes, width), jnp.bfloat16),
        in_specs=[vmem] * 4,
        out_specs=vmem,
        compiler_params=params(16),
        cost_estimate=estimate(2 * nodes * mean.shape[1] * width, 0),
        name="dense",
    )(mean, own, weights, bias)


def mix_weights(bases, self_weight, coef):
    mixed = jnp.einsum(
        "rb,bij->rij", coef, bases.astype(jnp.float32), precision=lax.Precision.HIGHEST
    ).astype(jnp.bfloat16)
    return jnp.concatenate([mixed, self_weight[None]], axis=0)


def general_layers(
    features, edges, send, weights_first, weights_second, bias_first, bias_second, relations
):
    node_rows, width = features.shape
    devices, slot = send.shape
    half = relations // 2
    swap = [(i, i ^ 1) for i in range(devices)]
    side = lax.axis_index("dom") & 1

    def send_all(rows, weights):
        rows = rows[send]
        halves = [
            jnp.concatenate([weights[:half], weights[relations:]], axis=0).reshape(-1, width),
            jnp.concatenate([weights[half:relations], weights[relations:]], axis=0).reshape(-1, width),
        ]
        halves = jnp.broadcast_to(jnp.stack(halves)[None], (devices // 2, 2) + halves[0].shape)
        rows = jnp.concatenate([rows, halves.reshape(devices, -1, width)], axis=1)
        return lax.all_to_all(rows, "dom", split_axis=0, concat_axis=0, tiled=True)

    def take_all(incoming):
        mine = jnp.swapaxes(incoming[:, slot:].reshape(devices, half + 1, -1, width), 0, 1)
        mine = mine.reshape(-1, width)
        other = lax.ppermute(mine[: half * width], "dom", swap)
        mine, own = mine[: half * width], mine[half * width :]
        low, high = jnp.where(side == 0, mine, other), jnp.where(side == 0, other, mine)
        return incoming[:, :slot].reshape(-1, width), jnp.concatenate([low, high, own], axis=0)

    local, remote, degree = build_streamed_call(
        *edges, node_rows=node_rows, relations=relations, remote_rows=devices * slot
    )

    def layer(rows, weights, bias, last):
        incoming = send_all(rows, weights)
        pooled = local_streamed(local, rows, group=512)
        table, full = take_all(incoming)
        mean = remote_streamed(remote, table, pooled, degree, relations=relations, group=512)
        return dense(mean, rows, full, bias[None], last=last)

    hidden = layer(features, weights_first, bias_first, False)
    return layer(hidden, weights_second, bias_second, True)


def shards(
    features,
    edge_source,
    edge_relation,
    edge_target,
    block_count,
    send_list,
    bases_first,
    self_first,
    coef_first,
    bias_first,
    bases_second,
    self_second,
    coef_second,
    bias_second,
):
    node_rows, width = features.shape
    relations = coef_first.shape[0]
    devices, slot = send_list.shape[1:]
    remote_rows = devices * slot
    send = send_list[0]
    edges = (edge_target[0, :, 0], block_count, edge_source[0], edge_relation[0], edge_target[0])
    if 2 * node_rows * relations * (node_rows + remote_rows) > WHOLE_MAX:
        return general_layers(
            features,
            edges,
            send,
            mix_weights(bases_first, self_first, coef_first),
            mix_weights(bases_second, self_second, coef_second),
            bias_first,
            bias_second,
            relations,
        )
    outgoing = pack(
        features, send, bases_first, self_first, coef_first, bases_second, self_second, coef_second
    )
    incoming = lax.all_to_all(outgoing, "dom", split_axis=0, concat_axis=0, tiled=True)
    local, remote, pooled, degree = build(
        *edges, features, relations=relations, remote_rows=remote_rows
    )
    incoming, degree = lax.optimization_barrier((incoming, degree))

    def from_peer(array, mask):
        return lax.ppermute(array, "dom", [(i, i ^ mask) for i in range(devices)])

    next_at = slot + (relations // 2 + 1) * self_first.shape[0]
    swapped = from_peer(incoming[:, slot:next_at], 1)
    row = self_first.shape[0]
    pieces = {
        (0, e): incoming[:, next_at + e * row : next_at + (e + 1) * row].reshape(width, width)
        for e in range(EACH)
    }

    def widen(mask):
        for (k, e), piece in sorted(pieces.items()):
            pieces[k | mask, e] = from_peer(piece, mask)

    mask = relations // EACH // 2
    widen(mask)
    mean = pool(remote, pooled, incoming, degree, relations=relations, slot=slot)
    pieces, mean = lax.optimization_barrier((pieces, mean))
    mask //= 2
    widen(mask)
    hidden, picked, self_next = middle(
        mean, features, incoming, swapped, bias_first[None], send, relations=relations
    )
    table = lax.all_to_all(picked, "dom", split_axis=0, concat_axis=0, tiled=True)
    while mask > 1:
        mask //= 2
        widen(mask)
    pieces = [piece for _, piece in sorted(pieces.items())]
    partial = first(
        local, hidden, degree, self_next, bias_second[None], pieces, relations=relations
    )
    table, partial = lax.optimization_barrier((table, partial))
    return last(remote, table.reshape(-1, width), degree, partial, pieces, relations=relations)


def solution(mesh):
    placed = (
        P("dom", None),
        P("dom", None, None),
        P("dom", None, None),
        P("dom", None, None),
        P("dom"),
        P("dom", None, None),
        P(None, "dom", None),
        P("dom", None),
        P(),
        P(),
        P(None, "dom", None),
        P("dom", None),
        P(),
        P(),
    )
    return jax.shard_map(
        shards, mesh=mesh, in_specs=placed, out_specs=P("dom", None), check_vma=False
    )
```

```python
import functools

import jax
import jax.numpy as jnp
from jax import lax
from jax.experimental import pallas as pl
from jax.experimental.pallas import tpu as pltpu
from jax.sharding import PartitionSpec as P

WIN = 16
CHUNK = 512
GROUP = 8
EACH = 1
MIB = 1 << 20
WHOLE_MAX = 36 * MIB
CONTRACT_LANES = (((1,), (1,)), ((), ()))


def estimate(flops, nbytes):
    return pl.CostEstimate(flops=int(flops), bytes_accessed=int(nbytes), transcendentals=0)


def params(mib, **more):
    return pltpu.CompilerParams(vmem_limit_bytes=mib * MIB, **more)


def hot(rows, lanes):
    row_ids = lax.broadcasted_iota(jnp.int32, (rows, lanes.shape[1]), 0)
    return jnp.where(row_ids == lanes, 1.0, 0.0)


def code_edges(source_ref, relation_ref, target_ref, slot_ref, code_ref, low_ref, relations):
    slot = relation_ref[...] * WIN + (target_ref[...] & (WIN - 1))
    slot_ref[...] = slot
    code_ref[...] = (source_ref[...] // CHUNK) * (WIN * relations) + slot
    low_ref[...] = source_ref[...] & (CHUNK - 1)


def link_blocks(tile_ref, count_ref, head_ref, next_ref, tiles):
    def clear(t, carry):
        head_ref[t] = -1
        return carry

    lax.fori_loop(0, tiles, clear, 0)

    def link(b, carry):
        t = tile_ref[b] // WIN
        next_ref[b] = head_ref[t]
        head_ref[t] = b
        return carry

    lax.fori_loop(0, count_ref[0], link, 0)


def pair_of(first, next_ref):
    second = jnp.where(first >= 0, next_ref[jnp.maximum(first, 0)], -1)
    after = jnp.where(second >= 0, next_ref[jnp.maximum(second, 0)], -1)
    return second, after


def some_rows(ref, blocks):
    return jnp.concatenate(
        [jnp.where(b >= 0, ref[pl.ds(jnp.maximum(b, 0), 1), :], -1) for b in blocks], axis=1
    )


def count_blocks(blocks, slot_ref, code_ref, low_ref, rows, slots):
    left = hot(rows, some_rows(code_ref, blocks)).astype(jnp.bfloat16)
    right = hot(CHUNK, some_rows(low_ref, blocks)).astype(jnp.bfloat16)
    counts = lax.dot_general(left, right, CONTRACT_LANES, preferred_element_type=jnp.float32)
    degree = jnp.sum(hot(slots, some_rows(slot_ref, blocks)), axis=1, keepdims=True)
    return counts, degree


def put_counts(counts, local_ref, remote_ref, row, slots, locals_):
    for piece in range(counts.shape[0] // slots):
        part = counts[piece * slots : (piece + 1) * slots].astype(jnp.bfloat16)
        if piece < locals_:
            local_ref[pl.ds(row, slots), pl.ds(piece * CHUNK, CHUNK)] = part
        else:
            remote_ref[pl.ds(row, slots), pl.ds((piece - locals_) * CHUNK, CHUNK)] = part


def build_streamed(
    tile_ref, count_ref, source_ref, relation_ref, target_ref,
    local_ref, remote_ref, degree_ref,
    head_ref, next_ref, slot_ref, code_ref, low_ref, sum_ref,
    *, tiles, relations, locals_, pieces,
):
    slots = WIN * relations
    rows = pieces * slots
    t = pl.program_id(0)

    @pl.when(t == 0)
    def _():
        code_edges(source_ref, relation_ref, target_ref, slot_ref, code_ref, low_ref, relations)
        link_blocks(tile_ref, count_ref, head_ref, next_ref, tiles)

    sum_ref[...] = jnp.zeros_like(sum_ref)
    degree_ref[...] = jnp.zeros_like(degree_ref)

    def step(first):
        second, after = pair_of(first, next_ref)
        counts, degree = count_blocks([first, second], slot_ref, code_ref, low_ref, rows, slots)
        sum_ref[...] += counts
        degree_ref[...] += degree
        return after

    lax.while_loop(lambda first: first >= 0, step, head_ref[t])
    put_counts(sum_ref[...], local_ref, remote_ref, 0, slots, locals_)


def build_streamed_call(tile_of, count, source, relation, target, *, node_rows, relations, remote_rows):
    blocks, width = source.shape
    tiles, slots = node_rows // WIN, WIN * relations
    locals_, remotes = node_rows // CHUNK, remote_rows // CHUNK
    pieces = locals_ + remotes
    smem = pl.BlockSpec(memory_space=pltpu.SMEM)
    shapes = [
        ((tiles * slots, node_rows), jnp.bfloat16),
        ((tiles * slots, remote_rows), jnp.bfloat16),
        ((tiles * slots, 1), jnp.float32),
    ]
    whole = pl.BlockSpec((blocks, width), lambda t: (0, 0))
    return pl.pallas_call(
        functools.partial(
            build_streamed, tiles=tiles, relations=relations, locals_=locals_, pieces=pieces
        ),
        grid=(tiles,),
        out_shape=[jax.ShapeDtypeStruct(s, d) for s, d in shapes],
        in_specs=[smem, smem, whole, whole, whole],
        out_specs=[pl.BlockSpec((slots, s[1]), lambda t: (t, 0)) for s, _ in shapes],
        scratch_shapes=[
            pltpu.SMEM((tiles,), jnp.int32),
            pltpu.SMEM((blocks,), jnp.int32),
            pltpu.VMEM((blocks, width), jnp.int32),
            pltpu.VMEM((blocks, width), jnp.int32),
            pltpu.VMEM((blocks, width), jnp.int32),
            pltpu.VMEM((pieces * slots, CHUNK), jnp.float32),
        ],
        compiler_params=params(40),
        cost_estimate=estimate(
            4 * (tiles + blocks // 4) * pieces * slots * CHUNK * width,
            2 * tiles * slots * pieces * CHUNK,
        ),
        name="build",
    )(tile_of, count, source, relation, target)


def local_streamed_body(counts_ref, table_ref, pooled_ref):
    pooled_ref[...] = jnp.dot(
        counts_ref[...], table_ref[...], preferred_element_type=jnp.float32
    )


def local_streamed(counts, table, *, group):
    rows, depth = counts.shape
    width = table.shape[1]
    return pl.pallas_call(
        local_streamed_body,
        grid=(rows // group,),
        out_shape=jax.ShapeDtypeStruct((rows, width), jnp.float32),
        in_specs=[
            pl.BlockSpec((group, depth), lambda i: (i, 0)),
            pl.BlockSpec((depth, width), lambda i: (0, 0)),
        ],
        out_specs=pl.BlockSpec((group, width), lambda i: (i, 0)),
        compiler_params=params(40),
        cost_estimate=estimate(2 * rows * depth * width, 2 * rows * depth),
        name="local",
    )(counts, table)


def put_means(mean, mean_ref, first_tile, relations):
    slots = WIN * relations
    width = mean.shape[1]
    for tile in range(mean.shape[0] // slots):
        at = pl.multiple_of((first_tile + tile) * WIN, WIN)
        for relation in range(relations):
            start = tile * slots + relation * WIN
            mean_ref[pl.ds(at, WIN), pl.ds(relation * width, width)] = mean[start : start + WIN]


def remote_streamed_body(counts_ref, table_ref, pooled_ref, degree_ref, mean_ref, *, relations):
    total = pooled_ref[...] + jnp.dot(
        counts_ref[...], table_ref[...], preferred_element_type=jnp.float32
    )
    mean = total * (1.0 / jnp.maximum(degree_ref[...], 1.0))
    put_means(mean.astype(jnp.bfloat16), mean_ref, 0, relations)


def remote_streamed(counts, table, pooled, degree, *, relations, group):
    rows, depth = counts.shape
    width = table.shape[1]
    return pl.pallas_call(
        functools.partial(remote_streamed_body, relations=relations),
        grid=(rows // group,),
        out_shape=jax.ShapeDtypeStruct((rows // relations, relations * width), jnp.bfloat16),
        in_specs=[
            pl.BlockSpec((group, depth), lambda i: (i, 0)),
            pl.BlockSpec((depth, width), lambda i: (0, 0)),
            pl.BlockSpec((group, width), lambda i: (i, 0)),
            pl.BlockSpec((group, 1), lambda i: (i, 0)),
        ],
        out_specs=pl.BlockSpec((group // relations, relations * width), lambda i: (i, 0)),
        compiler_params=params(40),
        cost_estimate=estimate(2 * rows * depth * width, 2 * rows * depth),
        name="remote",
    )(counts, table, pooled, degree)


def in_vmem(array):
    return pltpu.with_memory_space_constraint(array, pltpu.VMEM)


def in_hbm(*arrays):
    return [pltpu.with_memory_space_constraint(array, pltpu.HBM) for array in arrays]


def start_all(sems, *pairs):
    copies = [pltpu.make_async_copy(a, b, sems.at[i]) for i, (a, b) in enumerate(pairs)]
    for copy in copies:
        copy.start()
    return copies


def wait_all(copies):
    for copy in copies:
        copy.wait()


def build_body(
    tile_ref, count_ref, source_hbm, relation_hbm, target_hbm, own_hbm,
    local_ref, remote_ref, pooled_ref, degree_hbm, ahead_ref,
    source_ref, relation_ref, target_ref, own_ref, degree_ref,
    local_v, remote_v, pooled_v, head_ref, next_ref, list_ref, slot_ref, code_ref, low_ref, sum_ref,
    sems, in_sems, *, tiles, relations, locals_, pieces,
):
    slots = WIN * relations
    rows = pieces * slots
    inputs = start_all(
        in_sems,
        (source_hbm, source_ref),
        (relation_hbm, relation_ref),
        (target_hbm, target_ref),
        (own_hbm, own_ref),
    )
    wait_all(inputs)
    code_edges(source_ref, relation_ref, target_ref, slot_ref, code_ref, low_ref, relations)
    link_blocks(tile_ref, count_ref, head_ref, next_ref, tiles)
    head_ref[tiles] = -1
    degree_ref[tiles // GROUP] = jnp.zeros((slots, GROUP), jnp.float32)
    counted = functools.partial(
        count_blocks, slot_ref=slot_ref, code_ref=code_ref, low_ref=low_ref, rows=rows, slots=slots
    )

    def place(t, piece):
        row = pl.multiple_of(t * slots, slots)
        ref, at = (local_v, piece) if piece < locals_ else (remote_v, piece - locals_)
        return ref, (pl.ds(row, slots), pl.ds(at * CHUNK, CHUNK))

    def part(counts, piece):
        return counts[piece * slots : (piece + 1) * slots]

    def add(t, blocks):
        counts, degree = counted(blocks)
        for piece in range(pieces):
            ref, where = place(t, piece)
            total = ref[where].astype(jnp.float32) + part(counts, piece)
            ref[where] = total.astype(jnp.bfloat16)
        add_degree(t, degree)

    def add_degree(t, degree):
        lanes = lax.broadcasted_iota(jnp.int32, (slots, GROUP), 1)
        degree_ref[t // GROUP] += jnp.where(lanes == t % GROUP, degree, 0.0)

    def copy_tile(t):
        some = pl.ds(pl.multiple_of(t * slots, slots), slots)
        pltpu.make_async_copy(local_v.at[some], local_ref.at[some], sems.at[0]).start()
        pltpu.make_async_copy(remote_v.at[some], remote_ref.at[some], sems.at[1]).start()

    def base(i, carry):
        afters = []
        for u in range(GROUP):
            t = i * GROUP + u
            first = head_ref[t]
            second, after = pair_of(first, next_ref)
            counts, degree = counted([first, second])
            for piece in range(pieces):
                ref, where = place(t, piece)
                ref[where] = part(counts, piece).astype(jnp.bfloat16)
            degree_ref[i, :, pl.ds(u, 1)] = degree
            head_ref[t] = after
            afters.append(after)
        for u, after in enumerate(afters):

            @pl.when(after < 0)
            def _():
                copy_tile(i * GROUP + u)

        return carry

    lax.fori_loop(0, tiles // GROUP, base, 0)

    def sort_tile(t, sizes):
        short, mid, long = sizes
        first = head_ref[t]
        _, third = pair_of(first, next_ref)
        _, fifth = pair_of(third, next_ref)
        list_ref[0, short] = t
        list_ref[1, mid] = t
        list_ref[2, long] = t
        more = first >= 0
        return (
            short + jnp.where(more & (third < 0), 1, 0),
            mid + jnp.where(more & (third >= 0) & (fifth < 0), 1, 0),
            long + jnp.where(more & (fifth >= 0), 1, 0),
        )

    zero = jnp.int32(0)
    short, mid, long = lax.fori_loop(0, tiles, sort_tile, (zero, zero, zero))
    for k in range(4):
        list_ref[0, short + k] = tiles
        list_ref[1, mid + k] = tiles

    def add_short(j, carry):
        for k in range(4):
            t = list_ref[0, 4 * j + k]
            first = head_ref[t]
            second, _ = pair_of(first, next_ref)
            add(t, [first, second])
        for k in range(4):
            t = list_ref[0, 4 * j + k]

            @pl.when(t < tiles)
            def _():
                copy_tile(t)

        return carry

    def add_mid(j, carry):
        for k in range(2):
            t = list_ref[1, 2 * j + k]
            first = head_ref[t]
            second, third = pair_of(first, next_ref)
            fourth, _ = pair_of(third, next_ref)
            add(t, [first, second, third, fourth])
        for k in range(2):
            t = list_ref[1, 2 * j + k]

            @pl.when(t < tiles)
            def _():
                copy_tile(t)

        return carry

    def add_long(j, carry):
        t = list_ref[2, j]
        for piece in range(pieces):
            ref, where = place(t, piece)
            sum_ref[pl.ds(piece * slots, slots), :] = ref[where].astype(jnp.float32)

        def step(first):
            second, after = pair_of(first, next_ref)
            counts, degree = counted([first, second])
            sum_ref[...] += counts
            add_degree(t, degree)
            return after

        lax.while_loop(lambda first: first >= 0, step, head_ref[t])
        for piece in range(pieces):
            ref, where = place(t, piece)
            ref[where] = sum_ref[pl.ds(piece * slots, slots), :].astype(jnp.bfloat16)
        copy_tile(t)
        return carry

    lax.fori_loop(0, (short + 3) // 4, add_short, 0)
    lax.fori_loop(0, (mid + 1) // 2, add_mid, 0)
    lax.fori_loop(0, long, add_long, 0)

    def pool_own(i, carry):
        some = pl.ds(pl.multiple_of(i * GROUP * slots, GROUP * slots), GROUP * slots)
        pooled_v[some, :] = jnp.dot(
            local_v[some, :], own_ref[...], preferred_element_type=jnp.float32
        ).astype(jnp.bfloat16)
        pltpu.make_async_copy(pooled_v.at[some], pooled_ref.at[some], sems.at[2]).start()
        return carry

    lax.fori_loop(0, tiles // GROUP, pool_own, 0)
    ahead_ref[...] = remote_v[: GROUP * slots, :]
    every = pl.ds(0, tiles * slots)
    pltpu.make_async_copy(local_v.at[every], local_ref, sems.at[0]).wait()
    pltpu.make_async_copy(remote_v.at[every], remote_ref, sems.at[1]).wait()
    pltpu.make_async_copy(pooled_v, pooled_ref, sems.at[2]).wait()
    pltpu.sync_copy(degree_ref.at[pl.ds(0, tiles // GROUP)], degree_hbm)


def build(tile_of, count, source, relation, target, own, *, relations, remote_rows):
    blocks, block_width = source.shape
    node_rows, width = own.shape
    tiles, slots = node_rows // WIN, WIN * relations
    rows = tiles * slots
    locals_, remotes = node_rows // CHUNK, remote_rows // CHUNK
    pieces = locals_ + remotes
    vmem = pl.BlockSpec(memory_space=pltpu.VMEM)
    smem = pl.BlockSpec(memory_space=pltpu.SMEM)
    hbm = pl.BlockSpec(memory_space=pltpu.HBM)
    return pl.pallas_call(
        functools.partial(
            build_body, tiles=tiles, relations=relations, locals_=locals_, pieces=pieces
        ),
        out_shape=[
            pltpu.HBM((rows, node_rows), jnp.bfloat16),
            pltpu.HBM((rows, remote_rows), jnp.bfloat16),
            pltpu.HBM((rows, width), jnp.bfloat16),
            pltpu.HBM((tiles // GROUP, slots, GROUP), jnp.float32),
            pltpu.VMEM((GROUP * slots, remote_rows), jnp.bfloat16),
        ],
        in_specs=[smem, smem] + [hbm] * 4,
        out_specs=[hbm] * 4 + [pl.BlockSpec(memory_space=pltpu.VMEM)],
        scratch_shapes=[
            pltpu.VMEM((blocks, block_width), jnp.int32),
            pltpu.VMEM((blocks, block_width), jnp.int32),
            pltpu.VMEM((blocks, block_width), jnp.int32),
            pltpu.VMEM((node_rows, width), jnp.bfloat16),
            pltpu.VMEM((tiles // GROUP + 1, slots, GROUP), jnp.float32),
            pltpu.VMEM((rows + slots, node_rows), jnp.bfloat16),
            pltpu.VMEM((rows + slots, remote_rows), jnp.bfloat16),
            pltpu.VMEM((rows, width), jnp.bfloat16),
            pltpu.SMEM((tiles + 1,), jnp.int32),
            pltpu.SMEM((blocks,), jnp.int32),
            pltpu.SMEM((3, tiles + 8), jnp.int32),
            pltpu.VMEM((blocks, block_width), jnp.int32),
            pltpu.VMEM((blocks, block_width), jnp.int32),
            pltpu.VMEM((blocks, block_width), jnp.int32),
            pltpu.VMEM((pieces * slots, CHUNK), jnp.float32),
            pltpu.SemaphoreType.DMA((3,)),
            pltpu.SemaphoreType.DMA((4,)),
        ],
        compiler_params=params(58),
        cost_estimate=estimate(
            4 * (tiles + blocks // 4) * pieces * slots * CHUNK * block_width
            + 2 * rows * node_rows * width,
            2 * rows * pieces * CHUNK,
        ),
        name="build",
    )(tile_of, count, *in_hbm(source, relation, target, own))


def pool_groups(
    counts_ref, counts_v, sems, table_ref, degree_ref, mean_ref, relations, begun, extra=None, ahead=None
):
    slots = WIN * relations
    size = GROUP * slots
    groups = counts_ref.shape[0] // size
    held = 0 if ahead is None else 1

    def rows(i):
        return pl.ds(pl.multiple_of(i * size, size), size)

    def count_copy(i):
        return pltpu.make_async_copy(counts_ref.at[rows(i)], counts_v.at[rows(i)], sems.at[0, i])

    def extra_copy(i):
        return pltpu.make_async_copy(extra[0].at[rows(i)], extra[1].at[rows(i)], sems.at[1, i])

    def begin(i, carry):
        count_copy(i).start()
        if extra is not None:
            extra_copy(i).start()
        return carry

    def finish(i, total):
        if extra is not None:
            extra_copy(i).wait()
            total += extra[1][rows(i), :].astype(jnp.float32)
        share = 1.0 / jnp.maximum(degree_ref[i], 1.0)
        for u in range(GROUP):
            mean = total[u * slots : (u + 1) * slots] * share[:, u : u + 1]
            put_means(mean.astype(jnp.bfloat16), mean_ref, i * GROUP + u, relations)

    def step(i, carry):
        count_copy(i).wait()
        finish(
            i, jnp.dot(counts_v[rows(i), :], table_ref[...], preferred_element_type=jnp.float32)
        )
        return carry

    if held and extra is not None:
        extra_copy(0).start()
    lax.fori_loop(held, groups, begin, 0)
    begun()
    if held:
        finish(0, jnp.dot(ahead[...], table_ref[...], preferred_element_type=jnp.float32))
    lax.fori_loop(held, groups, step, 0)


def copy_table(incoming_ref, table_ref, slot):
    for device in range(incoming_ref.shape[0]):
        table_ref[device * slot : (device + 1) * slot, :] = incoming_ref[device, :slot, :]


def pool_body(
    counts_ref, pooled_ref, incoming_ref, degree_hbm, ahead_ref, mean_ref,
    counts_v, pooled_v, table_v, degree_v, sems, in_sems, *, relations, slot,
):
    inputs = start_all(in_sems, (degree_hbm, degree_v))

    def begun():
        copy_table(incoming_ref, table_v, slot)
        wait_all(inputs)

    pool_groups(
        counts_ref, counts_v, sems, table_v, degree_v, mean_ref, relations, begun,
        extra=(pooled_ref, pooled_v), ahead=ahead_ref,
    )


def pool(counts, pooled, incoming, degree, ahead, *, relations, slot):
    rows, depth = counts.shape
    width = incoming.shape[2]
    vmem = pl.BlockSpec(memory_space=pltpu.VMEM)
    hbm = pl.BlockSpec(memory_space=pltpu.HBM)
    return pl.pallas_call(
        functools.partial(pool_body, relations=relations, slot=slot),
        out_shape=jax.ShapeDtypeStruct((rows // relations, relations * width), jnp.bfloat16),
        in_specs=[hbm, hbm, vmem, hbm, vmem],
        out_specs=vmem,
        scratch_shapes=[
            pltpu.VMEM(counts.shape, counts.dtype),
            pltpu.VMEM(pooled.shape, pooled.dtype),
            pltpu.VMEM((depth, width), jnp.bfloat16),
            pltpu.VMEM(degree.shape, degree.dtype),
            pltpu.SemaphoreType.DMA((2, degree.shape[0])),
            pltpu.SemaphoreType.DMA((1,)),
        ],
        compiler_params=params(44),
        cost_estimate=estimate(2 * rows * depth * width, 2 * rows * depth),
        name="pool",
    )(*in_hbm(counts, pooled), incoming, *in_hbm(degree), in_vmem(ahead))


def pick_rows(send_ref, rows_ref, emit, done):
    devices, slot = send_ref.shape
    depth = rows_ref.shape[0]
    columns = send_ref[...].astype(jnp.float32).T.astype(jnp.int32)
    lanes = lax.broadcasted_iota(jnp.int32, (slot, depth), 1)
    step = 8
    for start in range(0, devices, step):
        chosen = jnp.concatenate(
            [
                jnp.where(columns[:, device : device + 1] == lanes, 1.0, 0.0).astype(jnp.bfloat16)
                for device in range(start, start + step)
            ],
            axis=0,
        )
        picked = jnp.dot(chosen, rows_ref[...], preferred_element_type=jnp.float32)
        for k in range(step):
            emit(start + k, picked[k * slot : (k + 1) * slot].astype(jnp.bfloat16))
        done(start, step)


def send_out(out_v, out_ref, sems, start, count):
    some = pl.ds(start, count)
    pltpu.make_async_copy(out_v.at[some], out_ref.at[some], sems.at[0]).start()


def middle_body(
    mean_ref, own_hbm, incoming_ref, swapped_ref, bias_hbm, send_hbm,
    hidden_hbm, out_ref, self_hbm,
    own_v, bias_v, send_v, hidden_v, out_v, self_v, weights_v, sems, in_sems,
    *, relations, slot,
):
    inputs = start_all(in_sems, (own_hbm, own_v), (bias_hbm, bias_v), (send_hbm, send_v))
    width = own_v.shape[1]
    half = relations // 2
    devices = incoming_ref.shape[0]
    piece = width // devices
    block = (half + 1) * width
    for device in range(devices):
        for m in range(half + 1):
            at = m * width + device * piece
            weights_v[at : at + piece, :] = incoming_ref[
                device, slot + m * piece : slot + (m + 1) * piece, :
            ]
            weights_v[block + at : block + at + piece, :] = swapped_ref[
                device, m * piece : (m + 1) * piece, :
            ]
    side = lax.axis_index("dom") & 1
    mine_at = pl.multiple_of(side * (half * width), width)
    other_at = pl.multiple_of((1 - side) * (half * width), width)
    own_at = pl.multiple_of(half * width + side * block, width)
    next_at = pl.multiple_of(half * width + (1 - side) * block, width)
    self_v[...] = weights_v[pl.ds(next_at, width), :]
    total = jnp.dot(
        mean_ref[:, pl.ds(mine_at, half * width)],
        weights_v[: half * width, :],
        preferred_element_type=jnp.float32,
    )
    total += jnp.dot(
        mean_ref[:, pl.ds(other_at, half * width)],
        weights_v[block : block + half * width, :],
        preferred_element_type=jnp.float32,
    )
    wait_all(inputs)
    total += jnp.dot(
        own_v[...], weights_v[pl.ds(own_at, width), :], preferred_element_type=jnp.float32
    )
    hidden_v[...] = jnp.maximum(total + bias_v[...], 0.0).astype(jnp.bfloat16)
    outputs = [
        pltpu.make_async_copy(hidden_v, hidden_hbm, sems.at[1]),
        pltpu.make_async_copy(self_v, self_hbm, sems.at[2]),
    ]
    for copy in outputs:
        copy.start()

    def emit(device, picked):
        out_v[device, :, :] = picked

    pick_rows(send_v, hidden_v, emit, functools.partial(send_out, out_v, out_ref, sems))
    pltpu.make_async_copy(out_v, out_ref, sems.at[0]).wait()
    wait_all(outputs)


def middle(mean, own, incoming, swapped, bias, send, *, relations):
    nodes, width = own.shape
    devices, slot = send.shape
    vmem = pl.BlockSpec(memory_space=pltpu.VMEM)
    hbm = pl.BlockSpec(memory_space=pltpu.HBM)
    return pl.pallas_call(
        functools.partial(middle_body, relations=relations, slot=slot),
        out_shape=[
            pltpu.HBM((nodes, width), jnp.bfloat16),
            pltpu.HBM((devices, slot, width), jnp.bfloat16),
            pltpu.HBM((width, width), jnp.bfloat16),
        ],
        in_specs=[vmem, hbm, vmem, vmem, hbm, hbm],
        out_specs=[hbm] * 3,
        scratch_shapes=[
            pltpu.VMEM(own.shape, own.dtype),
            pltpu.VMEM(bias.shape, bias.dtype),
            pltpu.VMEM(send.shape, send.dtype),
            pltpu.VMEM((nodes, width), jnp.bfloat16),
            pltpu.VMEM((devices, slot, width), jnp.bfloat16),
            pltpu.VMEM((width, width), jnp.bfloat16),
            pltpu.VMEM(((relations + 2) * width, width), jnp.bfloat16),
            pltpu.SemaphoreType.DMA((3,)),
            pltpu.SemaphoreType.DMA((3,)),
        ],
        compiler_params=params(24),
        cost_estimate=estimate(2 * nodes * mean.shape[1] * width, 0),
        name="middle",
    )(mean, *in_hbm(own), incoming, swapped, *in_hbm(bias, send))


def weight_copies(pieces, weights_v, relations):
    width = weights_v.shape[1]
    ways = relations // EACH
    class_ = lax.axis_index("dom") & (ways - 1)

    def rows(k):
        relation = (class_ ^ (k // EACH)) + ways * (k % EACH)
        return weights_v.at[pl.ds(pl.multiple_of(relation * width, width), width)]

    return [(piece, rows(k)) for k, piece in enumerate(pieces)]


def first_body(
    counts_ref, remote_ref, own_hbm, degree_hbm, self_hbm, bias_hbm, *refs, relations
):
    pieces, refs = refs[:relations], refs[relations:]
    out_hbm, ahead_ref, *refs = refs
    own_v, degree_v, self_v, bias_v, out_v, weights_v, counts_v, mean_v, sems, in_sems = refs
    inputs = start_all(in_sems, (own_hbm, own_v), (degree_hbm, degree_v))
    later = []

    def begun():
        later.extend(
            start_all(
                in_sems.at[pl.ds(2, 3 + relations)],
                (remote_ref.at[pl.ds(0, ahead_ref.shape[0])], ahead_ref),
                (self_hbm, self_v),
                (bias_hbm, bias_v),
                *weight_copies(pieces, weights_v, relations),
            )
        )
        wait_all(inputs)

    pool_groups(counts_ref, counts_v, sems, own_v, degree_v, mean_v, relations, begun)
    wait_all(later)
    total = jnp.dot(mean_v[...], weights_v[...], preferred_element_type=jnp.float32)
    total += jnp.dot(own_v[...], self_v[...], preferred_element_type=jnp.float32)
    out_v[...] = total + bias_v[...]
    pltpu.sync_copy(out_v, out_hbm)


def first(counts, remote, own, degree, self_weight, bias, pieces, *, relations):
    rows, depth = counts.shape
    nodes, width = own.shape
    hbm = pl.BlockSpec(memory_space=pltpu.HBM)
    return pl.pallas_call(
        functools.partial(first_body, relations=relations),
        out_shape=[
            pltpu.HBM((nodes, width), jnp.float32),
            pltpu.VMEM((GROUP * WIN * relations, remote.shape[1]), jnp.bfloat16),
        ],
        in_specs=[hbm] * (6 + relations),
        out_specs=[hbm, pl.BlockSpec(memory_space=pltpu.VMEM)],
        scratch_shapes=[
            pltpu.VMEM(own.shape, own.dtype),
            pltpu.VMEM(degree.shape, degree.dtype),
            pltpu.VMEM(self_weight.shape, self_weight.dtype),
            pltpu.VMEM(bias.shape, bias.dtype),
            pltpu.VMEM((nodes, width), jnp.float32),
            pltpu.VMEM((relations * width, width), jnp.bfloat16),
            pltpu.VMEM(counts.shape, counts.dtype),
            pltpu.VMEM((nodes, relations * width), jnp.bfloat16),
            pltpu.SemaphoreType.DMA((1, degree.shape[0])),
            pltpu.SemaphoreType.DMA((5 + relations,)),
        ],
        compiler_params=params(44),
        cost_estimate=estimate(
            2 * rows * depth * width + 2 * nodes * relations * width * width, 2 * rows * depth
        ),
        name="first",
    )(*in_hbm(counts, remote, own, degree, self_weight, bias, *pieces))


def last_body(counts_ref, table_ref, ahead_ref, degree_hbm, partial_hbm, *refs, relations):
    pieces, refs = refs[:relations], refs[relations:]
    out_ref, degree_v, partial_v, weights_v, counts_v, mean_v, sems, in_sems = refs
    inputs = start_all(in_sems, (degree_hbm, degree_v))
    later = []

    def begun():
        later.extend(
            start_all(
                in_sems.at[pl.ds(1, 1 + relations)],
                (partial_hbm, partial_v),
                *weight_copies(pieces, weights_v, relations),
            )
        )
        wait_all(inputs)

    pool_groups(
        counts_ref, counts_v, sems, table_ref, degree_v, mean_v, relations, begun, ahead=ahead_ref
    )
    wait_all(later)
    total = jnp.dot(mean_v[...], weights_v[...], preferred_element_type=jnp.float32)
    out_ref[...] = (total + partial_v[...]).astype(out_ref.dtype)


def last(counts, table, ahead, degree, partial, pieces, *, relations):
    rows, depth = counts.shape
    width = table.shape[1]
    nodes = rows // relations
    vmem = pl.BlockSpec(memory_space=pltpu.VMEM)
    hbm = pl.BlockSpec(memory_space=pltpu.HBM)
    return pl.pallas_call(
        functools.partial(last_body, relations=relations),
        out_shape=jax.ShapeDtypeStruct((nodes, width), jnp.bfloat16),
        in_specs=[hbm, vmem, vmem] + [hbm] * (2 + relations),
        out_specs=vmem,
        scratch_shapes=[
            pltpu.VMEM(degree.shape, degree.dtype),
            pltpu.VMEM(partial.shape, partial.dtype),
            pltpu.VMEM((relations * width, width), jnp.bfloat16),
            pltpu.VMEM(counts.shape, counts.dtype),
            pltpu.VMEM((nodes, relations * width), jnp.bfloat16),
            pltpu.SemaphoreType.DMA((1, degree.shape[0])),
            pltpu.SemaphoreType.DMA((2 + relations,)),
        ],
        compiler_params=params(44),
        cost_estimate=estimate(
            2 * rows * depth * width + 2 * nodes * relations * width * width, 2 * rows * depth
        ),
        name="last",
    )(*in_hbm(counts), table, in_vmem(ahead), *in_hbm(degree, partial, *pieces))


def pack_body(*refs):
    inputs_hbm, out_ref, inputs_v, (out_v, sems, in_sems) = refs[:8], refs[8], refs[9:17], refs[17:]
    inputs = start_all(in_sems, *zip(inputs_hbm, inputs_v))
    coef_first, coef_second, bases_first, bases_second, self_first, self_second, features, send = (
        inputs_v
    )
    relations, bases = coef_first.shape
    devices, slot = send.shape
    piece = self_first.shape[0]
    half = relations // 2
    wait_all(inputs)

    def mix(coef_ref, bases_ref):
        mixed = []
        for relation in range(relations):
            total = coef_ref[relation, 0] * bases_ref[0].astype(jnp.float32)
            for base in range(1, bases):
                total += coef_ref[relation, base] * bases_ref[base].astype(jnp.float32)
            mixed.append(total.astype(jnp.bfloat16))
        return mixed

    first = mix(coef_first, bases_first)
    second = mix(coef_second, bases_second)
    own = [self_first[...], self_second[...]]
    for device in range(devices):
        side = device % 2
        ways = relations // EACH
        rows = first[side * half : (side + 1) * half] + [own[side]] + second[device % ways :: ways]
        for k, value in enumerate(rows):
            at = slot + k * piece
            out_v[device, at : at + piece, :] = value

    def emit(device, picked):
        out_v[device, :slot, :] = picked

    pick_rows(send, features, emit, functools.partial(send_out, out_v, out_ref, sems))
    pltpu.make_async_copy(out_v, out_ref, sems.at[0]).wait()


def pack(features, send, bases_first, self_first, coef_first, bases_second, self_second, coef_second):
    devices, slot = send.shape
    relations = coef_first.shape[0]
    piece, width = self_first.shape
    hbm = pl.BlockSpec(memory_space=pltpu.HBM)
    shape = (devices, slot + (relations // 2 + 1 + EACH) * piece, width)
    args = (
        coef_first, coef_second, bases_first, bases_second, self_first, self_second, features, send,
    )
    return pl.pallas_call(
        pack_body,
        out_shape=pltpu.HBM(shape, jnp.bfloat16),
        in_specs=[hbm] * 8,
        out_specs=hbm,
        scratch_shapes=[
            *[pltpu.SMEM(a.shape, a.dtype) for a in args[:2]],
            *[pltpu.VMEM(a.shape, a.dtype) for a in args[2:]],
            pltpu.VMEM(shape, jnp.bfloat16),
            pltpu.SemaphoreType.DMA((1,)),
            pltpu.SemaphoreType.DMA((8,)),
        ],
        compiler_params=params(24),
        cost_estimate=estimate(2 * devices * slot * features.size, 0),
        name="pack",
    )(*in_hbm(*args))


def dense_body(mean_ref, own_ref, weights_ref, bias_ref, out_ref, *, last):
    depth = mean_ref.shape[1]
    total = jnp.dot(mean_ref[...], weights_ref[:depth], preferred_element_type=jnp.float32)
    total += jnp.dot(own_ref[...], weights_ref[depth:], preferred_element_type=jnp.float32)
    total += bias_ref[...]
    out_ref[...] = (total if last else jnp.maximum(total, 0.0)).astype(jnp.bfloat16)


def dense(mean, own, weights, bias, *, last):
    nodes, width = own.shape
    vmem = pl.BlockSpec(memory_space=pltpu.VMEM)
    return pl.pallas_call(
        functools.partial(dense_body, last=last),
        out_shape=jax.ShapeDtypeStruct((nodes, width), jnp.bfloat16),
        in_specs=[vmem] * 4,
        out_specs=vmem,
        compiler_params=params(16),
        cost_estimate=estimate(2 * nodes * mean.shape[1] * width, 0),
        name="dense",
    )(mean, own, weights, bias)


def mix_weights(bases, self_weight, coef):
    mixed = jnp.einsum(
        "rb,bij->rij", coef, bases.astype(jnp.float32), precision=lax.Precision.HIGHEST
    ).astype(jnp.bfloat16)
    return jnp.concatenate([mixed, self_weight[None]], axis=0)


def general_layers(
    features, edges, send, weights_first, weights_second, bias_first, bias_second, relations
):
    node_rows, width = features.shape
    devices, slot = send.shape
    half = relations // 2
    swap = [(i, i ^ 1) for i in range(devices)]
    side = lax.axis_index("dom") & 1

    def send_all(rows, weights):
        rows = rows[send]
        halves = [
            jnp.concatenate([weights[:half], weights[relations:]], axis=0).reshape(-1, width),
            jnp.concatenate([weights[half:relations], weights[relations:]], axis=0).reshape(-1, width),
        ]
        halves = jnp.broadcast_to(jnp.stack(halves)[None], (devices // 2, 2) + halves[0].shape)
        rows = jnp.concatenate([rows, halves.reshape(devices, -1, width)], axis=1)
        return lax.all_to_all(rows, "dom", split_axis=0, concat_axis=0, tiled=True)

    def take_all(incoming):
        mine = jnp.swapaxes(incoming[:, slot:].reshape(devices, half + 1, -1, width), 0, 1)
        mine = mine.reshape(-1, width)
        other = lax.ppermute(mine[: half * width], "dom", swap)
        mine, own = mine[: half * width], mine[half * width :]
        low, high = jnp.where(side == 0, mine, other), jnp.where(side == 0, other, mine)
        return incoming[:, :slot].reshape(-1, width), jnp.concatenate([low, high, own], axis=0)

    local, remote, degree = build_streamed_call(
        *edges, node_rows=node_rows, relations=relations, remote_rows=devices * slot
    )

    def layer(rows, weights, bias, last):
        incoming = send_all(rows, weights)
        pooled = local_streamed(local, rows, group=512)
        table, full = take_all(incoming)
        mean = remote_streamed(remote, table, pooled, degree, relations=relations, group=512)
        return dense(mean, rows, full, bias[None], last=last)

    hidden = layer(features, weights_first, bias_first, False)
    return layer(hidden, weights_second, bias_second, True)


def shards(
    features,
    edge_source,
    edge_relation,
    edge_target,
    block_count,
    send_list,
    bases_first,
    self_first,
    coef_first,
    bias_first,
    bases_second,
    self_second,
    coef_second,
    bias_second,
):
    node_rows, width = features.shape
    relations = coef_first.shape[0]
    devices, slot = send_list.shape[1:]
    remote_rows = devices * slot
    send = send_list[0]
    edges = (edge_target[0, :, 0], block_count, edge_source[0], edge_relation[0], edge_target[0])
    if 2 * node_rows * relations * (node_rows + remote_rows) > WHOLE_MAX:
        return general_layers(
            features,
            edges,
            send,
            mix_weights(bases_first, self_first, coef_first),
            mix_weights(bases_second, self_second, coef_second),
            bias_first,
            bias_second,
            relations,
        )
    outgoing = pack(
        features, send, bases_first, self_first, coef_first, bases_second, self_second, coef_second
    )
    incoming = lax.all_to_all(outgoing, "dom", split_axis=0, concat_axis=0, tiled=True)
    local, remote, pooled, degree, ahead = build(
        *edges, features, relations=relations, remote_rows=remote_rows
    )
    incoming, degree = lax.optimization_barrier((incoming, degree))

    def from_peer(array, mask):
        return lax.ppermute(array, "dom", [(i, i ^ mask) for i in range(devices)])

    next_at = slot + (relations // 2 + 1) * self_first.shape[0]
    swapped = from_peer(incoming[:, slot:next_at], 1)
    row = self_first.shape[0]
    pieces = {
        (0, e): incoming[:, next_at + e * row : next_at + (e + 1) * row].reshape(width, width)
        for e in range(EACH)
    }

    def widen(mask):
        for (k, e), piece in sorted(pieces.items()):
            pieces[k | mask, e] = from_peer(piece, mask)

    mask = relations // EACH // 2
    widen(mask)
    mean = pool(remote, pooled, incoming, degree, ahead, relations=relations, slot=slot)
    pieces, mean = lax.optimization_barrier((pieces, mean))
    mask //= 2
    widen(mask)
    hidden, picked, self_next = middle(
        mean, features, incoming, swapped, bias_first[None], send, relations=relations
    )
    table = lax.all_to_all(picked, "dom", split_axis=0, concat_axis=0, tiled=True)
    while mask > 1:
        mask //= 2
        widen(mask)
    pieces = [piece for _, piece in sorted(pieces.items())]
    partial, ahead = first(
        local, remote, hidden, degree, self_next, bias_second[None], pieces, relations=relations
    )
    table, partial = lax.optimization_barrier((table, partial))
    return last(
        remote, table.reshape(-1, width), ahead, degree, partial, pieces, relations=relations
    )


def solution(mesh):
    placed = (
        P("dom", None),
        P("dom", None, None),
        P("dom", None, None),
        P("dom", None, None),
        P("dom"),
        P("dom", None, None),
        P(None, "dom", None),
        P("dom", None),
        P(),
        P(),
        P(None, "dom", None),
        P("dom", None),
        P(),
        P(),
    )
    return jax.shard_map(
        shards, mesh=mesh, in_specs=placed, out_specs=P("dom", None), check_vma=False
    )
```

```python
import functools

import jax
import jax.numpy as jnp
from jax import lax
from jax.experimental import pallas as pl
from jax.experimental.pallas import tpu as pltpu
from jax.sharding import PartitionSpec as P

WIN = 16
CHUNK = 512
GROUP = 8
EACH = 1
MIB = 1 << 20
WHOLE_MAX = 36 * MIB
CONTRACT_LANES = (((1,), (1,)), ((), ()))


def estimate(flops, nbytes):
    return pl.CostEstimate(flops=int(flops), bytes_accessed=int(nbytes), transcendentals=0)


def params(mib, **more):
    return pltpu.CompilerParams(vmem_limit_bytes=mib * MIB, **more)


def hot(rows, lanes):
    row_ids = lax.broadcasted_iota(jnp.int32, (rows, lanes.shape[1]), 0)
    return jnp.where(row_ids == lanes, 1.0, 0.0)


def code_edges(source_ref, relation_ref, target_ref, slot_ref, code_ref, low_ref, relations):
    slot = relation_ref[...] * WIN + (target_ref[...] & (WIN - 1))
    slot_ref[...] = slot
    code_ref[...] = (source_ref[...] // CHUNK) * (WIN * relations) + slot
    low_ref[...] = source_ref[...] & (CHUNK - 1)


def link_blocks(tile_ref, count_ref, head_ref, next_ref, tiles):
    def clear(t, carry):
        head_ref[t] = -1
        return carry

    lax.fori_loop(0, tiles, clear, 0)

    def link(b, carry):
        t = tile_ref[b] // WIN
        next_ref[b] = head_ref[t]
        head_ref[t] = b
        return carry

    lax.fori_loop(0, count_ref[0], link, 0)


def pair_of(first, next_ref):
    second = jnp.where(first >= 0, next_ref[jnp.maximum(first, 0)], -1)
    after = jnp.where(second >= 0, next_ref[jnp.maximum(second, 0)], -1)
    return second, after


def some_rows(ref, blocks):
    return jnp.concatenate(
        [jnp.where(b >= 0, ref[pl.ds(jnp.maximum(b, 0), 1), :], -1) for b in blocks], axis=1
    )


def count_blocks(blocks, slot_ref, code_ref, low_ref, rows, slots):
    left = hot(rows, some_rows(code_ref, blocks)).astype(jnp.bfloat16)
    right = hot(CHUNK, some_rows(low_ref, blocks)).astype(jnp.bfloat16)
    counts = lax.dot_general(left, right, CONTRACT_LANES, preferred_element_type=jnp.float32)
    degree = jnp.sum(hot(slots, some_rows(slot_ref, blocks)), axis=1, keepdims=True)
    return counts, degree


def put_counts(counts, local_ref, remote_ref, row, slots, locals_):
    for piece in range(counts.shape[0] // slots):
        part = counts[piece * slots : (piece + 1) * slots].astype(jnp.bfloat16)
        if piece < locals_:
            local_ref[pl.ds(row, slots), pl.ds(piece * CHUNK, CHUNK)] = part
        else:
            remote_ref[pl.ds(row, slots), pl.ds((piece - locals_) * CHUNK, CHUNK)] = part


def build_streamed(
    tile_ref, count_ref, source_ref, relation_ref, target_ref,
    local_ref, remote_ref, degree_ref,
    head_ref, next_ref, slot_ref, code_ref, low_ref, sum_ref,
    *, tiles, relations, locals_, pieces,
):
    slots = WIN * relations
    rows = pieces * slots
    t = pl.program_id(0)

    @pl.when(t == 0)
    def _():
        code_edges(source_ref, relation_ref, target_ref, slot_ref, code_ref, low_ref, relations)
        link_blocks(tile_ref, count_ref, head_ref, next_ref, tiles)

    sum_ref[...] = jnp.zeros_like(sum_ref)
    degree_ref[...] = jnp.zeros_like(degree_ref)

    def step(first):
        second, after = pair_of(first, next_ref)
        counts, degree = count_blocks([first, second], slot_ref, code_ref, low_ref, rows, slots)
        sum_ref[...] += counts
        degree_ref[...] += degree
        return after

    lax.while_loop(lambda first: first >= 0, step, head_ref[t])
    put_counts(sum_ref[...], local_ref, remote_ref, 0, slots, locals_)


def build_streamed_call(tile_of, count, source, relation, target, *, node_rows, relations, remote_rows):
    blocks, width = source.shape
    tiles, slots = node_rows // WIN, WIN * relations
    locals_, remotes = node_rows // CHUNK, remote_rows // CHUNK
    pieces = locals_ + remotes
    smem = pl.BlockSpec(memory_space=pltpu.SMEM)
    shapes = [
        ((tiles * slots, node_rows), jnp.bfloat16),
        ((tiles * slots, remote_rows), jnp.bfloat16),
        ((tiles * slots, 1), jnp.float32),
    ]
    whole = pl.BlockSpec((blocks, width), lambda t: (0, 0))
    return pl.pallas_call(
        functools.partial(
            build_streamed, tiles=tiles, relations=relations, locals_=locals_, pieces=pieces
        ),
        grid=(tiles,),
        out_shape=[jax.ShapeDtypeStruct(s, d) for s, d in shapes],
        in_specs=[smem, smem, whole, whole, whole],
        out_specs=[pl.BlockSpec((slots, s[1]), lambda t: (t, 0)) for s, _ in shapes],
        scratch_shapes=[
            pltpu.SMEM((tiles,), jnp.int32),
            pltpu.SMEM((blocks,), jnp.int32),
            pltpu.VMEM((blocks, width), jnp.int32),
            pltpu.VMEM((blocks, width), jnp.int32),
            pltpu.VMEM((blocks, width), jnp.int32),
            pltpu.VMEM((pieces * slots, CHUNK), jnp.float32),
        ],
        compiler_params=params(40),
        cost_estimate=estimate(
            4 * (tiles + blocks // 4) * pieces * slots * CHUNK * width,
            2 * tiles * slots * pieces * CHUNK,
        ),
        name="build",
    )(tile_of, count, source, relation, target)


def local_streamed_body(counts_ref, table_ref, pooled_ref):
    pooled_ref[...] = jnp.dot(
        counts_ref[...], table_ref[...], preferred_element_type=jnp.float32
    )


def local_streamed(counts, table, *, group):
    rows, depth = counts.shape
    width = table.shape[1]
    return pl.pallas_call(
        local_streamed_body,
        grid=(rows // group,),
        out_shape=jax.ShapeDtypeStruct((rows, width), jnp.float32),
        in_specs=[
            pl.BlockSpec((group, depth), lambda i: (i, 0)),
            pl.BlockSpec((depth, width), lambda i: (0, 0)),
        ],
        out_specs=pl.BlockSpec((group, width), lambda i: (i, 0)),
        compiler_params=params(40),
        cost_estimate=estimate(2 * rows * depth * width, 2 * rows * depth),
        name="local",
    )(counts, table)


def put_means(mean, mean_ref, first_tile, relations):
    slots = WIN * relations
    width = mean.shape[1]
    for tile in range(mean.shape[0] // slots):
        at = pl.multiple_of((first_tile + tile) * WIN, WIN)
        for relation in range(relations):
            start = tile * slots + relation * WIN
            mean_ref[pl.ds(at, WIN), pl.ds(relation * width, width)] = mean[start : start + WIN]


def remote_streamed_body(counts_ref, table_ref, pooled_ref, degree_ref, mean_ref, *, relations):
    total = pooled_ref[...] + jnp.dot(
        counts_ref[...], table_ref[...], preferred_element_type=jnp.float32
    )
    mean = total * (1.0 / jnp.maximum(degree_ref[...], 1.0))
    put_means(mean.astype(jnp.bfloat16), mean_ref, 0, relations)


def remote_streamed(counts, table, pooled, degree, *, relations, group):
    rows, depth = counts.shape
    width = table.shape[1]
    return pl.pallas_call(
        functools.partial(remote_streamed_body, relations=relations),
        grid=(rows // group,),
        out_shape=jax.ShapeDtypeStruct((rows // relations, relations * width), jnp.bfloat16),
        in_specs=[
            pl.BlockSpec((group, depth), lambda i: (i, 0)),
            pl.BlockSpec((depth, width), lambda i: (0, 0)),
            pl.BlockSpec((group, width), lambda i: (i, 0)),
            pl.BlockSpec((group, 1), lambda i: (i, 0)),
        ],
        out_specs=pl.BlockSpec((group // relations, relations * width), lambda i: (i, 0)),
        compiler_params=params(40),
        cost_estimate=estimate(2 * rows * depth * width, 2 * rows * depth),
        name="remote",
    )(counts, table, pooled, degree)


def in_vmem(array):
    return pltpu.with_memory_space_constraint(array, pltpu.VMEM)


def in_hbm(*arrays):
    return [pltpu.with_memory_space_constraint(array, pltpu.HBM) for array in arrays]


def start_all(sems, *pairs):
    copies = [pltpu.make_async_copy(a, b, sems.at[i]) for i, (a, b) in enumerate(pairs)]
    for copy in copies:
        copy.start()
    return copies


def wait_all(copies):
    for copy in copies:
        copy.wait()


def build_body(
    tile_ref, count_ref, source_hbm, relation_hbm, target_hbm, own_hbm,
    local_ref, remote_ref, pooled_ref, degree_hbm,
    source_ref, relation_ref, target_ref, own_ref, degree_ref,
    local_v, remote_v, pooled_v, head_ref, next_ref, list_ref, slot_ref, code_ref, low_ref, sum_ref,
    sems, in_sems, *, tiles, relations, locals_, pieces,
):
    slots = WIN * relations
    rows = pieces * slots
    inputs = start_all(
        in_sems,
        (source_hbm, source_ref),
        (relation_hbm, relation_ref),
        (target_hbm, target_ref),
        (own_hbm, own_ref),
    )
    wait_all(inputs)
    code_edges(source_ref, relation_ref, target_ref, slot_ref, code_ref, low_ref, relations)
    link_blocks(tile_ref, count_ref, head_ref, next_ref, tiles)
    head_ref[tiles] = -1
    degree_ref[tiles // GROUP] = jnp.zeros((slots, GROUP), jnp.float32)
    counted = functools.partial(
        count_blocks, slot_ref=slot_ref, code_ref=code_ref, low_ref=low_ref, rows=rows, slots=slots
    )

    def place(t, piece):
        row = pl.multiple_of(t * slots, slots)
        ref, at = (local_v, piece) if piece < locals_ else (remote_v, piece - locals_)
        return ref, (pl.ds(row, slots), pl.ds(at * CHUNK, CHUNK))

    def part(counts, piece):
        return counts[piece * slots : (piece + 1) * slots]

    def add(t, blocks):
        counts, degree = counted(blocks)
        for piece in range(pieces):
            ref, where = place(t, piece)
            total = ref[where].astype(jnp.float32) + part(counts, piece)
            ref[where] = total.astype(jnp.bfloat16)
        add_degree(t, degree)

    def add_degree(t, degree):
        lanes = lax.broadcasted_iota(jnp.int32, (slots, GROUP), 1)
        degree_ref[t // GROUP] += jnp.where(lanes == t % GROUP, degree, 0.0)

    def copy_tile(t):
        some = pl.ds(pl.multiple_of(t * slots, slots), slots)
        pltpu.make_async_copy(local_v.at[some], local_ref.at[some], sems.at[0]).start()
        pltpu.make_async_copy(remote_v.at[some], remote_ref.at[some], sems.at[1]).start()

    def base(i, carry):
        afters = []
        for u in range(GROUP):
            t = i * GROUP + u
            first = head_ref[t]
            second, after = pair_of(first, next_ref)
            counts, degree = counted([first, second])
            for piece in range(pieces):
                ref, where = place(t, piece)
                ref[where] = part(counts, piece).astype(jnp.bfloat16)
            degree_ref[i, :, pl.ds(u, 1)] = degree
            head_ref[t] = after
            afters.append(after)
        for u, after in enumerate(afters):

            @pl.when(after < 0)
            def _():
                copy_tile(i * GROUP + u)

        return carry

    lax.fori_loop(0, tiles // GROUP, base, 0)

    def sort_tile(t, sizes):
        short, mid, long = sizes
        first = head_ref[t]
        _, third = pair_of(first, next_ref)
        _, fifth = pair_of(third, next_ref)
        list_ref[0, short] = t
        list_ref[1, mid] = t
        list_ref[2, long] = t
        more = first >= 0
        return (
            short + jnp.where(more & (third < 0), 1, 0),
            mid + jnp.where(more & (third >= 0) & (fifth < 0), 1, 0),
            long + jnp.where(more & (fifth >= 0), 1, 0),
        )

    zero = jnp.int32(0)
    short, mid, long = lax.fori_loop(0, tiles, sort_tile, (zero, zero, zero))
    for k in range(4):
        list_ref[0, short + k] = tiles
        list_ref[1, mid + k] = tiles

    def add_short(j, carry):
        for k in range(4):
            t = list_ref[0, 4 * j + k]
            first = head_ref[t]
            second, _ = pair_of(first, next_ref)
            add(t, [first, second])
        for k in range(4):
            t = list_ref[0, 4 * j + k]

            @pl.when(t < tiles)
            def _():
                copy_tile(t)

        return carry

    def add_mid(j, carry):
        for k in range(2):
            t = list_ref[1, 2 * j + k]
            first = head_ref[t]
            second, third = pair_of(first, next_ref)
            fourth, _ = pair_of(third, next_ref)
            add(t, [first, second, third, fourth])
        for k in range(2):
            t = list_ref[1, 2 * j + k]

            @pl.when(t < tiles)
            def _():
                copy_tile(t)

        return carry

    def add_long(j, carry):
        t = list_ref[2, j]
        for piece in range(pieces):
            ref, where = place(t, piece)
            sum_ref[pl.ds(piece * slots, slots), :] = ref[where].astype(jnp.float32)

        def step(first):
            second, after = pair_of(first, next_ref)
            counts, degree = counted([first, second])
            sum_ref[...] += counts
            add_degree(t, degree)
            return after

        lax.while_loop(lambda first: first >= 0, step, head_ref[t])
        for piece in range(pieces):
            ref, where = place(t, piece)
            ref[where] = sum_ref[pl.ds(piece * slots, slots), :].astype(jnp.bfloat16)
        copy_tile(t)
        return carry

    lax.fori_loop(0, (short + 3) // 4, add_short, 0)
    lax.fori_loop(0, (mid + 1) // 2, add_mid, 0)
    lax.fori_loop(0, long, add_long, 0)

    def pool_own(i, carry):
        some = pl.ds(pl.multiple_of(i * GROUP * slots, GROUP * slots), GROUP * slots)
        pooled_v[some, :] = jnp.dot(
            local_v[some, :], own_ref[...], preferred_element_type=jnp.float32
        ).astype(jnp.bfloat16)
        pltpu.make_async_copy(pooled_v.at[some], pooled_ref.at[some], sems.at[2]).start()
        return carry

    lax.fori_loop(0, tiles // GROUP, pool_own, 0)
    every = pl.ds(0, tiles * slots)
    pltpu.make_async_copy(local_v.at[every], local_ref, sems.at[0]).wait()
    pltpu.make_async_copy(remote_v.at[every], remote_ref, sems.at[1]).wait()
    pltpu.make_async_copy(pooled_v, pooled_ref, sems.at[2]).wait()
    pltpu.sync_copy(degree_ref.at[pl.ds(0, tiles // GROUP)], degree_hbm)


def build(tile_of, count, source, relation, target, own, *, relations, remote_rows):
    blocks, block_width = source.shape
    node_rows, width = own.shape
    tiles, slots = node_rows // WIN, WIN * relations
    rows = tiles * slots
    locals_, remotes = node_rows // CHUNK, remote_rows // CHUNK
    pieces = locals_ + remotes
    vmem = pl.BlockSpec(memory_space=pltpu.VMEM)
    smem = pl.BlockSpec(memory_space=pltpu.SMEM)
    hbm = pl.BlockSpec(memory_space=pltpu.HBM)
    return pl.pallas_call(
        functools.partial(
            build_body, tiles=tiles, relations=relations, locals_=locals_, pieces=pieces
        ),
        out_shape=[
            pltpu.HBM((rows, node_rows), jnp.bfloat16),
            pltpu.HBM((rows, remote_rows), jnp.bfloat16),
            pltpu.HBM((rows, width), jnp.bfloat16),
            pltpu.HBM((tiles // GROUP, slots, GROUP), jnp.float32),
        ],
        in_specs=[smem, smem] + [hbm] * 4,
        out_specs=[hbm] * 4,
        scratch_shapes=[
            pltpu.VMEM((blocks, block_width), jnp.int32),
            pltpu.VMEM((blocks, block_width), jnp.int32),
            pltpu.VMEM((blocks, block_width), jnp.int32),
            pltpu.VMEM((node_rows, width), jnp.bfloat16),
            pltpu.VMEM((tiles // GROUP + 1, slots, GROUP), jnp.float32),
            pltpu.VMEM((rows + slots, node_rows), jnp.bfloat16),
            pltpu.VMEM((rows + slots, remote_rows), jnp.bfloat16),
            pltpu.VMEM((rows, width), jnp.bfloat16),
            pltpu.SMEM((tiles + 1,), jnp.int32),
            pltpu.SMEM((blocks,), jnp.int32),
            pltpu.SMEM((3, tiles + 8), jnp.int32),
            pltpu.VMEM((blocks, block_width), jnp.int32),
            pltpu.VMEM((blocks, block_width), jnp.int32),
            pltpu.VMEM((blocks, block_width), jnp.int32),
            pltpu.VMEM((pieces * slots, CHUNK), jnp.float32),
            pltpu.SemaphoreType.DMA((3,)),
            pltpu.SemaphoreType.DMA((4,)),
        ],
        compiler_params=params(58),
        cost_estimate=estimate(
            4 * (tiles + blocks // 4) * pieces * slots * CHUNK * block_width
            + 2 * rows * node_rows * width,
            2 * rows * pieces * CHUNK,
        ),
        name="build",
    )(tile_of, count, *in_hbm(source, relation, target, own))


def pool_groups(
    counts_ref, counts_v, sems, table_ref, degree_ref, mean_ref, relations, begun, extra=None, ahead=None
):
    slots = WIN * relations
    size = GROUP * slots
    groups = counts_ref.shape[0] // size
    held = 0 if ahead is None else 1

    def rows(i):
        return pl.ds(pl.multiple_of(i * size, size), size)

    def count_copy(i):
        return pltpu.make_async_copy(counts_ref.at[rows(i)], counts_v.at[rows(i)], sems.at[0, i])

    def extra_copy(i):
        return pltpu.make_async_copy(extra[0].at[rows(i)], extra[1].at[rows(i)], sems.at[1, i])

    def begin(i, carry):
        count_copy(i).start()
        if extra is not None:
            extra_copy(i).start()
        return carry

    def finish(i, total):
        if extra is not None:
            extra_copy(i).wait()
            total += extra[1][rows(i), :].astype(jnp.float32)
        share = 1.0 / jnp.maximum(degree_ref[i], 1.0)
        for u in range(GROUP):
            mean = total[u * slots : (u + 1) * slots] * share[:, u : u + 1]
            put_means(mean.astype(jnp.bfloat16), mean_ref, i * GROUP + u, relations)

    def step(i, carry):
        count_copy(i).wait()
        finish(
            i, jnp.dot(counts_v[rows(i), :], table_ref[...], preferred_element_type=jnp.float32)
        )
        return carry

    if held and extra is not None:
        extra_copy(0).start()
    lax.fori_loop(held, groups, begin, 0)
    begun()
    if held:
        finish(0, jnp.dot(ahead[...], table_ref[...], preferred_element_type=jnp.float32))
    lax.fori_loop(held, groups, step, 0)


def copy_table(incoming_ref, table_ref, slot):
    for device in range(incoming_ref.shape[0]):
        table_ref[device * slot : (device + 1) * slot, :] = incoming_ref[device, :slot, :]


def pool_body(
    counts_ref, pooled_ref, incoming_ref, degree_hbm, mean_ref,
    counts_v, pooled_v, table_v, degree_v, sems, in_sems, *, relations, slot,
):
    inputs = start_all(in_sems, (degree_hbm, degree_v))

    def begun():
        copy_table(incoming_ref, table_v, slot)
        wait_all(inputs)

    pool_groups(
        counts_ref, counts_v, sems, table_v, degree_v, mean_ref, relations, begun,
        extra=(pooled_ref, pooled_v),
    )


def pool(counts, pooled, incoming, degree, *, relations, slot):
    rows, depth = counts.shape
    width = incoming.shape[2]
    vmem = pl.BlockSpec(memory_space=pltpu.VMEM)
    hbm = pl.BlockSpec(memory_space=pltpu.HBM)
    return pl.pallas_call(
        functools.partial(pool_body, relations=relations, slot=slot),
        out_shape=jax.ShapeDtypeStruct((rows // relations, relations * width), jnp.bfloat16),
        in_specs=[hbm, hbm, vmem, hbm],
        out_specs=vmem,
        scratch_shapes=[
            pltpu.VMEM(counts.shape, counts.dtype),
            pltpu.VMEM(pooled.shape, pooled.dtype),
            pltpu.VMEM((depth, width), jnp.bfloat16),
            pltpu.VMEM(degree.shape, degree.dtype),
            pltpu.SemaphoreType.DMA((2, degree.shape[0])),
            pltpu.SemaphoreType.DMA((1,)),
        ],
        compiler_params=params(44),
        cost_estimate=estimate(2 * rows * depth * width, 2 * rows * depth),
        name="pool",
    )(*in_hbm(counts, pooled), incoming, *in_hbm(degree))


def pick_rows(send_ref, rows_ref, emit, done):
    devices, slot = send_ref.shape
    depth = rows_ref.shape[0]
    columns = send_ref[...].astype(jnp.float32).T.astype(jnp.int32)
    lanes = lax.broadcasted_iota(jnp.int32, (slot, depth), 1)
    step = 8
    for start in range(0, devices, step):
        chosen = jnp.concatenate(
            [
                jnp.where(columns[:, device : device + 1] == lanes, 1.0, 0.0).astype(jnp.bfloat16)
                for device in range(start, start + step)
            ],
            axis=0,
        )
        picked = jnp.dot(chosen, rows_ref[...], preferred_element_type=jnp.float32)
        for k in range(step):
            emit(start + k, picked[k * slot : (k + 1) * slot].astype(jnp.bfloat16))
        done(start, step)


def send_out(out_v, out_ref, sems, start, count):
    some = pl.ds(start, count)
    pltpu.make_async_copy(out_v.at[some], out_ref.at[some], sems.at[0]).start()


def middle_body(
    mean_ref, own_hbm, incoming_ref, swapped_ref, bias_hbm, send_hbm,
    hidden_hbm, out_ref, self_hbm,
    own_v, bias_v, send_v, hidden_v, out_v, self_v, weights_v, sems, in_sems,
    *, relations, slot,
):
    inputs = start_all(in_sems, (own_hbm, own_v), (bias_hbm, bias_v), (send_hbm, send_v))
    width = own_v.shape[1]
    half = relations // 2
    devices = incoming_ref.shape[0]
    piece = width // devices
    block = (half + 1) * width
    for m in range(half + 1):
        mine = incoming_ref[:, slot + m * piece : slot + (m + 1) * piece, :]
        weights_v[m * width : (m + 1) * width, :] = mine.reshape(width, width)
        other = swapped_ref[:, m * piece : (m + 1) * piece, :]
        weights_v[block + m * width : block + (m + 1) * width, :] = other.reshape(width, width)
    side = lax.axis_index("dom") & 1
    mine_at = pl.multiple_of(side * (half * width), width)
    other_at = pl.multiple_of((1 - side) * (half * width), width)
    own_at = pl.multiple_of(half * width + side * block, width)
    next_at = pl.multiple_of(half * width + (1 - side) * block, width)
    self_v[...] = weights_v[pl.ds(next_at, width), :]
    total = jnp.dot(
        mean_ref[:, pl.ds(mine_at, half * width)],
        weights_v[: half * width, :],
        preferred_element_type=jnp.float32,
    )
    total += jnp.dot(
        mean_ref[:, pl.ds(other_at, half * width)],
        weights_v[block : block + half * width, :],
        preferred_element_type=jnp.float32,
    )
    wait_all(inputs)
    total += jnp.dot(
        own_v[...], weights_v[pl.ds(own_at, width), :], preferred_element_type=jnp.float32
    )
    hidden_v[...] = jnp.maximum(total + bias_v[...], 0.0).astype(jnp.bfloat16)
    outputs = [
        pltpu.make_async_copy(hidden_v, hidden_hbm, sems.at[1]),
        pltpu.make_async_copy(self_v, self_hbm, sems.at[2]),
    ]
    for copy in outputs:
        copy.start()

    def emit(device, picked):
        out_v[device, :, :] = picked

    pick_rows(send_v, hidden_v, emit, functools.partial(send_out, out_v, out_ref, sems))
    pltpu.make_async_copy(out_v, out_ref, sems.at[0]).wait()
    wait_all(outputs)


def middle(mean, own, incoming, swapped, bias, send, *, relations):
    nodes, width = own.shape
    devices, slot = send.shape
    vmem = pl.BlockSpec(memory_space=pltpu.VMEM)
    hbm = pl.BlockSpec(memory_space=pltpu.HBM)
    return pl.pallas_call(
        functools.partial(middle_body, relations=relations, slot=slot),
        out_shape=[
            pltpu.HBM((nodes, width), jnp.bfloat16),
            pltpu.HBM((devices, slot, width), jnp.bfloat16),
            pltpu.HBM((width, width), jnp.bfloat16),
        ],
        in_specs=[vmem, hbm, vmem, vmem, hbm, hbm],
        out_specs=[hbm] * 3,
        scratch_shapes=[
            pltpu.VMEM(own.shape, own.dtype),
            pltpu.VMEM(bias.shape, bias.dtype),
            pltpu.VMEM(send.shape, send.dtype),
            pltpu.VMEM((nodes, width), jnp.bfloat16),
            pltpu.VMEM((devices, slot, width), jnp.bfloat16),
            pltpu.VMEM((width, width), jnp.bfloat16),
            pltpu.VMEM(((relations + 2) * width, width), jnp.bfloat16),
            pltpu.SemaphoreType.DMA((3,)),
            pltpu.SemaphoreType.DMA((3,)),
        ],
        compiler_params=params(24),
        cost_estimate=estimate(2 * nodes * mean.shape[1] * width, 0),
        name="middle",
    )(mean, *in_hbm(own), incoming, swapped, *in_hbm(bias, send))


def weight_copies(pieces, weights_v, relations):
    width = weights_v.shape[1]
    ways = relations // EACH
    class_ = lax.axis_index("dom") & (ways - 1)

    def rows(k):
        relation = (class_ ^ (k // EACH)) + ways * (k % EACH)
        return weights_v.at[pl.ds(pl.multiple_of(relation * width, width), width)]

    return [(piece, rows(k)) for k, piece in enumerate(pieces)]


def first_body(
    counts_ref, remote_ref, own_hbm, degree_hbm, self_hbm, bias_hbm, *refs, relations
):
    pieces, refs = refs[:relations], refs[relations:]
    out_hbm, ahead_ref, *refs = refs
    own_v, degree_v, self_v, bias_v, out_v, weights_v, counts_v, mean_v, sems, in_sems = refs
    inputs = start_all(in_sems, (own_hbm, own_v), (degree_hbm, degree_v))
    later = []

    def begun():
        later.extend(
            start_all(
                in_sems.at[pl.ds(2, 3 + relations)],
                (remote_ref.at[pl.ds(0, ahead_ref.shape[0])], ahead_ref),
                (self_hbm, self_v),
                (bias_hbm, bias_v),
                *weight_copies(pieces, weights_v, relations),
            )
        )
        wait_all(inputs)

    pool_groups(counts_ref, counts_v, sems, own_v, degree_v, mean_v, relations, begun)
    wait_all(later)
    total = jnp.dot(mean_v[...], weights_v[...], preferred_element_type=jnp.float32)
    total += jnp.dot(own_v[...], self_v[...], preferred_element_type=jnp.float32)
    out_v[...] = total + bias_v[...]
    pltpu.sync_copy(out_v, out_hbm)


def first(counts, remote, own, degree, self_weight, bias, pieces, *, relations):
    rows, depth = counts.shape
    nodes, width = own.shape
    hbm = pl.BlockSpec(memory_space=pltpu.HBM)
    return pl.pallas_call(
        functools.partial(first_body, relations=relations),
        out_shape=[
            pltpu.HBM((nodes, width), jnp.float32),
            pltpu.VMEM((GROUP * WIN * relations, remote.shape[1]), jnp.bfloat16),
        ],
        in_specs=[hbm] * (6 + relations),
        out_specs=[hbm, pl.BlockSpec(memory_space=pltpu.VMEM)],
        scratch_shapes=[
            pltpu.VMEM(own.shape, own.dtype),
            pltpu.VMEM(degree.shape, degree.dtype),
            pltpu.VMEM(self_weight.shape, self_weight.dtype),
            pltpu.VMEM(bias.shape, bias.dtype),
            pltpu.VMEM((nodes, width), jnp.float32),
            pltpu.VMEM((relations * width, width), jnp.bfloat16),
            pltpu.VMEM(counts.shape, counts.dtype),
            pltpu.VMEM((nodes, relations * width), jnp.bfloat16),
            pltpu.SemaphoreType.DMA((1, degree.shape[0])),
            pltpu.SemaphoreType.DMA((5 + relations,)),
        ],
        compiler_params=params(44),
        cost_estimate=estimate(
            2 * rows * depth * width + 2 * nodes * relations * width * width, 2 * rows * depth
        ),
        name="first",
    )(*in_hbm(counts, remote, own, degree, self_weight, bias, *pieces))


def last_body(counts_ref, table_ref, ahead_ref, degree_hbm, partial_hbm, *refs, relations):
    pieces, refs = refs[:relations], refs[relations:]
    out_ref, degree_v, partial_v, weights_v, counts_v, mean_v, sems, in_sems = refs
    inputs = start_all(in_sems, (degree_hbm, degree_v))
    later = []

    def begun():
        later.extend(
            start_all(
                in_sems.at[pl.ds(1, 1 + relations)],
                (partial_hbm, partial_v),
                *weight_copies(pieces, weights_v, relations),
            )
        )
        wait_all(inputs)

    pool_groups(
        counts_ref, counts_v, sems, table_ref, degree_v, mean_v, relations, begun, ahead=ahead_ref
    )
    wait_all(later)
    total = jnp.dot(mean_v[...], weights_v[...], preferred_element_type=jnp.float32)
    out_ref[...] = (total + partial_v[...]).astype(out_ref.dtype)


def last(counts, table, ahead, degree, partial, pieces, *, relations):
    rows, depth = counts.shape
    width = table.shape[1]
    nodes = rows // relations
    vmem = pl.BlockSpec(memory_space=pltpu.VMEM)
    hbm = pl.BlockSpec(memory_space=pltpu.HBM)
    return pl.pallas_call(
        functools.partial(last_body, relations=relations),
        out_shape=jax.ShapeDtypeStruct((nodes, width), jnp.bfloat16),
        in_specs=[hbm, vmem, vmem] + [hbm] * (2 + relations),
        out_specs=vmem,
        scratch_shapes=[
            pltpu.VMEM(degree.shape, degree.dtype),
            pltpu.VMEM(partial.shape, partial.dtype),
            pltpu.VMEM((relations * width, width), jnp.bfloat16),
            pltpu.VMEM(counts.shape, counts.dtype),
            pltpu.VMEM((nodes, relations * width), jnp.bfloat16),
            pltpu.SemaphoreType.DMA((1, degree.shape[0])),
            pltpu.SemaphoreType.DMA((2 + relations,)),
        ],
        compiler_params=params(44),
        cost_estimate=estimate(
            2 * rows * depth * width + 2 * nodes * relations * width * width, 2 * rows * depth
        ),
        name="last",
    )(*in_hbm(counts), table, in_vmem(ahead), *in_hbm(degree, partial, *pieces))


def pack_body(*refs):
    inputs_hbm, out_ref, inputs_v, (out_v, sems, in_sems) = refs[:8], refs[8], refs[9:17], refs[17:]
    inputs = start_all(in_sems, *zip(inputs_hbm, inputs_v))
    coef_first, coef_second, bases_first, bases_second, self_first, self_second, features, send = (
        inputs_v
    )
    relations, bases = coef_first.shape
    devices, slot = send.shape
    piece = self_first.shape[0]
    half = relations // 2
    wait_all(inputs)

    def mix(coef_ref, bases_ref):
        mixed = []
        for relation in range(relations):
            total = coef_ref[relation, 0] * bases_ref[0].astype(jnp.float32)
            for base in range(1, bases):
                total += coef_ref[relation, base] * bases_ref[base].astype(jnp.float32)
            mixed.append(total.astype(jnp.bfloat16))
        return mixed

    first = mix(coef_first, bases_first)
    second = mix(coef_second, bases_second)
    own = [self_first[...], self_second[...]]
    for device in range(devices):
        side = device % 2
        ways = relations // EACH
        rows = first[side * half : (side + 1) * half] + [own[side]] + second[device % ways :: ways]
        for k, value in enumerate(rows):
            at = slot + k * piece
            out_v[device, at : at + piece, :] = value

    def emit(device, picked):
        out_v[device, :slot, :] = picked

    pick_rows(send, features, emit, functools.partial(send_out, out_v, out_ref, sems))
    pltpu.make_async_copy(out_v, out_ref, sems.at[0]).wait()


def pack(features, send, bases_first, self_first, coef_first, bases_second, self_second, coef_second):
    devices, slot = send.shape
    relations = coef_first.shape[0]
    piece, width = self_first.shape
    hbm = pl.BlockSpec(memory_space=pltpu.HBM)
    shape = (devices, slot + (relations // 2 + 1 + EACH) * piece, width)
    args = (
        coef_first, coef_second, bases_first, bases_second, self_first, self_second, features, send,
    )
    return pl.pallas_call(
        pack_body,
        out_shape=pltpu.HBM(shape, jnp.bfloat16),
        in_specs=[hbm] * 8,
        out_specs=hbm,
        scratch_shapes=[
            *[pltpu.SMEM(a.shape, a.dtype) for a in args[:2]],
            *[pltpu.VMEM(a.shape, a.dtype) for a in args[2:]],
            pltpu.VMEM(shape, jnp.bfloat16),
            pltpu.SemaphoreType.DMA((1,)),
            pltpu.SemaphoreType.DMA((8,)),
        ],
        compiler_params=params(24),
        cost_estimate=estimate(2 * devices * slot * features.size, 0),
        name="pack",
    )(*in_hbm(*args))


def dense_body(mean_ref, own_ref, weights_ref, bias_ref, out_ref, *, last):
    depth = mean_ref.shape[1]
    total = jnp.dot(mean_ref[...], weights_ref[:depth], preferred_element_type=jnp.float32)
    total += jnp.dot(own_ref[...], weights_ref[depth:], preferred_element_type=jnp.float32)
    total += bias_ref[...]
    out_ref[...] = (total if last else jnp.maximum(total, 0.0)).astype(jnp.bfloat16)


def dense(mean, own, weights, bias, *, last):
    nodes, width = own.shape
    vmem = pl.BlockSpec(memory_space=pltpu.VMEM)
    return pl.pallas_call(
        functools.partial(dense_body, last=last),
        out_shape=jax.ShapeDtypeStruct((nodes, width), jnp.bfloat16),
        in_specs=[vmem] * 4,
        out_specs=vmem,
        compiler_params=params(16),
        cost_estimate=estimate(2 * nodes * mean.shape[1] * width, 0),
        name="dense",
    )(mean, own, weights, bias)


def mix_weights(bases, self_weight, coef):
    mixed = jnp.einsum(
        "rb,bij->rij", coef, bases.astype(jnp.float32), precision=lax.Precision.HIGHEST
    ).astype(jnp.bfloat16)
    return jnp.concatenate([mixed, self_weight[None]], axis=0)


def general_layers(
    features, edges, send, weights_first, weights_second, bias_first, bias_second, relations
):
    node_rows, width = features.shape
    devices, slot = send.shape
    half = relations // 2
    swap = [(i, i ^ 1) for i in range(devices)]
    side = lax.axis_index("dom") & 1

    def send_all(rows, weights):
        rows = rows[send]
        halves = [
            jnp.concatenate([weights[:half], weights[relations:]], axis=0).reshape(-1, width),
            jnp.concatenate([weights[half:relations], weights[relations:]], axis=0).reshape(-1, width),
        ]
        halves = jnp.broadcast_to(jnp.stack(halves)[None], (devices // 2, 2) + halves[0].shape)
        rows = jnp.concatenate([rows, halves.reshape(devices, -1, width)], axis=1)
        return lax.all_to_all(rows, "dom", split_axis=0, concat_axis=0, tiled=True)

    def take_all(incoming):
        mine = jnp.swapaxes(incoming[:, slot:].reshape(devices, half + 1, -1, width), 0, 1)
        mine = mine.reshape(-1, width)
        other = lax.ppermute(mine[: half * width], "dom", swap)
        mine, own = mine[: half * width], mine[half * width :]
        low, high = jnp.where(side == 0, mine, other), jnp.where(side == 0, other, mine)
        return incoming[:, :slot].reshape(-1, width), jnp.concatenate([low, high, own], axis=0)

    local, remote, degree = build_streamed_call(
        *edges, node_rows=node_rows, relations=relations, remote_rows=devices * slot
    )

    def layer(rows, weights, bias, last):
        incoming = send_all(rows, weights)
        pooled = local_streamed(local, rows, group=512)
        table, full = take_all(incoming)
        mean = remote_streamed(remote, table, pooled, degree, relations=relations, group=512)
        return dense(mean, rows, full, bias[None], last=last)

    hidden = layer(features, weights_first, bias_first, False)
    return layer(hidden, weights_second, bias_second, True)


def shards(
    features,
    edge_source,
    edge_relation,
    edge_target,
    block_count,
    send_list,
    bases_first,
    self_first,
    coef_first,
    bias_first,
    bases_second,
    self_second,
    coef_second,
    bias_second,
):
    node_rows, width = features.shape
    relations = coef_first.shape[0]
    devices, slot = send_list.shape[1:]
    remote_rows = devices * slot
    send = send_list[0]
    edges = (edge_target[0, :, 0], block_count, edge_source[0], edge_relation[0], edge_target[0])
    if 2 * node_rows * relations * (node_rows + remote_rows) > WHOLE_MAX:
        return general_layers(
            features,
            edges,
            send,
            mix_weights(bases_first, self_first, coef_first),
            mix_weights(bases_second, self_second, coef_second),
            bias_first,
            bias_second,
            relations,
        )
    outgoing = pack(
        features, send, bases_first, self_first, coef_first, bases_second, self_second, coef_second
    )
    incoming = lax.all_to_all(outgoing, "dom", split_axis=0, concat_axis=0, tiled=True)
    local, remote, pooled, degree = build(
        *edges, features, relations=relations, remote_rows=remote_rows
    )
    incoming, degree = lax.optimization_barrier((incoming, degree))

    def from_peer(array, mask):
        return lax.ppermute(array, "dom", [(i, i ^ mask) for i in range(devices)])

    next_at = slot + (relations // 2 + 1) * self_first.shape[0]
    swapped = from_peer(incoming[:, slot:next_at], 1)
    row = self_first.shape[0]
    pieces = {
        (0, e): incoming[:, next_at + e * row : next_at + (e + 1) * row].reshape(width, width)
        for e in range(EACH)
    }

    ways = relations // EACH
    for k in range(2, ways, 2):
        for e in range(EACH):
            pieces[k, e] = from_peer(pieces[0, e], k)
    mean = pool(remote, pooled, incoming, degree, relations=relations, slot=slot)
    pieces, mean = lax.optimization_barrier((pieces, mean))
    hidden, picked, self_next = middle(
        mean, features, incoming, swapped, bias_first[None], send, relations=relations
    )
    table = lax.all_to_all(picked, "dom", split_axis=0, concat_axis=0, tiled=True)
    pieces.update({(k | 1, e): from_peer(piece, 1) for (k, e), piece in sorted(pieces.items())})
    pieces = [piece for _, piece in sorted(pieces.items())]
    partial, ahead = first(
        local, remote, hidden, degree, self_next, bias_second[None], pieces, relations=relations
    )
    table, partial = lax.optimization_barrier((table, partial))
    return last(
        remote, table.reshape(-1, width), ahead, degree, partial, pieces, relations=relations
    )


def solution(mesh):
    placed = (
        P("dom", None),
        P("dom", None, None),
        P("dom", None, None),
        P("dom", None, None),
        P("dom"),
        P("dom", None, None),
        P(None, "dom", None),
        P("dom", None),
        P(),
        P(),
        P(None, "dom", None),
        P("dom", None),
        P(),
        P(),
    )
    return jax.shard_map(
        shards, mesh=mesh, in_specs=placed, out_specs=P("dom", None), check_vma=False
    )
```

```python
import functools

import jax
import jax.numpy as jnp
from jax import lax
from jax.experimental import pallas as pl
from jax.experimental.pallas import tpu as pltpu
from jax.sharding import PartitionSpec as P

WIN = 16
CHUNK = 512
GROUP = 8
EACH = 1
MIB = 1 << 20
WHOLE_MAX = 36 * MIB
CONTRACT_LANES = (((1,), (1,)), ((), ()))


def estimate(flops, nbytes):
    return pl.CostEstimate(flops=int(flops), bytes_accessed=int(nbytes), transcendentals=0)


def params(mib, **more):
    return pltpu.CompilerParams(vmem_limit_bytes=mib * MIB, **more)


def hot(rows, lanes):
    row_ids = lax.broadcasted_iota(jnp.int32, (rows, lanes.shape[1]), 0)
    return jnp.where(row_ids == lanes, 1.0, 0.0)


def code_edges(source_ref, relation_ref, target_ref, slot_ref, code_ref, low_ref, relations):
    slot = relation_ref[...] * WIN + (target_ref[...] & (WIN - 1))
    slot_ref[...] = slot
    code_ref[...] = (source_ref[...] // CHUNK) * (WIN * relations) + slot
    low_ref[...] = source_ref[...] & (CHUNK - 1)


def link_blocks(tile_ref, count_ref, head_ref, next_ref, tiles):
    def clear(t, carry):
        head_ref[t] = -1
        return carry

    lax.fori_loop(0, tiles, clear, 0)

    def link(b, carry):
        t = tile_ref[b] // WIN
        next_ref[b] = head_ref[t]
        head_ref[t] = b
        return carry

    lax.fori_loop(0, count_ref[0], link, 0)


def pair_of(first, next_ref):
    second = jnp.where(first >= 0, next_ref[jnp.maximum(first, 0)], -1)
    after = jnp.where(second >= 0, next_ref[jnp.maximum(second, 0)], -1)
    return second, after


def some_rows(ref, blocks):
    return jnp.concatenate(
        [jnp.where(b >= 0, ref[pl.ds(jnp.maximum(b, 0), 1), :], -1) for b in blocks], axis=1
    )


def count_blocks(blocks, slot_ref, code_ref, low_ref, rows, slots):
    left = hot(rows, some_rows(code_ref, blocks)).astype(jnp.bfloat16)
    right = hot(CHUNK, some_rows(low_ref, blocks)).astype(jnp.bfloat16)
    counts = lax.dot_general(left, right, CONTRACT_LANES, preferred_element_type=jnp.float32)
    degree = jnp.sum(hot(slots, some_rows(slot_ref, blocks)), axis=1, keepdims=True)
    return counts, degree


def put_counts(counts, local_ref, remote_ref, row, slots, locals_):
    for piece in range(counts.shape[0] // slots):
        part = counts[piece * slots : (piece + 1) * slots].astype(jnp.bfloat16)
        if piece < locals_:
            local_ref[pl.ds(row, slots), pl.ds(piece * CHUNK, CHUNK)] = part
        else:
            remote_ref[pl.ds(row, slots), pl.ds((piece - locals_) * CHUNK, CHUNK)] = part


def build_streamed(
    tile_ref, count_ref, source_ref, relation_ref, target_ref,
    local_ref, remote_ref, degree_ref,
    head_ref, next_ref, slot_ref, code_ref, low_ref, sum_ref,
    *, tiles, relations, locals_, pieces,
):
    slots = WIN * relations
    rows = pieces * slots
    t = pl.program_id(0)

    @pl.when(t == 0)
    def _():
        code_edges(source_ref, relation_ref, target_ref, slot_ref, code_ref, low_ref, relations)
        link_blocks(tile_ref, count_ref, head_ref, next_ref, tiles)

    sum_ref[...] = jnp.zeros_like(sum_ref)
    degree_ref[...] = jnp.zeros_like(degree_ref)

    def step(first):
        second, after = pair_of(first, next_ref)
        counts, degree = count_blocks([first, second], slot_ref, code_ref, low_ref, rows, slots)
        sum_ref[...] += counts
        degree_ref[...] += degree
        return after

    lax.while_loop(lambda first: first >= 0, step, head_ref[t])
    put_counts(sum_ref[...], local_ref, remote_ref, 0, slots, locals_)


def build_streamed_call(tile_of, count, source, relation, target, *, node_rows, relations, remote_rows):
    blocks, width = source.shape
    tiles, slots = node_rows // WIN, WIN * relations
    locals_, remotes = node_rows // CHUNK, remote_rows // CHUNK
    pieces = locals_ + remotes
    smem = pl.BlockSpec(memory_space=pltpu.SMEM)
    shapes = [
        ((tiles * slots, node_rows), jnp.bfloat16),
        ((tiles * slots, remote_rows), jnp.bfloat16),
        ((tiles * slots, 1), jnp.float32),
    ]
    whole = pl.BlockSpec((blocks, width), lambda t: (0, 0))
    return pl.pallas_call(
        functools.partial(
            build_streamed, tiles=tiles, relations=relations, locals_=locals_, pieces=pieces
        ),
        grid=(tiles,),
        out_shape=[jax.ShapeDtypeStruct(s, d) for s, d in shapes],
        in_specs=[smem, smem, whole, whole, whole],
        out_specs=[pl.BlockSpec((slots, s[1]), lambda t: (t, 0)) for s, _ in shapes],
        scratch_shapes=[
            pltpu.SMEM((tiles,), jnp.int32),
            pltpu.SMEM((blocks,), jnp.int32),
            pltpu.VMEM((blocks, width), jnp.int32),
            pltpu.VMEM((blocks, width), jnp.int32),
            pltpu.VMEM((blocks, width), jnp.int32),
            pltpu.VMEM((pieces * slots, CHUNK), jnp.float32),
        ],
        compiler_params=params(40),
        cost_estimate=estimate(
            4 * (tiles + blocks // 4) * pieces * slots * CHUNK * width,
            2 * tiles * slots * pieces * CHUNK,
        ),
        name="build",
    )(tile_of, count, source, relation, target)


def local_streamed_body(counts_ref, table_ref, pooled_ref):
    pooled_ref[...] = jnp.dot(
        counts_ref[...], table_ref[...], preferred_element_type=jnp.float32
    )


def local_streamed(counts, table, *, group):
    rows, depth = counts.shape
    width = table.shape[1]
    return pl.pallas_call(
        local_streamed_body,
        grid=(rows // group,),
        out_shape=jax.ShapeDtypeStruct((rows, width), jnp.float32),
        in_specs=[
            pl.BlockSpec((group, depth), lambda i: (i, 0)),
            pl.BlockSpec((depth, width), lambda i: (0, 0)),
        ],
        out_specs=pl.BlockSpec((group, width), lambda i: (i, 0)),
        compiler_params=params(40),
        cost_estimate=estimate(2 * rows * depth * width, 2 * rows * depth),
        name="local",
    )(counts, table)


def put_means(mean, mean_ref, first_tile, relations):
    slots = WIN * relations
    width = mean.shape[1]
    for tile in range(mean.shape[0] // slots):
        at = pl.multiple_of((first_tile + tile) * WIN, WIN)
        for relation in range(relations):
            start = tile * slots + relation * WIN
            mean_ref[pl.ds(at, WIN), pl.ds(relation * width, width)] = mean[start : start + WIN]


def remote_streamed_body(counts_ref, table_ref, pooled_ref, degree_ref, mean_ref, *, relations):
    total = pooled_ref[...] + jnp.dot(
        counts_ref[...], table_ref[...], preferred_element_type=jnp.float32
    )
    mean = total * (1.0 / jnp.maximum(degree_ref[...], 1.0))
    put_means(mean.astype(jnp.bfloat16), mean_ref, 0, relations)


def remote_streamed(counts, table, pooled, degree, *, relations, group):
    rows, depth = counts.shape
    width = table.shape[1]
    return pl.pallas_call(
        functools.partial(remote_streamed_body, relations=relations),
        grid=(rows // group,),
        out_shape=jax.ShapeDtypeStruct((rows // relations, relations * width), jnp.bfloat16),
        in_specs=[
            pl.BlockSpec((group, depth), lambda i: (i, 0)),
            pl.BlockSpec((depth, width), lambda i: (0, 0)),
            pl.BlockSpec((group, width), lambda i: (i, 0)),
            pl.BlockSpec((group, 1), lambda i: (i, 0)),
        ],
        out_specs=pl.BlockSpec((group // relations, relations * width), lambda i: (i, 0)),
        compiler_params=params(40),
        cost_estimate=estimate(2 * rows * depth * width, 2 * rows * depth),
        name="remote",
    )(counts, table, pooled, degree)


def in_vmem(array):
    return pltpu.with_memory_space_constraint(array, pltpu.VMEM)


def in_hbm(*arrays):
    return [pltpu.with_memory_space_constraint(array, pltpu.HBM) for array in arrays]


def start_all(sems, *pairs):
    copies = [pltpu.make_async_copy(a, b, sems.at[i]) for i, (a, b) in enumerate(pairs)]
    for copy in copies:
        copy.start()
    return copies


def wait_all(copies):
    for copy in copies:
        copy.wait()


def build_body(
    tile_ref, count_ref, source_hbm, relation_hbm, target_hbm, own_hbm,
    local_ref, remote_ref, pooled_ref, degree_hbm,
    source_ref, relation_ref, target_ref, own_ref, degree_ref,
    local_v, remote_v, pooled_v, head_ref, next_ref, list_ref, slot_ref, code_ref, low_ref, sum_ref,
    sems, in_sems, *, tiles, relations, locals_, pieces,
):
    slots = WIN * relations
    rows = pieces * slots
    inputs = start_all(
        in_sems,
        (source_hbm, source_ref),
        (relation_hbm, relation_ref),
        (target_hbm, target_ref),
        (own_hbm, own_ref),
    )
    wait_all(inputs)
    code_edges(source_ref, relation_ref, target_ref, slot_ref, code_ref, low_ref, relations)
    link_blocks(tile_ref, count_ref, head_ref, next_ref, tiles)
    head_ref[tiles] = -1
    degree_ref[tiles // GROUP] = jnp.zeros((slots, GROUP), jnp.float32)
    counted = functools.partial(
        count_blocks, slot_ref=slot_ref, code_ref=code_ref, low_ref=low_ref, rows=rows, slots=slots
    )

    def place(t, piece):
        row = pl.multiple_of(t * slots, slots)
        ref, at = (local_v, piece) if piece < locals_ else (remote_v, piece - locals_)
        return ref, (pl.ds(row, slots), pl.ds(at * CHUNK, CHUNK))

    def part(counts, piece):
        return counts[piece * slots : (piece + 1) * slots]

    def add(t, blocks):
        counts, degree = counted(blocks)
        for piece in range(pieces):
            ref, where = place(t, piece)
            total = ref[where].astype(jnp.float32) + part(counts, piece)
            ref[where] = total.astype(jnp.bfloat16)
        add_degree(t, degree)

    def add_degree(t, degree):
        lanes = lax.broadcasted_iota(jnp.int32, (slots, GROUP), 1)
        degree_ref[t // GROUP] += jnp.where(lanes == t % GROUP, degree, 0.0)

    def copy_tile(t):
        some = pl.ds(pl.multiple_of(t * slots, slots), slots)
        pltpu.make_async_copy(local_v.at[some], local_ref.at[some], sems.at[0]).start()
        pltpu.make_async_copy(remote_v.at[some], remote_ref.at[some], sems.at[1]).start()

    def base(i, carry):
        afters = []
        for u in range(GROUP):
            t = i * GROUP + u
            first = head_ref[t]
            second, after = pair_of(first, next_ref)
            counts, degree = counted([first, second])
            for piece in range(pieces):
                ref, where = place(t, piece)
                ref[where] = part(counts, piece).astype(jnp.bfloat16)
            degree_ref[i, :, pl.ds(u, 1)] = degree
            head_ref[t] = after
            afters.append(after)
        for u, after in enumerate(afters):

            @pl.when(after < 0)
            def _():
                copy_tile(i * GROUP + u)

        return carry

    lax.fori_loop(0, tiles // GROUP, base, 0)

    def sort_tile(t, sizes):
        short, mid, long = sizes
        first = head_ref[t]
        _, third = pair_of(first, next_ref)
        _, fifth = pair_of(third, next_ref)
        list_ref[0, short] = t
        list_ref[1, mid] = t
        list_ref[2, long] = t
        more = first >= 0
        return (
            short + jnp.where(more & (third < 0), 1, 0),
            mid + jnp.where(more & (third >= 0) & (fifth < 0), 1, 0),
            long + jnp.where(more & (fifth >= 0), 1, 0),
        )

    zero = jnp.int32(0)
    short, mid, long = lax.fori_loop(0, tiles, sort_tile, (zero, zero, zero))
    for k in range(4):
        list_ref[0, short + k] = tiles
        list_ref[1, mid + k] = tiles

    def add_short(j, carry):
        for k in range(4):
            t = list_ref[0, 4 * j + k]
            first = head_ref[t]
            second, _ = pair_of(first, next_ref)
            add(t, [first, second])
        for k in range(4):
            t = list_ref[0, 4 * j + k]

            @pl.when(t < tiles)
            def _():
                copy_tile(t)

        return carry

    def add_mid(j, carry):
        for k in range(2):
            t = list_ref[1, 2 * j + k]
            first = head_ref[t]
            second, third = pair_of(first, next_ref)
            fourth, _ = pair_of(third, next_ref)
            add(t, [first, second, third, fourth])
        for k in range(2):
            t = list_ref[1, 2 * j + k]

            @pl.when(t < tiles)
            def _():
                copy_tile(t)

        return carry

    def add_long(j, carry):
        t = list_ref[2, j]
        for piece in range(pieces):
            ref, where = place(t, piece)
            sum_ref[pl.ds(piece * slots, slots), :] = ref[where].astype(jnp.float32)

        def step(first):
            second, after = pair_of(first, next_ref)
            counts, degree = counted([first, second])
            sum_ref[...] += counts
            add_degree(t, degree)
            return after

        lax.while_loop(lambda first: first >= 0, step, head_ref[t])
        for piece in range(pieces):
            ref, where = place(t, piece)
            ref[where] = sum_ref[pl.ds(piece * slots, slots), :].astype(jnp.bfloat16)
        copy_tile(t)
        return carry

    lax.fori_loop(0, (short + 3) // 4, add_short, 0)
    lax.fori_loop(0, (mid + 1) // 2, add_mid, 0)
    lax.fori_loop(0, long, add_long, 0)

    def pool_own(i, carry):
        some = pl.ds(pl.multiple_of(i * GROUP * slots, GROUP * slots), GROUP * slots)
        pooled_v[some, :] = jnp.dot(
            local_v[some, :], own_ref[...], preferred_element_type=jnp.float32
        ).astype(jnp.bfloat16)
        pltpu.make_async_copy(pooled_v.at[some], pooled_ref.at[some], sems.at[2]).start()
        return carry

    lax.fori_loop(0, tiles // GROUP, pool_own, 0)
    every = pl.ds(0, tiles * slots)
    pltpu.make_async_copy(local_v.at[every], local_ref, sems.at[0]).wait()
    pltpu.make_async_copy(remote_v.at[every], remote_ref, sems.at[1]).wait()
    pltpu.make_async_copy(pooled_v, pooled_ref, sems.at[2]).wait()
    pltpu.sync_copy(degree_ref.at[pl.ds(0, tiles // GROUP)], degree_hbm)


def build(tile_of, count, source, relation, target, own, *, relations, remote_rows):
    blocks, block_width = source.shape
    node_rows, width = own.shape
    tiles, slots = node_rows // WIN, WIN * relations
    rows = tiles * slots
    locals_, remotes = node_rows // CHUNK, remote_rows // CHUNK
    pieces = locals_ + remotes
    vmem = pl.BlockSpec(memory_space=pltpu.VMEM)
    smem = pl.BlockSpec(memory_space=pltpu.SMEM)
    hbm = pl.BlockSpec(memory_space=pltpu.HBM)
    return pl.pallas_call(
        functools.partial(
            build_body, tiles=tiles, relations=relations, locals_=locals_, pieces=pieces
        ),
        out_shape=[
            pltpu.HBM((rows, node_rows), jnp.bfloat16),
            pltpu.HBM((rows, remote_rows), jnp.bfloat16),
            pltpu.HBM((rows, width), jnp.bfloat16),
            pltpu.HBM((tiles // GROUP, slots, GROUP), jnp.float32),
        ],
        in_specs=[smem, smem] + [hbm] * 4,
        out_specs=[hbm] * 4,
        scratch_shapes=[
            pltpu.VMEM((blocks, block_width), jnp.int32),
            pltpu.VMEM((blocks, block_width), jnp.int32),
            pltpu.VMEM((blocks, block_width), jnp.int32),
            pltpu.VMEM((node_rows, width), jnp.bfloat16),
            pltpu.VMEM((tiles // GROUP + 1, slots, GROUP), jnp.float32),
            pltpu.VMEM((rows + slots, node_rows), jnp.bfloat16),
            pltpu.VMEM((rows + slots, remote_rows), jnp.bfloat16),
            pltpu.VMEM((rows, width), jnp.bfloat16),
            pltpu.SMEM((tiles + 1,), jnp.int32),
            pltpu.SMEM((blocks,), jnp.int32),
            pltpu.SMEM((3, tiles + 8), jnp.int32),
            pltpu.VMEM((blocks, block_width), jnp.int32),
            pltpu.VMEM((blocks, block_width), jnp.int32),
            pltpu.VMEM((blocks, block_width), jnp.int32),
            pltpu.VMEM((pieces * slots, CHUNK), jnp.float32),
            pltpu.SemaphoreType.DMA((3,)),
            pltpu.SemaphoreType.DMA((4,)),
        ],
        compiler_params=params(58),
        cost_estimate=estimate(
            4 * (tiles + blocks // 4) * pieces * slots * CHUNK * block_width
            + 2 * rows * node_rows * width,
            2 * rows * pieces * CHUNK,
        ),
        name="build",
    )(tile_of, count, *in_hbm(source, relation, target, own))


def pool_groups(
    counts_ref, counts_v, sems, table_ref, degree_ref, mean_ref, relations, begun, extra=None, ahead=None
):
    slots = WIN * relations
    size = GROUP * slots
    groups = counts_ref.shape[0] // size
    held = 0 if ahead is None else 1

    def rows(i):
        return pl.ds(pl.multiple_of(i * size, size), size)

    def count_copy(i):
        return pltpu.make_async_copy(counts_ref.at[rows(i)], counts_v.at[rows(i)], sems.at[0, i])

    def extra_copy(i):
        return pltpu.make_async_copy(extra[0].at[rows(i)], extra[1].at[rows(i)], sems.at[1, i])

    def begin(i, carry):
        count_copy(i).start()
        if extra is not None:
            extra_copy(i).start()
        return carry

    def finish(i, total):
        if extra is not None:
            total += extra[1][rows(i), :].astype(jnp.float32)
        share = 1.0 / jnp.maximum(degree_ref[i], 1.0)
        for u in range(GROUP):
            mean = total[u * slots : (u + 1) * slots] * share[:, u : u + 1]
            put_means(mean.astype(jnp.bfloat16), mean_ref, i * GROUP + u, relations)

    def step(i, carry):
        count_copy(i).wait()
        if extra is not None:
            extra_copy(i).wait()
        finish(
            i, jnp.dot(counts_v[rows(i), :], table_ref[...], preferred_element_type=jnp.float32)
        )
        return carry

    lax.fori_loop(held, groups, begin, 0)
    begun()
    if held:
        finish(0, jnp.dot(ahead[...], table_ref[...], preferred_element_type=jnp.float32))
    lax.fori_loop(held, groups, step, 0)


def copy_table(incoming_ref, table_ref, slot):
    for device in range(incoming_ref.shape[0]):
        table_ref[device * slot : (device + 1) * slot, :] = incoming_ref[device, :slot, :]


def pool_body(
    counts_ref, pooled_ref, incoming_ref, degree_hbm, mean_ref,
    counts_v, pooled_v, table_v, degree_v, sems, in_sems, *, relations, slot,
):
    inputs = start_all(in_sems, (degree_hbm, degree_v))

    def begun():
        copy_table(incoming_ref, table_v, slot)
        wait_all(inputs)

    pool_groups(
        counts_ref, counts_v, sems, table_v, degree_v, mean_ref, relations, begun,
        extra=(pooled_ref, pooled_v),
    )


def pool(counts, pooled, incoming, degree, *, relations, slot):
    rows, depth = counts.shape
    width = incoming.shape[2]
    vmem = pl.BlockSpec(memory_space=pltpu.VMEM)
    hbm = pl.BlockSpec(memory_space=pltpu.HBM)
    return pl.pallas_call(
        functools.partial(pool_body, relations=relations, slot=slot),
        out_shape=jax.ShapeDtypeStruct((rows // relations, relations * width), jnp.bfloat16),
        in_specs=[hbm, hbm, vmem, hbm],
        out_specs=vmem,
        scratch_shapes=[
            pltpu.VMEM(counts.shape, counts.dtype),
            pltpu.VMEM(pooled.shape, pooled.dtype),
            pltpu.VMEM((depth, width), jnp.bfloat16),
            pltpu.VMEM(degree.shape, degree.dtype),
            pltpu.SemaphoreType.DMA((2, degree.shape[0])),
            pltpu.SemaphoreType.DMA((1,)),
        ],
        compiler_params=params(44),
        cost_estimate=estimate(2 * rows * depth * width, 2 * rows * depth),
        name="pool",
    )(*in_hbm(counts, pooled), incoming, *in_hbm(degree))


def pick_rows(send_ref, rows_ref, emit, done):
    devices, slot = send_ref.shape
    depth = rows_ref.shape[0]
    columns = send_ref[...].astype(jnp.float32).T.astype(jnp.int32)
    lanes = lax.broadcasted_iota(jnp.int32, (slot, depth), 1)
    step = 8
    for start in range(0, devices, step):
        chosen = jnp.concatenate(
            [
                jnp.where(columns[:, device : device + 1] == lanes, 1.0, 0.0).astype(jnp.bfloat16)
                for device in range(start, start + step)
            ],
            axis=0,
        )
        picked = jnp.dot(chosen, rows_ref[...], preferred_element_type=jnp.float32)
        for k in range(step):
            emit(start + k, picked[k * slot : (k + 1) * slot].astype(jnp.bfloat16))
        done(start, step)


def send_out(out_v, out_ref, sems, start, count):
    some = pl.ds(start, count)
    pltpu.make_async_copy(out_v.at[some], out_ref.at[some], sems.at[0]).start()


def middle_body(
    mean_ref, own_hbm, incoming_ref, swapped_ref, bias_hbm, send_hbm,
    hidden_hbm, out_ref, self_hbm,
    own_v, bias_v, send_v, hidden_v, out_v, self_v, weights_v, sems, in_sems,
    *, relations, slot,
):
    inputs = start_all(in_sems, (own_hbm, own_v), (bias_hbm, bias_v), (send_hbm, send_v))
    width = own_v.shape[1]
    half = relations // 2
    devices = incoming_ref.shape[0]
    piece = width // devices
    block = (half + 1) * width
    for device in range(devices):
        for m in range(half + 1):
            at = m * width + device * piece
            weights_v[at : at + piece, :] = incoming_ref[
                device, slot + m * piece : slot + (m + 1) * piece, :
            ]
            weights_v[block + at : block + at + piece, :] = swapped_ref[
                device, m * piece : (m + 1) * piece, :
            ]
    side = lax.axis_index("dom") & 1
    mine_at = pl.multiple_of(side * (half * width), width)
    other_at = pl.multiple_of((1 - side) * (half * width), width)
    own_at = pl.multiple_of(half * width + side * block, width)
    next_at = pl.multiple_of(half * width + (1 - side) * block, width)
    self_v[...] = weights_v[pl.ds(next_at, width), :]
    total = jnp.dot(
        mean_ref[:, pl.ds(mine_at, half * width)],
        weights_v[: half * width, :],
        preferred_element_type=jnp.float32,
    )
    total += jnp.dot(
        mean_ref[:, pl.ds(other_at, half * width)],
        weights_v[block : block + half * width, :],
        preferred_element_type=jnp.float32,
    )
    wait_all(inputs)
    total += jnp.dot(
        own_v[...], weights_v[pl.ds(own_at, width), :], preferred_element_type=jnp.float32
    )
    hidden_v[...] = jnp.maximum(total + bias_v[...], 0.0).astype(jnp.bfloat16)
    outputs = [
        pltpu.make_async_copy(hidden_v, hidden_hbm, sems.at[1]),
        pltpu.make_async_copy(self_v, self_hbm, sems.at[2]),
    ]
    for copy in outputs:
        copy.start()

    def emit(device, picked):
        out_v[device, :, :] = picked

    pick_rows(send_v, hidden_v, emit, functools.partial(send_out, out_v, out_ref, sems))
    pltpu.make_async_copy(out_v, out_ref, sems.at[0]).wait()
    wait_all(outputs)


def middle(mean, own, incoming, swapped, bias, send, *, relations):
    nodes, width = own.shape
    devices, slot = send.shape
    vmem = pl.BlockSpec(memory_space=pltpu.VMEM)
    hbm = pl.BlockSpec(memory_space=pltpu.HBM)
    return pl.pallas_call(
        functools.partial(middle_body, relations=relations, slot=slot),
        out_shape=[
            pltpu.HBM((nodes, width), jnp.bfloat16),
            pltpu.HBM((devices, slot, width), jnp.bfloat16),
            pltpu.HBM((width, width), jnp.bfloat16),
        ],
        in_specs=[vmem, hbm, vmem, vmem, hbm, hbm],
        out_specs=[hbm] * 3,
        scratch_shapes=[
            pltpu.VMEM(own.shape, own.dtype),
            pltpu.VMEM(bias.shape, bias.dtype),
            pltpu.VMEM(send.shape, send.dtype),
            pltpu.VMEM((nodes, width), jnp.bfloat16),
            pltpu.VMEM((devices, slot, width), jnp.bfloat16),
            pltpu.VMEM((width, width), jnp.bfloat16),
            pltpu.VMEM(((relations + 2) * width, width), jnp.bfloat16),
            pltpu.SemaphoreType.DMA((3,)),
            pltpu.SemaphoreType.DMA((3,)),
        ],
        compiler_params=params(24),
        cost_estimate=estimate(2 * nodes * mean.shape[1] * width, 0),
        name="middle",
    )(mean, *in_hbm(own), incoming, swapped, *in_hbm(bias, send))


def weight_copies(pieces, weights_v, relations):
    width = weights_v.shape[1]
    ways = relations // EACH
    class_ = lax.axis_index("dom") & (ways - 1)

    def rows(k):
        relation = (class_ ^ (k // EACH)) + ways * (k % EACH)
        return weights_v.at[pl.ds(pl.multiple_of(relation * width, width), width)]

    return [(piece, rows(k)) for k, piece in enumerate(pieces)]


def first_body(
    counts_ref, remote_ref, own_hbm, degree_hbm, self_hbm, bias_hbm, *refs, relations
):
    pieces, refs = refs[:relations], refs[relations:]
    out_hbm, ahead_ref, *refs = refs
    own_v, degree_v, self_v, bias_v, out_v, weights_v, counts_v, mean_v, sems, in_sems = refs
    inputs = start_all(in_sems, (own_hbm, own_v), (degree_hbm, degree_v))
    later = []

    def begun():
        later.extend(
            start_all(
                in_sems.at[pl.ds(2, 3 + relations)],
                (remote_ref.at[pl.ds(0, ahead_ref.shape[0])], ahead_ref),
                (self_hbm, self_v),
                (bias_hbm, bias_v),
                *weight_copies(pieces, weights_v, relations),
            )
        )
        wait_all(inputs)

    pool_groups(counts_ref, counts_v, sems, own_v, degree_v, mean_v, relations, begun)
    wait_all(later)
    total = jnp.dot(mean_v[...], weights_v[...], preferred_element_type=jnp.float32)
    total += jnp.dot(own_v[...], self_v[...], preferred_element_type=jnp.float32)
    out_v[...] = total + bias_v[...]
    pltpu.sync_copy(out_v, out_hbm)


def first(counts, remote, own, degree, self_weight, bias, pieces, *, relations):
    rows, depth = counts.shape
    nodes, width = own.shape
    hbm = pl.BlockSpec(memory_space=pltpu.HBM)
    return pl.pallas_call(
        functools.partial(first_body, relations=relations),
        out_shape=[
            pltpu.HBM((nodes, width), jnp.float32),
            pltpu.VMEM((GROUP * WIN * relations, remote.shape[1]), jnp.bfloat16),
        ],
        in_specs=[hbm] * (6 + relations),
        out_specs=[hbm, pl.BlockSpec(memory_space=pltpu.VMEM)],
        scratch_shapes=[
            pltpu.VMEM(own.shape, own.dtype),
            pltpu.VMEM(degree.shape, degree.dtype),
            pltpu.VMEM(self_weight.shape, self_weight.dtype),
            pltpu.VMEM(bias.shape, bias.dtype),
            pltpu.VMEM((nodes, width), jnp.float32),
            pltpu.VMEM((relations * width, width), jnp.bfloat16),
            pltpu.VMEM(counts.shape, counts.dtype),
            pltpu.VMEM((nodes, relations * width), jnp.bfloat16),
            pltpu.SemaphoreType.DMA((1, degree.shape[0])),
            pltpu.SemaphoreType.DMA((5 + relations,)),
        ],
        compiler_params=params(44),
        cost_estimate=estimate(
            2 * rows * depth * width + 2 * nodes * relations * width * width, 2 * rows * depth
        ),
        name="first",
    )(*in_hbm(counts, remote, own, degree, self_weight, bias, *pieces))


def last_body(counts_ref, table_ref, ahead_ref, degree_hbm, partial_hbm, *refs, relations):
    pieces, refs = refs[:relations], refs[relations:]
    out_ref, degree_v, partial_v, weights_v, counts_v, mean_v, sems, in_sems = refs
    inputs = start_all(in_sems, (degree_hbm, degree_v))
    later = []

    def begun():
        later.extend(
            start_all(
                in_sems.at[pl.ds(1, 1 + relations)],
                (partial_hbm, partial_v),
                *weight_copies(pieces, weights_v, relations),
            )
        )
        wait_all(inputs)

    pool_groups(
        counts_ref, counts_v, sems, table_ref, degree_v, mean_v, relations, begun, ahead=ahead_ref
    )
    wait_all(later)
    total = jnp.dot(mean_v[...], weights_v[...], preferred_element_type=jnp.float32)
    out_ref[...] = (total + partial_v[...]).astype(out_ref.dtype)


def last(counts, table, ahead, degree, partial, pieces, *, relations):
    rows, depth = counts.shape
    width = table.shape[1]
    nodes = rows // relations
    vmem = pl.BlockSpec(memory_space=pltpu.VMEM)
    hbm = pl.BlockSpec(memory_space=pltpu.HBM)
    return pl.pallas_call(
        functools.partial(last_body, relations=relations),
        out_shape=jax.ShapeDtypeStruct((nodes, width), jnp.bfloat16),
        in_specs=[hbm, vmem, vmem] + [hbm] * (2 + relations),
        out_specs=vmem,
        scratch_shapes=[
            pltpu.VMEM(degree.shape, degree.dtype),
            pltpu.VMEM(partial.shape, partial.dtype),
            pltpu.VMEM((relations * width, width), jnp.bfloat16),
            pltpu.VMEM(counts.shape, counts.dtype),
            pltpu.VMEM((nodes, relations * width), jnp.bfloat16),
            pltpu.SemaphoreType.DMA((1, degree.shape[0])),
            pltpu.SemaphoreType.DMA((2 + relations,)),
        ],
        compiler_params=params(44),
        cost_estimate=estimate(
            2 * rows * depth * width + 2 * nodes * relations * width * width, 2 * rows * depth
        ),
        name="last",
    )(*in_hbm(counts), table, in_vmem(ahead), *in_hbm(degree, partial, *pieces))


def pack_body(*refs):
    inputs_hbm, out_ref, inputs_v, (out_v, sems, in_sems) = refs[:8], refs[8], refs[9:17], refs[17:]
    inputs = start_all(in_sems, *zip(inputs_hbm, inputs_v))
    coef_first, coef_second, bases_first, bases_second, self_first, self_second, features, send = (
        inputs_v
    )
    relations, bases = coef_first.shape
    devices, slot = send.shape
    piece = self_first.shape[0]
    half = relations // 2
    wait_all(inputs)

    def mix(coef_ref, bases_ref):
        mixed = []
        for relation in range(relations):
            total = coef_ref[relation, 0] * bases_ref[0].astype(jnp.float32)
            for base in range(1, bases):
                total += coef_ref[relation, base] * bases_ref[base].astype(jnp.float32)
            mixed.append(total.astype(jnp.bfloat16))
        return mixed

    first = mix(coef_first, bases_first)
    second = mix(coef_second, bases_second)
    own = [self_first[...], self_second[...]]
    for device in range(devices):
        side = device % 2
        ways = relations // EACH
        rows = first[side * half : (side + 1) * half] + [own[side]] + second[device % ways :: ways]
        for k, value in enumerate(rows):
            at = slot + k * piece
            out_v[device, at : at + piece, :] = value

    def emit(device, picked):
        out_v[device, :slot, :] = picked

    pick_rows(send, features, emit, functools.partial(send_out, out_v, out_ref, sems))
    pltpu.make_async_copy(out_v, out_ref, sems.at[0]).wait()


def pack(features, send, bases_first, self_first, coef_first, bases_second, self_second, coef_second):
    devices, slot = send.shape
    relations = coef_first.shape[0]
    piece, width = self_first.shape
    hbm = pl.BlockSpec(memory_space=pltpu.HBM)
    shape = (devices, slot + (relations // 2 + 1 + EACH) * piece, width)
    args = (
        coef_first, coef_second, bases_first, bases_second, self_first, self_second, features, send,
    )
    return pl.pallas_call(
        pack_body,
        out_shape=pltpu.HBM(shape, jnp.bfloat16),
        in_specs=[hbm] * 8,
        out_specs=hbm,
        scratch_shapes=[
            *[pltpu.SMEM(a.shape, a.dtype) for a in args[:2]],
            *[pltpu.VMEM(a.shape, a.dtype) for a in args[2:]],
            pltpu.VMEM(shape, jnp.bfloat16),
            pltpu.SemaphoreType.DMA((1,)),
            pltpu.SemaphoreType.DMA((8,)),
        ],
        compiler_params=params(24),
        cost_estimate=estimate(2 * devices * slot * features.size, 0),
        name="pack",
    )(*in_hbm(*args))


def dense_body(mean_ref, own_ref, weights_ref, bias_ref, out_ref, *, last):
    depth = mean_ref.shape[1]
    total = jnp.dot(mean_ref[...], weights_ref[:depth], preferred_element_type=jnp.float32)
    total += jnp.dot(own_ref[...], weights_ref[depth:], preferred_element_type=jnp.float32)
    total += bias_ref[...]
    out_ref[...] = (total if last else jnp.maximum(total, 0.0)).astype(jnp.bfloat16)


def dense(mean, own, weights, bias, *, last):
    nodes, width = own.shape
    vmem = pl.BlockSpec(memory_space=pltpu.VMEM)
    return pl.pallas_call(
        functools.partial(dense_body, last=last),
        out_shape=jax.ShapeDtypeStruct((nodes, width), jnp.bfloat16),
        in_specs=[vmem] * 4,
        out_specs=vmem,
        compiler_params=params(16),
        cost_estimate=estimate(2 * nodes * mean.shape[1] * width, 0),
        name="dense",
    )(mean, own, weights, bias)


def mix_weights(bases, self_weight, coef):
    mixed = jnp.einsum(
        "rb,bij->rij", coef, bases.astype(jnp.float32), precision=lax.Precision.HIGHEST
    ).astype(jnp.bfloat16)
    return jnp.concatenate([mixed, self_weight[None]], axis=0)


def general_layers(
    features, edges, send, weights_first, weights_second, bias_first, bias_second, relations
):
    node_rows, width = features.shape
    devices, slot = send.shape
    half = relations // 2
    swap = [(i, i ^ 1) for i in range(devices)]
    side = lax.axis_index("dom") & 1

    def send_all(rows, weights):
        rows = rows[send]
        halves = [
            jnp.concatenate([weights[:half], weights[relations:]], axis=0).reshape(-1, width),
            jnp.concatenate([weights[half:relations], weights[relations:]], axis=0).reshape(-1, width),
        ]
        halves = jnp.broadcast_to(jnp.stack(halves)[None], (devices // 2, 2) + halves[0].shape)
        rows = jnp.concatenate([rows, halves.reshape(devices, -1, width)], axis=1)
        return lax.all_to_all(rows, "dom", split_axis=0, concat_axis=0, tiled=True)

    def take_all(incoming):
        mine = jnp.swapaxes(incoming[:, slot:].reshape(devices, half + 1, -1, width), 0, 1)
        mine = mine.reshape(-1, width)
        other = lax.ppermute(mine[: half * width], "dom", swap)
        mine, own = mine[: half * width], mine[half * width :]
        low, high = jnp.where(side == 0, mine, other), jnp.where(side == 0, other, mine)
        return incoming[:, :slot].reshape(-1, width), jnp.concatenate([low, high, own], axis=0)

    local, remote, degree = build_streamed_call(
        *edges, node_rows=node_rows, relations=relations, remote_rows=devices * slot
    )

    def layer(rows, weights, bias, last):
        incoming = send_all(rows, weights)
        pooled = local_streamed(local, rows, group=512)
        table, full = take_all(incoming)
        mean = remote_streamed(remote, table, pooled, degree, relations=relations, group=512)
        return dense(mean, rows, full, bias[None], last=last)

    hidden = layer(features, weights_first, bias_first, False)
    return layer(hidden, weights_second, bias_second, True)


def shards(
    features,
    edge_source,
    edge_relation,
    edge_target,
    block_count,
    send_list,
    bases_first,
    self_first,
    coef_first,
    bias_first,
    bases_second,
    self_second,
    coef_second,
    bias_second,
):
    node_rows, width = features.shape
    relations = coef_first.shape[0]
    devices, slot = send_list.shape[1:]
    remote_rows = devices * slot
    send = send_list[0]
    edges = (edge_target[0, :, 0], block_count, edge_source[0], edge_relation[0], edge_target[0])
    if 2 * node_rows * relations * (node_rows + remote_rows) > WHOLE_MAX:
        return general_layers(
            features,
            edges,
            send,
            mix_weights(bases_first, self_first, coef_first),
            mix_weights(bases_second, self_second, coef_second),
            bias_first,
            bias_second,
            relations,
        )
    outgoing = pack(
        features, send, bases_first, self_first, coef_first, bases_second, self_second, coef_second
    )
    incoming = lax.all_to_all(outgoing, "dom", split_axis=0, concat_axis=0, tiled=True)
    local, remote, pooled, degree = build(
        *edges, features, relations=relations, remote_rows=remote_rows
    )
    incoming, degree = lax.optimization_barrier((incoming, degree))

    def from_peer(array, mask):
        return lax.ppermute(array, "dom", [(i, i ^ mask) for i in range(devices)])

    next_at = slot + (relations // 2 + 1) * self_first.shape[0]
    swapped = from_peer(incoming[:, slot:next_at], 1)
    row = self_first.shape[0]
    pieces = {
        (0, e): incoming[:, next_at + e * row : next_at + (e + 1) * row].reshape(width, width)
        for e in range(EACH)
    }

    def widen(mask):
        for (k, e), piece in sorted(pieces.items()):
            pieces[k | mask, e] = from_peer(piece, mask)

    mask = relations // EACH // 2
    widen(mask)
    mean = pool(remote, pooled, incoming, degree, relations=relations, slot=slot)
    pieces, mean = lax.optimization_barrier((pieces, mean))
    mask //= 2
    widen(mask)
    hidden, picked, self_next = middle(
        mean, features, incoming, swapped, bias_first[None], send, relations=relations
    )
    table = lax.all_to_all(picked, "dom", split_axis=0, concat_axis=0, tiled=True)
    while mask > 1:
        mask //= 2
        widen(mask)
    pieces = [piece for _, piece in sorted(pieces.items())]
    partial, ahead = first(
        local, remote, hidden, degree, self_next, bias_second[None], pieces, relations=relations
    )
    table, partial = lax.optimization_barrier((table, partial))
    return last(
        remote, table.reshape(-1, width), ahead, degree, partial, pieces, relations=relations
    )


def solution(mesh):
    placed = (
        P("dom", None),
        P("dom", None, None),
        P("dom", None, None),
        P("dom", None, None),
        P("dom"),
        P("dom", None, None),
        P(None, "dom", None),
        P("dom", None),
        P(),
        P(),
        P(None, "dom", None),
        P("dom", None),
        P(),
        P(),
    )
    return jax.shard_map(
        shards, mesh=mesh, in_specs=placed, out_specs=P("dom", None), check_vma=False
    )
```
